32 devices in a mesh: dp: 4 (over y, x), ctx: 8 (over z, core).
Axes of the slice: x: 2, y: 2, z: 4, core: 2. Of those that a mesh axis runs over, the one named last changes fastest.
Arguments:
- tokens: bfloat16 [4, 1024, 1024], P('dp', 'ctx'), may hold values from -50 to 50
- cotangent: bfloat16 [4, 1024, 1024], P('dp', 'ctx'), may hold values from -6 to 6
- weights: float32 [12596224], P('ctx'), may hold values from -5 to 5, as said below
- first_moment: float32 [12596224], P('ctx'), may hold values from -48 to 48
- second_moment: float32 [12596224], P('ctx'), may hold values from 100 to 3000
Outputs:
- layer_out: bfloat16 [4, 1024, 1024], P('dp', 'ctx')
- token_grads: float32 [4, 1024, 1024], P('dp', 'ctx')
- weight_grads: float32 [12596224], P('ctx')
- new_weights: float32 [12596224], P('ctx')
- new_first: float32 [12596224], P('ctx')
- new_second: float32 [12596224], P('ctx')
The draws below stay inside these ranges and needn't reach their ends.
Inputs may be any that keep to these rules, and one draw needn't show every extreme that they name: `weights`: the parameters laid end to end in the order of the first step.
All inputs are finite; a program needn't handle non-finite values.
Results may differ from the reference program's by a relative error of at most 0.012.
Values may be sent and summed in bfloat16 or wider, within the bound.
A program may use at most 320 MiB of HBM per device.

```python
import math
import jax
import jax.numpy as jnp
from jax import lax

D = 1024
FF = 4096
HEADS = 16
HEAD_DIM = 64
ROT = 16
STEP = 3
LENGTH = 1024
SEQS = 4
NPARAM = 12596224


def clipped_normal(index_key, dims_of):
    return jnp.clip(jax.random.normal(index_key, dims_of, jnp.float32), -5.0, 5.0)


def rough_draw(index_key, dims_of):
    return clipped_normal(index_key, dims_of)


def draw_tokens(key, part):
    keys_list = jax.random.split(key, 3)
    base_draw = clipped_normal(keys_list[0], (SEQS, LENGTH, D))
    row_scale = jnp.exp(jax.random.uniform(keys_list[1], (SEQS, LENGTH, 1), jnp.float32, -1.15, 1.15))
    col_scale = jnp.exp(jax.random.uniform(keys_list[2], (1, 1, D), jnp.float32, -1.15, 1.15))
    return (base_draw * row_scale * col_scale).astype(jnp.bfloat16)


def draw_weights(key, part):
    keys_list = jax.random.split(key, 7)
    weight_qkv = rough_draw(keys_list[0], (D, 3 * D)) * D ** (-0.5)
    weight_out = rough_draw(keys_list[1], (D, D)) * 8.0 * D ** (-0.5)
    weight_up = rough_draw(keys_list[2], (D, FF)) * D ** (-0.5)
    weight_down = rough_draw(keys_list[3], (FF, D)) * FF ** (-0.5)
    gain_rows = 1.0 + jax.random.uniform(keys_list[4], (2, D), jnp.float32, -0.5, 0.5)
    biases = 0.3 * rough_draw(keys_list[5], (7, D))
    vectors = jnp.stack([gain_rows[0], biases[0], gain_rows[1], biases[1], biases[2], biases[3], biases[4], biases[5], biases[6]])
    bias_up = 0.3 * rough_draw(keys_list[6], (FF,))
    return jnp.concatenate([weight_qkv.reshape(-1), weight_out.reshape(-1), weight_up.reshape(-1), weight_down.reshape(-1), vectors.reshape(-1), bias_up])


def block_scale(own_key, extent, cuts, least, high):
    gain = 1.0
    for dim, parts in cuts:
        heights = jax.random.uniform(jax.random.fold_in(jax.random.fold_in(own_key, 6), dim), (parts,), jnp.float32, least / len(cuts), high / len(cuts))
        gain = gain * jnp.repeat(jnp.exp(heights), extent[dim] // parts).reshape((-1,) + (1,) * (len(extent) - 1 - dim))
    return gain


def gaussian(stream_key, dims, width, most, cuts=(), held_as=jnp.bfloat16):
    values = jax.random.normal(stream_key, dims, jnp.float32) * width
    if len(cuts) > 0:
        values = block_scale(stream_key, dims, cuts, -0.22, 0.18) * values
    return jnp.clip(values, min=-most, max=most).astype(held_as)


def setup_inputs(seed: int = 0) -> dict:
    streams_of = jax.random.split(jax.random.key(seed), 6)
    return {
        "tokens": draw_tokens(jax.random.fold_in(streams_of[5], 71), 0),
        "cotangent": gaussian(streams_of[1], (SEQS, LENGTH, D), 1.0, 6.0, ((0, 4), (1, 8))),
        "weights": draw_weights(jax.random.fold_in(streams_of[5], 71), 0),
        "first_moment": gaussian(streams_of[3], (NPARAM,), 8.0, 48.0, ((0, 8),), jnp.float32),
        "second_moment": jnp.clip(jnp.exp(math.log(3000.0) - 3.4011974 * jax.random.uniform(streams_of[4], (NPARAM,), jnp.float32) ** block_scale(streams_of[4], (NPARAM,), ((0, 8),), -0.2, 0.2)), 100.0, 3000.0),
    }


@jax.custom_vjp
def low(v):
    return lax.optimization_barrier(v.astype(jnp.bfloat16)).astype(jnp.float32)

@jax.custom_vjp
def low_back(v):
    return v

def low_keep(v):
    return (low(v), None)

def low_pass(kept, grad):
    return (grad,)

def back_keep(v):
    return (v, None)

def back_low(kept, grad):
    return (low(grad),)
low.defvjp(low_keep, low_pass)
low_back.defvjp(back_keep, back_low)
HIGHEST = lax.Precision.HIGHEST
BETA_ONE = 0.9
BETA_TWO = 0.95
LEARN_RATE = 0.004
DECAY_RATE = 0.1
EPSILON = 1e-08

def matmul(left_op, right_op):
    return jnp.dot(left_op, right_op, precision=HIGHEST)

def unpack(flat_params):
    lengths = [D * 3 * D, D * D, D * FF, FF * D, 9 * D, FF]
    dims_list = [(D, 3 * D), (D, D), (D, FF), (FF, D), (9, D), (FF,)]
    pieces = []
    offset = 0
    for length, dims_of in zip(lengths, dims_list):
        pieces.append(lax.slice_in_dim(flat_params, offset, offset + length).reshape(dims_of))
        offset += length
    return pieces

def rotary_tables(positions):
    halfrot = ROT // 2
    frequency = 10000.0 ** (-2.0 * jnp.arange(halfrot, dtype=jnp.float32) / ROT)
    angles = positions.astype(jnp.float32)[:, None] * frequency[None, :]
    return (jnp.cos(angles)[:, None, :], jnp.sin(angles)[:, None, :])

def rotate(head_vals, cosine, sine_table):
    halfrot = ROT // 2
    first_half = head_vals[..., :halfrot]
    second_half = head_vals[..., halfrot:ROT]
    return jnp.concatenate([first_half * cosine - second_half * sine_table, second_half * cosine + first_half * sine_table, head_vals[..., ROT:]], axis=-1)

def layer_norm(values, gain_row, shift_row):
    average = lax.optimization_barrier(jnp.mean(values, axis=-1, keepdims=True))
    centred = values - average
    spread = lax.optimization_barrier(jnp.mean(centred * centred, axis=-1, keepdims=True))
    return centred * lax.rsqrt(spread + 1e-05) * gain_row + shift_row

def attention(queries, keys_all, values_all):
    length = queries.shape[0]
    qblock = 512 if length % 512 == 0 else length
    key_pos = jnp.arange(length)

    def one_block(block_idx):
        first_row = (block_idx * qblock).astype(jnp.int32)
        rows_q = lax.dynamic_slice_in_dim(queries, first_row, qblock, 0)
        query_pos = first_row + jnp.arange(qblock)
        scores = jnp.einsum('qhd,khd->hqk', rows_q, keys_all, precision=HIGHEST)
        scores = low_back(scores)
        allowed = key_pos[None, None, :] <= query_pos[None, :, None]
        scores = jnp.where(allowed, scores, -1e+30)
        row_top = lax.optimization_barrier(jnp.max(scores, axis=-1, keepdims=True))
        log_total = row_top + jnp.log(lax.optimization_barrier(jnp.sum(jnp.exp(scores - row_top), axis=-1, keepdims=True)))
        probability = low(jnp.exp(scores - log_total))
        return jnp.einsum('hqk,khd->qhd', probability, values_all, precision=HIGHEST)
    blocks = lax.map(jax.checkpoint(one_block), jnp.arange(length // qblock))
    return blocks.reshape(length, D)

def forward(inputs, flat_params, cosine, sine_table):
    weight_qkv, weight_out, weight_up, weight_down, vectors, bias_up = unpack(low(flat_params))
    length = inputs.shape[0]
    norm_one = low(layer_norm(inputs, vectors[0], vectors[1]))
    norm_two = low(layer_norm(inputs, vectors[2], vectors[3]))
    joined_qkv = low_back(matmul(norm_one, weight_qkv) + vectors[4:7].reshape(-1))
    query_h = joined_qkv[:, :D].reshape(length, HEADS, HEAD_DIM)
    key_h = joined_qkv[:, D:2 * D].reshape(length, HEADS, HEAD_DIM)
    value_h = joined_qkv[:, 2 * D:].reshape(length, HEADS, HEAD_DIM)
    queries = low(rotate(query_h, cosine, sine_table) * 0.125)
    keys_rot = low(rotate(key_h, cosine, sine_table))
    values_low = low(value_h)
    mixed = low(low_back(attention(queries, keys_rot, values_low)))
    branch_attn = matmul(mixed, weight_out) + vectors[7]
    upward = low_back(matmul(norm_two, weight_up) + bias_up)
    hidden = low(jax.nn.gelu(upward, approximate=False))
    branch_mlp = matmul(hidden, weight_down) + vectors[8]
    return inputs + branch_attn + branch_mlp

def reference(tokens, cotangent, weights, first_moment, second_moment):
    cosine, sine_table = rotary_tables(jnp.arange(LENGTH))

    def per_sequence(running, seq_pair):
        seq_tokens, seq_cot = seq_pair
        result, pullback = jax.vjp(lambda inputs, params: forward(inputs, params, cosine, sine_table), seq_tokens.astype(jnp.float32), weights)
        d_inputs, d_params = pullback(seq_cot.astype(jnp.float32))
        return (running + d_params, (result.astype(jnp.bfloat16), d_inputs))
    grad_sum, (layer_out, token_grads) = lax.scan(per_sequence, jnp.zeros_like(weights), (tokens, cotangent))
    new_first = BETA_ONE * first_moment + (1.0 - BETA_ONE) * grad_sum
    new_second = BETA_TWO * second_moment + (1.0 - BETA_TWO) * grad_sum * grad_sum
    corrected_m = new_first / (1.0 - BETA_ONE ** STEP)
    corrected_v = new_second / (1.0 - BETA_TWO ** STEP)
    new_weights = weights - LEARN_RATE * (corrected_m / (jnp.sqrt(corrected_v) + EPSILON) + DECAY_RATE * weights)
    return (layer_out, token_grads, grad_sum, new_weights, new_first, new_second)
```

```python
from functools import partial
import math

import numpy as np
import jax
import jax.numpy as jnp
from jax import lax
from jax.experimental import pallas as pl
from jax.experimental.pallas import tpu as pltpu
from jax.sharding import PartitionSpec as P

D = 1024
FF = 4096
HEADS = 16
HEAD_DIM = 64
ROT = 16
STEP = 3
BETA_ONE = 0.9
BETA_TWO = 0.95
LEARN_RATE = 0.004
DECAY_RATE = 0.1
EPSILON = 1e-08

F32 = jnp.float32
BF16 = jnp.bfloat16
MESH = pl.DeviceIdType.MESH
V = 8
CHIPS = V // 2
OWN = 12301
ALI = 12288
VECS = 104
HEAD = 112
RB = 256


class Geo:
    def __init__(self, mesh, tokens):
        self.q = mesh.shape["dp"]
        self.rep = mesh.shape["ctx"] // V
        self.tl = tokens // V
        self.t = tokens
        q = self.q
        self.qr = 512 // q
        self.ho = 128 // q
        self.u2 = 128 // q
        self.u3 = 384 // q
        self.seg = 1536 // q
        self.zr = V * self.seg
        self.ap = 1024 // q
        self.bp = 512 // q
        self.er = 2 * self.ap

    def place(self):
        d = lax.axis_index("dp")
        a = lax.axis_index("ctx")
        return d, a // self.rep, a % self.rep

    def dev(self, e, j, rho):
        return {"dp": e, "ctx": j * self.rep + rho}

    def maps(self):
        q, out = self.q, []
        for e in range(q):
            for i in range(2):
                for s in range(3):
                    out.append((e, self.seg * i + self.qr * s, self.qr, 0, 512 * i + self.qr * e, 128 * s))
            for b in range(8):
                out.append((e, 2 * self.seg + self.ho * b, self.ho, 1, self.ho * e, 128 * b))
            parts = (
                (0, self.u2, 2 * self.seg + self.ap),
                (128, self.u3, 3 * self.seg),
                (512, self.u3, 4 * self.seg),
                (896, self.u2, 5 * self.seg),
            )
            for r0, nr, off in parts:
                for t in range(4):
                    out.append((e, off + nr * t, nr, 2, r0 + nr * e, 128 * t))
            for t in range(4):
                for b in range(8):
                    row = 5 * self.seg + self.bp + self.ap * t + self.ho * b
                    out.append((e, row, self.ho, 3, 128 * t + self.ho * e, 128 * b))
        return out


def dot(a, b):
    return jnp.dot(a, b, preferred_element_type=F32)


def dot_nt(a, b):
    return lax.dot_general(a, b, (((1,), (1,)), ((), ())), preferred_element_type=F32)


def dot_tn(a, b):
    return lax.dot_general(a, b, (((0,), (0,)), ((), ())), preferred_element_type=F32)


def mult(x, n):
    return pl.multiple_of(x, n)


def view(part):
    return part[0].at[part[1]] if isinstance(part, tuple) else part


def rcopy(src, dst, ssem, rsem, dev):
    return pltpu.make_async_remote_copy(
        src_ref=view(src),
        dst_ref=view(dst),
        send_sem=view(ssem),
        recv_sem=view(rsem),
        device_id=dev,
        device_id_type=MESH,
    )


class Sends:
    def __init__(self, ssem, rsem):
        self.ssem, self.rsem, self.used, self.open = ssem, rsem, 0, []

    def slot(self):
        self.used += 1
        return (self.ssem, self.used - 1)

    def send(self, cond, src, dst, rs, dev):
        slot = self.slot()
        make = lambda: rcopy(src, dst, slot, (self.rsem, rs), dev)
        self.when(cond, lambda: make().start())
        self.open.append((cond, lambda: make().wait_send()))

    def copy(self, cond, src, dst):
        slot = self.slot()
        make = lambda: pltpu.make_async_copy(view(src), view(dst), view(slot))
        self.when(cond, lambda: make().start())
        self.open.append((cond, lambda: make().wait()))

    @staticmethod
    def when(cond, act):
        if cond is None:
            act()
        else:
            pl.when(cond)(act)

    def finish(self, since=0):
        for cond, act in self.open[since:]:
            self.when(cond, act)
        del self.open[since:]


def arrive(part, sem):
    pltpu.make_async_copy(view(part), view(part), view(sem)).wait()


def entry_barrier(geo, d, i, rho):
    sem = pltpu.get_barrier_semaphore()
    for k in range(1, V):
        pl.semaphore_signal(sem, inc=1, device_id=geo.dev(d, (i + k) % V, rho), device_id_type=MESH)
    for k in range(1, geo.q):
        pl.semaphore_signal(sem, inc=1, device_id=geo.dev((d + k) % geo.q, i, rho), device_id_type=MESH)
    pl.semaphore_wait(sem, V - 1 + geo.q - 1)


def cut_share(geo, i, buf, e_ref):
    q, base = geo.q, HEAD - 13 * i

    def put(j, e, row, n, start, stride):
        e_ref[j, e, pl.ds(row, n), :] = buf[pl.ds(start, n, stride=stride), :].astype(BF16)

    @pl.when(i < 2)
    def _():
        def body(n, c):
            e, s = n % q, n // q
            for b in range(8):
                put(b, e, mult(geo.qr * s, 16), geo.qr, base + 24 * geo.qr * e + 8 * s + b, 24)
            return c

        lax.fori_loop(0, 3 * q, body, 0)

    def rows_part(a0, ro, shift, count):
        def body(n, c):
            e, bl = n % q, n // q
            bb = bl + shift
            for b in range(8):
                put(
                    bb % V,
                    e,
                    mult(ro + geo.ap * (bb // V) + geo.ho * b, 16),
                    geo.ho,
                    base + a0 + 8 * (128 * bl + geo.ho * e) + b,
                    8,
                )
            return c

        lax.fori_loop(0, count * q, body, 0)

    def cols_part(a0, nr, ro):
        def body(n, c):
            e, t = n % q, n // q
            for b in range(8):
                put(b, e, mult(ro + nr * t, 16), nr, base + a0 + 32 * nr * e + 8 * t + b, 32)
            return c

        lax.fori_loop(0, 4 * q, body, 0)

    @pl.when(i == 2)
    def _():
        rows_part(0, 0, 0, 8)
        cols_part(8192, geo.u2, geo.ap)

    @pl.when((i == 3) | (i == 4))
    def _():
        cols_part(0, geo.u3, 0)

    @pl.when(i == 5)
    def _():
        cols_part(0, geo.u2, 0)
        rows_part(4096, geo.bp, 0, 8)

    @pl.when(i >= 6)
    def _():
        rows_part(0, 0, 4 * (i - 6), 12)


def owner_moves(geo, i, j):
    k = i - 6
    return (
        (i < 6, 0, mult(geo.seg * i, 16), geo.seg),
        (i >= 6, mult(geo.ap * k, 16), mult(6 * geo.seg + 2 * geo.ap * k, 16), geo.ap),
        ((i >= 6) & (j // 4 == k), mult(geo.ap * (1 - k), 16), 6 * geo.seg + geo.ap, geo.ap),
    )


def gather_kernel(geo, w_hbm, x_hbm, g_hbm, z_ref, x_ref, g_ref, v_ref, buf, hb, e_ref, vs, lsem, ssem, rsem):
    q, tl = geo.q, geo.tl
    d, i, rho = geo.place()
    z, c = i // 2, i % 2
    sib = 2 * z + 1 - c
    dev = partial(geo.dev, rho=rho)
    tx = Sends(ssem, rsem)
    send = tx.send

    load = pltpu.make_async_copy(w_hbm, buf.at[pl.ds(HEAD, OWN)], lsem.at[0])
    load.start()
    rows_own = pl.ds(mult(i * tl, 16), tl)
    own = [
        pltpu.make_async_copy(x_hbm, x_ref.at[rows_own], lsem.at[1]),
        pltpu.make_async_copy(g_hbm, g_ref.at[rows_own], lsem.at[2]),
    ]
    for cp in own:
        cp.start()
    entry_barrier(geo, d, i, rho)

    halo = pl.ds(OWN - 109, 109)
    send(i < V - 1, (w_hbm, halo), (hb, pl.ds(0, 109)), 0, dev(d, (i + 1) % V))

    def chain(a, src, ref):
        dst = (ref, rows_own)
        send(None, src, dst, 2 + a, dev(d, sib))
        send(z < CHIPS - 1, src, dst, 4 + 6 * a, dev(d, (i + 2) % V))
        send(z > 0, src, dst, 7 + 6 * a, dev(d, (i + V - 2) % V))

    def hop(a, ref, k):
        for s, sign in ((0, 1), (1, -1)):
            there = (z >= k + 1) if sign == 1 else (z + k + 1 < CHIPS)
            src_i = (i - 2 * sign * (k + 1) + 2 * V) % V
            rows = pl.ds(mult(src_i * tl, 16), tl)
            rs = 4 + 6 * a + 3 * s + k
            part = (ref, rows)

            @pl.when(there)
            def _():
                arrive(part, (rsem, rs))

            send(there, part, part, 2 + a, dev(d, sib))
            if k < CHIPS - 2:
                on = (z < CHIPS - 1) if sign == 1 else (z > 0)
                send(there & on, part, part, rs + 1, dev(d, (i + 2 * sign + V) % V))

    chain(0, x_hbm, x_ref)
    load.wait()

    @pl.when(i > 0)
    def _():
        arrive((hb, pl.ds(0, 109)), (rsem, 0))
        buf[pl.ds(HEAD - 104, 104), :] = hb[pl.ds(5, 104), :]

    @pl.when(i == V - 1)
    def _():
        vs[...] = buf[pl.ds(HEAD + OWN - VECS, VECS), :].astype(BF16)
        v_ref[...] = vs[...]

    cut_share(geo, i, buf, e_ref)
    hop(0, x_ref, 0)

    for k in range(1, V):
        send(i == V - 1, vs, v_ref, 1, dev(d, (i + k) % V))

    for k in range(1, CHIPS):
        for cc in range(2):
            j = (2 * (z + k) + cc) % V
            for ok, erow, zrow, n in owner_moves(geo, i, j):
                src = (e_ref, (j, d, pl.ds(erow, n)))
                send(ok, src, (z_ref, (d, pl.ds(zrow, n))), 16 + k, dev(d, j))
        if k < CHIPS - 1:
            hop(0, x_ref, k)
    whole = slice(None)
    for ok, erow, zrow, n in owner_moves(geo, i, sib):
        src = (e_ref, (sib, whole, pl.ds(erow, n)))
        send(ok, src, (z_ref, (whole, pl.ds(zrow, n))), 16, dev(d, sib))
    for ok, erow, zrow, n in owner_moves(geo, i, i):
        tx.copy(ok, (e_ref, (i, whole, pl.ds(erow, n))), (z_ref, (whole, pl.ds(zrow, n))))

    chain(1, g_hbm, g_ref)
    seg2 = 2 * geo.seg
    for k in range(1, CHIPS):
        rows = pl.ds(mult(((z + CHIPS - k) % CHIPS) * seg2, 16), seg2)
        arrive((z_ref, (0, pl.ds(0, seg2))), (rsem, 16 + k))
        for m in range(1, q):
            send(None, (z_ref, (d, rows)), (z_ref, (d, rows)), 20 + k, dev((d + m) % q, i))
        hop(1, g_ref, k - 1)
    for cp in own:
        cp.wait()

    @pl.when(i < V - 1)
    def _():
        arrive(v_ref, (rsem, 1))

    for ref, a in ((x_ref, 0), (g_ref, 1)):
        arrive((ref, pl.ds(0, CHIPS * tl)), (rsem, 2 + a))
    sib_owner_rows(geo, sib, z_ref, (rsem, 16))
    for k in range(1, CHIPS):
        arrive((z_ref, (pl.ds(0, q - 1), pl.ds(0, seg2))), (rsem, 20 + k))
    tx.finish()


def sib_owner_rows(geo, sib, z_ref, sem):
    _, i, _ = geo.place()

    @pl.when(sib < 6)
    def _():
        arrive((z_ref, (slice(None), pl.ds(0, geo.seg))), sem)

    @pl.when((sib >= 6) & (i // 4 == sib - 6))
    def _():
        arrive((z_ref, (slice(None), pl.ds(0, 2 * geo.ap))), sem)

    @pl.when((sib >= 6) & (i // 4 != sib - 6))
    def _():
        arrive((z_ref, (slice(None), pl.ds(0, geo.ap))), sem)


def gather(geo, w, x, g):
    q = geo.q
    vm = pl.BlockSpec(memory_space=pltpu.VMEM)
    hbm = pl.BlockSpec(memory_space=pl.ANY)
    return pl.pallas_call(
        partial(gather_kernel, geo),
        out_shape=(
            jax.ShapeDtypeStruct((q, geo.zr, 128), BF16),
            jax.ShapeDtypeStruct((geo.t, D), BF16),
            jax.ShapeDtypeStruct((geo.t, D), BF16),
            jax.ShapeDtypeStruct((VECS, 128), BF16),
        ),
        in_specs=[hbm] * 3,
        out_specs=(vm,) * 4,
        scratch_shapes=[
            pltpu.VMEM((HEAD + OWN + 3, 128), F32),
            pltpu.VMEM((112, 128), F32),
            pltpu.VMEM((V, q, geo.er, 128), BF16),
            pltpu.VMEM((VECS, 128), BF16),
            pltpu.SemaphoreType.DMA((4,)),
            pltpu.SemaphoreType.DMA((80,)),
            pltpu.SemaphoreType.DMA((24,)),
        ],
        compiler_params=pltpu.CompilerParams(
            collective_id=0, has_side_effects=True, vmem_limit_bytes=60 << 20
        ),
        name="gather",
    )(w, x, g)


def rot_tables(t):
    half = ROT // 2
    freq = (10000.0 ** (-2.0 * np.arange(half, dtype=np.float32) / ROT)).astype(np.float32)
    ang = np.arange(t, dtype=np.float32)[:, None] * freq[None, :]
    cos = np.ones((t, 128), np.float32)
    sin = np.zeros((t, 128), np.float32)
    for h in range(2):
        for k in range(2):
            lo = 64 * h + half * k
            cos[:, lo : lo + half] = np.cos(ang)
            sin[:, lo : lo + half] = np.sin(ang) * (1 if k else -1)
    return jnp.asarray(cos), jnp.asarray(sin)


def rot(v, cos, sin, lane, back):
    up = pltpu.roll(v, 120, 1)
    down = pltpu.roll(v, 8, 1)
    partner = jnp.where(lane % 16 < 8, up, down)
    turn = partner * sin
    return v * cos - turn if back else v * cos + turn


def compute_kernel(
    geo, z_ref, x_ref, g_ref, v_ref, cos_ref, sin_ref, po_ref, pa_ref, gz_ref, vp_ref,
    vf, rowv, wq, wo, wu, wd, xh, n1, n2, qs, ks, vv, hid, gp, du, ob, do, dqkv, dqs, dk, dv, acc,
):
    t = geo.t
    d, j, rho = geo.place()
    mats = (wq, wo, wu, wd)
    nrb = t // RB
    for e, zrow, n, m, row, lane in geo.maps():
        mats[m][row : row + n, lane : lane + 128] = z_ref[e, zrow : zrow + n, :]
    vf[...] = v_ref[...].astype(F32)
    for k in range(9):
        for b in range(8):
            rowv[k : k + 1, 128 * b : 128 * b + 128] = vf[8 * k + b : 8 * k + b + 1, :]
    acc[...] = jnp.zeros_like(acc)
    dk[...] = jnp.zeros_like(dk)
    dv[...] = jnp.zeros_like(dv)

    def rb_of(r):
        return pl.ds(mult(r * RB, RB), RB)

    lane = lax.broadcasted_iota(jnp.int32, (RB, 128), 1)

    def forward(r, carry):
        rb = rb_of(r)
        x = x_ref[rb, :].astype(F32)
        mean = jnp.mean(x, axis=1, keepdims=True)
        mid = x - mean
        var = jnp.mean(mid * mid, axis=1, keepdims=True)
        inv = lax.rsqrt(var + 1e-05)
        xhat = mid * inv
        xh[rb, 0:1] = mean
        xh[rb, 1:2] = inv
        one = (xhat * rowv[0:1, :] + rowv[1:2, :]).astype(BF16)
        two = (xhat * rowv[2:3, :] + rowv[3:4, :]).astype(BF16)
        n1[rb, :] = one
        n2[rb, :] = two
        qkv = dot(one, wq[...])
        cos, sin = cos_ref[rb, :], sin_ref[rb, :]
        qh = qkv[:, 0:128] + vf[pl.ds(32 + j, 1), :]
        kh = qkv[:, 128:256] + vf[pl.ds(40 + j, 1), :]
        vh = qkv[:, 256:384] + vf[pl.ds(48 + j, 1), :]
        qs[rb, :] = (rot(qh, cos, sin, lane, False) * 0.125).astype(BF16)
        ks[rb, :] = rot(kh, cos, sin, lane, False).astype(BF16)
        vv[rb, :] = vh.astype(BF16)
        up = dot(two, wu[...])
        for b in range(4):
            cols = slice(128 * b, 128 * b + 128)
            u = up[:, cols] + vf[pl.ds(72 + 8 * b + j, 1), :]
            phi = 0.5 + 0.5 * lax.erf(u * (1.0 / math.sqrt(2.0)))
            hid[rb, cols] = (u * phi).astype(BF16)
            gp[rb, cols] = phi + u * (jnp.exp(-0.5 * u * u) * (1.0 / math.sqrt(2.0 * math.pi)))
        return carry

    lax.fori_loop(0, nrb, forward, 0)

    def back_mlp(r, carry):
        rb = rb_of(r)
        g = g_ref[rb, :]
        dh = dot_nt(g, wd[...])
        low = (dh * gp[rb, :]).astype(BF16)
        du[rb, :] = low
        do[rb, :] = dot_nt(g, wo[...]).astype(BF16)
        acc[4:5, :] += jnp.sum(g.astype(F32), axis=0, keepdims=True)
        acc[5:6, 0:512] += jnp.sum(low.astype(F32), axis=0, keepdims=True)
        return carry

    lax.fori_loop(0, nrb, back_mlp, 0)

    left = lax.broadcasted_iota(jnp.int32, (RB, 128), 1) < 64
    diag = lax.broadcasted_iota(jnp.int32, (RB, RB), 0) >= lax.broadcasted_iota(jnp.int32, (RB, RB), 1)
    zero = jnp.zeros((), BF16)
    for r in range(nrb):
        rb = slice(r * RB, r * RB + RB)
        n = (r + 1) * RB
        outs, dqh = [], []
        for h in range(2):
            mine = left if h == 0 else jnp.logical_not(left)
            qm = jnp.where(mine, qs[rb, :], zero)
            gm = jnp.where(mine, do[rb, :], zero)
            s = dot_nt(qm, ks[0:n, :])
            tail = jnp.where(diag, s[:, n - RB : n], -1e30)
            s = tail if r == 0 else jnp.concatenate([s[:, : n - RB], tail], axis=1)
            top = jnp.max(s, axis=1, keepdims=True)
            ex = jnp.exp(s - top)
            prob = ex * (1.0 / jnp.sum(ex, axis=1, keepdims=True))
            low = prob.astype(BF16)
            outs.append(dot(low, vv[0:n, :]))
            dp = dot_nt(gm, vv[0:n, :])
            delta = jnp.sum(prob * dp, axis=1, keepdims=True)
            ds = (prob * (dp - delta)).astype(BF16)
            dqh.append(dot(ds, ks[0:n, :]))
            dk[0:n, :] += dot_tn(ds, qm)
            dv[0:n, :] += dot_tn(low, gm)
        ob[rb, :] = jnp.where(left, outs[0], outs[1]).astype(BF16)
        dqs[rb, :] = jnp.where(left, dqh[0], dqh[1])

    def back(r, carry):
        rb = rb_of(r)
        cos, sin = cos_ref[rb, :], sin_ref[rb, :]
        po_ref[rb, :] = (dot(hid[rb, :], wd[...]) + dot(ob[rb, :], wo[...])).astype(BF16)
        low = jnp.concatenate(
            [
                (rot(dqs[rb, :], cos, sin, lane, True) * 0.125).astype(BF16),
                rot(dk[rb, :], cos, sin, lane, True).astype(BF16),
                dv[rb, :].astype(BF16),
            ],
            axis=1,
        )
        dqkv[rb, :] = low
        acc[6:7, 0:384] += jnp.sum(low.astype(F32), axis=0, keepdims=True)
        xhat = (x_ref[rb, :].astype(F32) - xh[rb, 0:1]) * xh[rb, 1:2]
        d1 = dot_nt(low, wq[...])
        acc[0:1, :] += jnp.sum(d1 * xhat, axis=0, keepdims=True)
        acc[1:2, :] += jnp.sum(d1, axis=0, keepdims=True)
        d2 = dot_nt(du[rb, :], wu[...])
        acc[2:3, :] += jnp.sum(d2 * xhat, axis=0, keepdims=True)
        acc[3:4, :] += jnp.sum(d2, axis=0, keepdims=True)
        pa_ref[rb, :] = (d1 * rowv[0:1, :] + d2 * rowv[2:3, :]).astype(BF16)
        return carry

    lax.fori_loop(0, nrb, back, 0)
    def grad_cols(left_ref, right_ref, out, blocks):
        def body(k, carry):
            cols = pl.ds(mult(k * 256, 256), 256)
            out[cols, :] = dot_tn(left_ref[:, cols], right_ref[...]).astype(BF16)
            return carry

        lax.fori_loop(0, blocks, body, 0)

    grad_cols(hid, g_ref, wd, 2)
    grad_cols(n2, du, wu, 4)
    grad_cols(n1, dqkv, wq, 4)
    wo[...] = dot_tn(ob[...], g_ref[...]).astype(BF16)
    for e, zrow, n, m, row, lane in geo.maps():
        gz_ref[e, zrow : zrow + n, :] = mats[m][row : row + n, lane : lane + 128]
    vp_ref[...] = jnp.zeros_like(vp_ref)
    first = jnp.where(j == 0, 1.0, 0.0)
    for b in range(8):
        cols = slice(128 * b, 128 * b + 128)
        for k in range(4):
            vp_ref[8 * k + b : 8 * k + b + 1, :] = acc[k : k + 1, cols]
        for k in (7, 8):
            vp_ref[8 * k + b : 8 * k + b + 1, :] = acc[4:5, cols] * first
    for k in range(3):
        vp_ref[pl.ds(32 + 8 * k + j, 1), :] = acc[6:7, 128 * k : 128 * k + 128]
    for k in range(4):
        vp_ref[pl.ds(72 + 8 * k + j, 1), :] = acc[5:6, 128 * k : 128 * k + 128]


def compute(geo, zs, x, g, v):
    q, t = geo.q, geo.t
    vm = pl.BlockSpec(memory_space=pltpu.VMEM)
    cos, sin = rot_tables(t)
    return pl.pallas_call(
        partial(compute_kernel, geo),
        out_shape=(
            jax.ShapeDtypeStruct((t, D), BF16),
            jax.ShapeDtypeStruct((t, D), BF16),
            jax.ShapeDtypeStruct((q, geo.zr, 128), BF16),
            jax.ShapeDtypeStruct((VECS, 128), F32),
        ),
        in_specs=[vm] * 6,
        out_specs=(vm,) * 4,
        scratch_shapes=[
            pltpu.VMEM((VECS, 128), F32),
            pltpu.VMEM((16, D), F32),
            pltpu.VMEM((D, 384), BF16),
            pltpu.VMEM((128, D), BF16),
            pltpu.VMEM((D, 512), BF16),
            pltpu.VMEM((512, D), BF16),
            pltpu.VMEM((t, 2), F32),
            pltpu.VMEM((t, D), BF16),
            pltpu.VMEM((t, D), BF16),
            pltpu.VMEM((t, 128), BF16),
            pltpu.VMEM((t, 128), BF16),
            pltpu.VMEM((t, 128), BF16),
            pltpu.VMEM((t, 512), BF16),
            pltpu.VMEM((t, 512), F32),
            pltpu.VMEM((t, 512), BF16),
            pltpu.VMEM((t, 128), BF16),
            pltpu.VMEM((t, 128), BF16),
            pltpu.VMEM((t, 384), BF16),
            pltpu.VMEM((t, 128), F32),
            pltpu.VMEM((t, 128), F32),
            pltpu.VMEM((t, 128), F32),
            pltpu.VMEM((8, D), F32),
        ],
        compiler_params=pltpu.CompilerParams(vmem_limit_bytes=63 << 20),
        name="compute",
    )(zs, x, g, v, cos, sin)


def scatter_kernel(
    geo, gz_ref, po_ref, pa_ref, vp_ref, v_ref, x_ref, g_ref, w_hbm, m_hbm, s_hbm,
    lo_ref, tg_ref, wg_hbm, nw_hbm, nm_hbm, ns_hbm,
    wb, mb, sb, ob, gb, hb, rz, rb, fb, sibo, siba, rcvo, rcva, vr, vsum, vq, lsem, ssem, rsem,
):
    q, tl = geo.q, geo.tl
    d, i, rho = geo.place()
    z, c = i // 2, i % 2
    sib = 2 * z + 1 - c
    dev = partial(geo.dev, rho=rho)
    tx = Sends(ssem, rsem)
    send = tx.send
    whole = slice(None)
    loads = [
        pltpu.make_async_copy(h, b.at[pl.ds(0, OWN)], lsem.at[k])
        for k, (h, b) in enumerate(((w_hbm, wb), (m_hbm, mb), (s_hbm, sb)))
    ]
    entry_barrier(geo, d, i, rho)
    for k in range(1, q):
        e = (d + k) % q
        send(None, (gz_ref, e), (rb, k - 1), 7 + k, dev(e, i))
    for a, (p, sb_) in enumerate(((po_ref, sibo), (pa_ref, siba))):
        for k in range(CHIPS):
            rows = pl.ds(mult((2 * k + 1 - c) * tl, 16), tl)
            send(None, (p, rows), (sb_, k), a, dev(d, sib))
    send(i < V - 1, vp_ref, (vr, i), 4, dev(d, V - 1))
    for ld in loads:
        ld.start()
    for a, (p, sn, rc) in enumerate(((po_ref, sibo, rcvo), (pa_ref, siba, rcva))):
        arrive(sn, (rsem, a))
        for k in range(CHIPS):
            rows = pl.ds(mult((2 * k + c) * tl, 16), tl)
            sn[k] = (p[rows, :].astype(F32) + sn[k].astype(F32)).astype(BF16)
        for k in range(1, CHIPS):
            to = (z + k) % CHIPS
            send(None, (sn, to), (rc, k - 1), 2 + a, dev(d, 2 * to + c))
    for k in range(1, q):
        arrive((rb, k - 1), (rsem, 7 + k))

    step = 256

    def add(n, carry):
        rows = pl.ds(mult(n * step, step), step)
        tot = gz_ref[d, rows, :].astype(F32)
        for k in range(q - 1):
            tot = tot + rb[k, rows, :].astype(F32)
        rz[rows, :] = tot.astype(BF16)
        return carry

    lax.fori_loop(0, geo.zr // step, add, 0)
    for k in range(V):
        o = (i + k) % V
        at = len(tx.open)
        for m, (ok, erow, zrow, n) in enumerate(owner_moves(geo, o, i)):
            src, dst = (rz, pl.ds(zrow, n)), (fb, (i, d, pl.ds(erow, n)))
            if k:
                send(ok, src, dst, 17 if m == 2 else 16, dev(d, o))
            else:
                tx.copy(ok, src, dst)
        if k == 0:
            tx.finish(at)
    @pl.when(i < 6)
    def _():
        arrive((fb, (pl.ds(0, V - 1), 0, pl.ds(0, geo.seg))), (rsem, 16))

    @pl.when(i == 6)
    def _():
        arrive((fb, (pl.ds(0, V - 1), 0, pl.ds(0, geo.ap))), (rsem, 16))
        arrive((fb, (pl.ds(0, 4), 0, pl.ds(0, geo.ap))), (rsem, 17))

    @pl.when(i == 7)
    def _():
        arrive((fb, (pl.ds(0, V - 1), 0, pl.ds(0, geo.ap))), (rsem, 16))
        arrive((fb, (pl.ds(0, 3), 0, pl.ds(0, geo.ap))), (rsem, 17))

    for k in range(1, q):
        e = (d + k) % q
        small, large = (fb, (whole, d, pl.ds(0, geo.seg))), (fb, (whole, d))
        send(i < 6, small, small, 19 + k, dev(e, i))
        send(i >= 6, large, large, 19 + k, dev(e, i))

    arrive(rcvo, (rsem, 2))
    arrive(rcva, (rsem, 3))
    vecf = lambda k: jnp.concatenate(
        [v_ref[8 * k + b : 8 * k + b + 1, :].astype(F32) for b in range(8)], axis=1
    )
    bias = vecf(7) + vecf(8)
    x = x_ref[...].astype(F32)
    so = sibo[z].astype(F32) + rcvo[0].astype(F32) + rcvo[1].astype(F32) + rcvo[2].astype(F32)
    lo_ref[...] = (x + so + bias).astype(BF16)
    sa = siba[z].astype(F32) + rcva[0].astype(F32) + rcva[1].astype(F32) + rcva[2].astype(F32)
    mid = x - jnp.mean(x, axis=1, keepdims=True)
    inv = lax.rsqrt(jnp.mean(mid * mid, axis=1, keepdims=True) + 1e-05)
    xhat = mid * inv
    dx = inv * (sa - jnp.mean(sa, axis=1, keepdims=True) - xhat * jnp.mean(sa * xhat, axis=1, keepdims=True))
    tg_ref[...] = g_ref[...].astype(F32) + dx

    @pl.when(i == V - 1)
    def _():
        arrive((vr, pl.ds(0, V - 1)), (rsem, 4))
        tot = vp_ref[...]
        for k in range(V - 1):
            tot = tot + vr[k]
        vsum[...] = tot

    for k in range(1, q):
        send(i == V - 1, vsum, (vq, k - 1), 5, dev((d + k) % q, i))

    for k in range(1, q):
        @pl.when(i < 6)
        def _():
            arrive((fb, (whole, 0, pl.ds(0, geo.seg))), (rsem, 19 + k))

        @pl.when(i >= 6)
        def _():
            arrive((fb, (whole, 0)), (rsem, 19 + k))

    paste_share(geo, i, gb, fb)

    @pl.when(i > 0)
    def _():
        hb[1] = gb[pl.ds(0, VECS), :]

    send(i > 0, (hb, 1), (hb, 0), 6, dev(d, (i + V - 1) % V))

    @pl.when(i < V - 1)
    def _():
        arrive((hb, 0), (rsem, 6))
        gb[pl.ds(ALI, VECS), :] = hb[0]

    @pl.when(i == V - 1)
    def _():
        arrive(vq, (rsem, 5))
        tot = vsum[...]
        for k in range(q - 1):
            tot = tot + vq[k]
        gb[pl.ds(ALI, VECS), :] = tot

    for ld in loads:
        ld.wait()
    rows_n = 1024
    full = OWN // rows_n
    stores = []

    def adam(n, carry):
        rows = pl.ds(mult(n * rows_n, rows_n), rows_n)
        adam_rows(i, rows, n * rows_n, rows_n, wb, mb, sb, ob, gb)
        for k, (h, b) in enumerate(((wg_hbm, ob), (nw_hbm, wb), (nm_hbm, mb), (ns_hbm, sb))):
            pltpu.make_async_copy(b.at[rows], h.at[rows], lsem.at[4 + k]).start()
        return carry

    lax.fori_loop(0, full, adam, 0)
    rest = OWN - full * rows_n
    adam_rows(i, pl.ds(full * rows_n, 16), full * rows_n, 16, wb, mb, sb, ob, gb)
    for k, (h, b) in enumerate(((wg_hbm, ob), (nw_hbm, wb), (nm_hbm, mb), (ns_hbm, sb))):
        rows = pl.ds(full * rows_n, rest)
        pltpu.make_async_copy(b.at[rows], h.at[rows], lsem.at[4 + k]).start()
    for k, (h, b) in enumerate(((wg_hbm, ob), (nw_hbm, wb), (nm_hbm, mb), (ns_hbm, sb))):
        pltpu.make_async_copy(b.at[pl.ds(0, OWN)], h, lsem.at[4 + k]).wait()
    tx.finish()


def adam_rows(i, rows, start, n, wb, mb, sb, ob, gb):
    g = gb[pl.ds(13 * i + start, n), :]
    w = wb[rows, :]
    m = BETA_ONE * mb[rows, :] + (1.0 - BETA_ONE) * g
    s = BETA_TWO * sb[rows, :] + (1.0 - BETA_TWO) * g * g
    ob[rows, :] = g
    mb[rows, :] = m
    sb[rows, :] = s
    mh = m * (1.0 / (1.0 - BETA_ONE**STEP))
    vh = s * (1.0 / (1.0 - BETA_TWO**STEP))
    wb[rows, :] = w - LEARN_RATE * (mh / (jnp.sqrt(vh) + EPSILON) + DECAY_RATE * w)


def paste_share(geo, i, gb, f_ref):
    q = geo.q

    def put(j, e, row, n, start, stride):
        gb[pl.ds(start, n, stride=stride), :] = f_ref[j, e, pl.ds(row, n), :].astype(F32)

    @pl.when(i < 2)
    def _():
        def body(n, c):
            e, s = n % q, n // q
            for b in range(8):
                put(b, e, mult(geo.qr * s, 16), geo.qr, 24 * geo.qr * e + 8 * s + b, 24)
            return c

        lax.fori_loop(0, 3 * q, body, 0)

    def rows_part(a0, ro, shift, count):
        def body(n, c):
            e, bl = n % q, n // q
            bb = bl + shift
            for b in range(8):
                put(
                    bb % V,
                    e,
                    mult(ro + geo.ap * (bb // V) + geo.ho * b, 16),
                    geo.ho,
                    a0 + 8 * (128 * bl + geo.ho * e) + b,
                    8,
                )
            return c

        lax.fori_loop(0, count * q, body, 0)

    def cols_part(a0, nr, ro):
        def body(n, c):
            e, t = n % q, n // q
            for b in range(8):
                put(b, e, mult(ro + nr * t, 16), nr, a0 + 32 * nr * e + 8 * t + b, 32)
            return c

        lax.fori_loop(0, 4 * q, body, 0)

    @pl.when(i == 2)
    def _():
        rows_part(0, 0, 0, 8)
        cols_part(8192, geo.u2, geo.ap)

    @pl.when((i == 3) | (i == 4))
    def _():
        cols_part(0, geo.u3, 0)

    @pl.when(i == 5)
    def _():
        cols_part(0, geo.u2, 0)
        rows_part(4096, geo.bp, 0, 8)

    @pl.when(i >= 6)
    def _():
        rows_part(0, 0, 4 * (i - 6), 12)


def scatter(geo, gz, po, pa, vp, v, x, g, w, m, s):
    q, tl = geo.q, geo.tl
    vm = pl.BlockSpec(memory_space=pltpu.VMEM)
    hbm = pl.BlockSpec(memory_space=pl.ANY)
    flat = jax.ShapeDtypeStruct((OWN, 128), F32)
    big = pltpu.VMEM((OWN + 3, 128), F32)
    line = pltpu.VMEM((CHIPS, tl, D), BF16)
    line3 = pltpu.VMEM((CHIPS - 1, tl, D), BF16)
    return pl.pallas_call(
        partial(scatter_kernel, geo),
        out_shape=(
            jax.ShapeDtypeStruct((tl, D), BF16),
            jax.ShapeDtypeStruct((tl, D), F32),
            flat, flat, flat, flat,
        ),
        in_specs=[vm] * 7 + [hbm] * 3,
        out_specs=(vm, vm, hbm, hbm, hbm, hbm),
        scratch_shapes=[
            big, big, big, big,
            pltpu.VMEM((ALI + 128, 128), F32),
            pltpu.VMEM((2, VECS, 128), F32),
            pltpu.VMEM((geo.zr, 128), BF16),
            pltpu.VMEM((q - 1, geo.zr, 128), BF16),
            pltpu.VMEM((V, q, geo.er, 128), BF16),
            line, line, line3, line3,
            pltpu.VMEM((V - 1, VECS, 128), F32),
            pltpu.VMEM((VECS, 128), F32),
            pltpu.VMEM((q - 1, VECS, 128), F32),
            pltpu.SemaphoreType.DMA((8,)),
            pltpu.SemaphoreType.DMA((80,)),
            pltpu.SemaphoreType.DMA((32,)),
        ],
        compiler_params=pltpu.CompilerParams(
            collective_id=1, has_side_effects=True, vmem_limit_bytes=63 << 20
        ),
        name="scatter",
    )(gz, po, pa, vp, v, x, g, w, m, s)


def local(mesh, tokens, cotangent, weights, first_moment, second_moment):
    rep = mesh.shape["ctx"] // V
    rows = tokens.shape[1]
    x, g = tokens[0], cotangent[0]
    flats = [weights, first_moment, second_moment]
    if rep > 1:
        groups = [[rep * k + r for r in range(rep)] for k in range(V)]
        join = lambda a: lax.all_gather(a, "ctx", axis=0, axis_index_groups=groups, tiled=True)
        x, g = join(x), join(g)
        flats = [join(a) for a in flats]
    w, m, s = [a.reshape(OWN, 128) for a in flats]
    geo = Geo(mesh, x.shape[0] * V)
    zs, xs, gs, v = gather(geo, w, x, g)
    po, pa, gz, vp = compute(geo, zs, xs, gs, v)
    outs = list(scatter(geo, gz, po, pa, vp, v, x, g, w, m, s))
    outs[2:] = [a.reshape(-1) for a in outs[2:]]
    if rep > 1:
        r = lax.axis_index("ctx") % rep
        outs = [lax.dynamic_slice_in_dim(a, r * (a.shape[0] // rep), a.shape[0] // rep, 0) for a in outs]
    return (outs[0][None], outs[1][None], *outs[2:])


def solution(mesh):
    return jax.shard_map(
        partial(local, mesh),
        mesh=mesh,
        in_specs=(P("dp", "ctx", None), P("dp", "ctx", None), P("ctx"), P("ctx"), P("ctx")),
        out_specs=(P("dp", "ctx", None), P("dp", "ctx", None), P("ctx"), P("ctx"), P("ctx"), P("ctx")),
        check_vma=False,
    )
```

```python
from functools import partial
import math

import numpy as np
import jax
import jax.numpy as jnp
from jax import lax
from jax.experimental import pallas as pl
from jax.experimental.pallas import tpu as pltpu
from jax.sharding import PartitionSpec as P

D = 1024
FF = 4096
HEADS = 16
HEAD_DIM = 64
ROT = 16
STEP = 3
BETA_ONE = 0.9
BETA_TWO = 0.95
LEARN_RATE = 0.004
DECAY_RATE = 0.1
EPSILON = 1e-08

F32 = jnp.float32
BF16 = jnp.bfloat16
MESH = pl.DeviceIdType.MESH
V = 8
CHIPS = V // 2
OWN = 12301
ALI = 12288
VECS = 104
HEAD = 112
RB = 256
SPREAD = 31
SUMS = 80


class Geo:
    def __init__(self, mesh, tokens):
        self.q = mesh.shape["dp"]
        self.rep = mesh.shape["ctx"] // V
        self.tl = tokens // V
        self.t = tokens
        q = self.q
        self.qr = 512 // q
        self.ho = 128 // q
        self.u2 = 128 // q
        self.u3 = 384 // q
        self.seg = 1536 // q
        self.zr = V * self.seg
        self.ap = 1024 // q
        self.bp = 512 // q
        self.er = 2 * self.ap
        self.tight = tokens > 1024
        self.rba = RB // 2 if self.tight else RB
        self.square = q == 4
        self.ss = max(4, q - 1)

    def place(self):
        d = lax.axis_index("dp")
        a = lax.axis_index("ctx")
        return d, a // self.rep, a % self.rep

    def dev(self, e, j, rho):
        return {"dp": e, "ctx": j * self.rep + rho}

    def maps(self):
        q, out = self.q, []
        for e in range(q):
            for i in range(2):
                for s in range(3):
                    out.append((e, self.seg * i + self.qr * s, self.qr, 0, 512 * i + self.qr * e, 128 * s))
            for b in range(8):
                out.append((e, 2 * self.seg + self.ho * b, self.ho, 1, self.ho * e, 128 * b))
            parts = (
                (0, self.u2, 2 * self.seg + self.ap),
                (128, self.u3, 3 * self.seg),
                (512, self.u3, 4 * self.seg),
                (896, self.u2, 5 * self.seg),
            )
            for r0, nr, off in parts:
                for t in range(4):
                    out.append((e, off + nr * t, nr, 2, r0 + nr * e, 128 * t))
            for t in range(4):
                for b in range(8):
                    row = 5 * self.seg + self.bp + self.ap * t + self.ho * b
                    out.append((e, row, self.ho, 3, 128 * t + self.ho * e, 128 * b))
        return out


def dot(a, b):
    return jnp.dot(a, b, preferred_element_type=F32)


def dot_nt(a, b):
    return lax.dot_general(a, b, (((1,), (1,)), ((), ())), preferred_element_type=F32)


def dot_tn(a, b):
    return lax.dot_general(a, b, (((0,), (0,)), ((), ())), preferred_element_type=F32)


def mult(x, n):
    return pl.multiple_of(x, n)


def view(part):
    return part[0].at[part[1]] if isinstance(part, tuple) else part


def rcopy(src, dst, ssem, rsem, dev):
    return pltpu.make_async_remote_copy(
        src_ref=view(src),
        dst_ref=view(dst),
        send_sem=view(ssem),
        recv_sem=view(rsem),
        device_id=dev,
        device_id_type=MESH,
    )


class Sends:
    def __init__(self, ssem, rsem, used=None):
        self.ssem, self.rsem, self.used, self.open = ssem, rsem, used or [0], []

    def group(self):
        return Sends(self.ssem, self.rsem, self.used)

    def slot(self):
        self.used[0] += 1
        return (self.ssem, self.used[0] - 1)

    def send(self, cond, src, dst, rs, dev):
        slot = self.slot()
        make = lambda: rcopy(src, dst, slot, (self.rsem, rs), dev)
        self.when(cond, lambda: make().start())
        self.open.append((cond, lambda: make().wait_send()))

    def copy(self, cond, src, dst):
        slot = self.slot()
        make = lambda: pltpu.make_async_copy(view(src), view(dst), view(slot))
        self.when(cond, lambda: make().start())
        self.open.append((cond, lambda: make().wait()))

    @staticmethod
    def when(cond, act):
        if cond is None:
            act()
        else:
            pl.when(cond)(act)

    def finish(self):
        for cond, act in self.open:
            self.when(cond, act)
        self.open.clear()


def arrive(part, sem):
    pltpu.make_async_copy(view(part), view(part), view(sem)).wait()


def entry_barrier(geo, d, i, rho):
    sem = pltpu.get_barrier_semaphore()
    for k in range(1, V):
        pl.semaphore_signal(sem, inc=1, device_id=geo.dev(d, (i + k) % V, rho), device_id_type=MESH)
    for k in range(1, geo.q):
        pl.semaphore_signal(sem, inc=1, device_id=geo.dev((d + k) % geo.q, i, rho), device_id_type=MESH)
    pl.semaphore_wait(sem, V - 1 + geo.q - 1)


def cut_share(geo, i, buf, e_ref):
    q, base = geo.q, HEAD - 13 * i

    def put(j, e, row, n, start, stride):
        e_ref[j, e, pl.ds(row, n), :] = buf[pl.ds(start, n, stride=stride), :].astype(BF16)

    @pl.when(i < 2)
    def _():
        def body(n, c):
            e, s = n % q, n // q
            for b in range(8):
                put(b, e, mult(geo.qr * s, 16), geo.qr, base + 24 * geo.qr * e + 8 * s + b, 24)
            return c

        lax.fori_loop(0, 3 * q, body, 0)

    def rows_part(a0, ro, shift, count):
        def body(n, c):
            e, bl = n % q, n // q
            bb = bl + shift
            for b in range(8):
                put(
                    bb % V,
                    e,
                    mult(ro + geo.ap * (bb // V) + geo.ho * b, 16),
                    geo.ho,
                    base + a0 + 8 * (128 * bl + geo.ho * e) + b,
                    8,
                )
            return c

        lax.fori_loop(0, count * q, body, 0)

    def cols_part(a0, nr, ro):
        def body(n, c):
            e, t = n % q, n // q
            for b in range(8):
                put(b, e, mult(ro + nr * t, 16), nr, base + a0 + 32 * nr * e + 8 * t + b, 32)
            return c

        lax.fori_loop(0, 4 * q, body, 0)

    @pl.when(i == 2)
    def _():
        rows_part(0, 0, 0, 8)
        cols_part(8192, geo.u2, geo.ap)

    @pl.when((i == 3) | (i == 4))
    def _():
        cols_part(0, geo.u3, 0)

    @pl.when(i == 5)
    def _():
        cols_part(0, geo.u2, 0)
        rows_part(4096, geo.bp, 0, 8)

    @pl.when(i >= 6)
    def _():
        rows_part(0, 0, 4 * (i - 6), 12)


def owner_moves(geo, i, j):
    k = i - 6
    return (
        (i < 6, 0, mult(geo.seg * i, 16), geo.seg),
        (i >= 6, mult(geo.ap * k, 16), mult(6 * geo.seg + 2 * geo.ap * k, 16), geo.ap),
        ((i >= 6) & (j // 4 == k), mult(geo.ap * (1 - k), 16), 6 * geo.seg + geo.ap, geo.ap),
    )


def sib_owner_rows(geo, sib, z_ref, sem):
    _, i, _ = geo.place()

    @pl.when(sib < 6)
    def _():
        arrive((z_ref, (slice(None), pl.ds(0, geo.seg))), sem)

    @pl.when((sib >= 6) & (i // 4 == sib - 6))
    def _():
        arrive((z_ref, (slice(None), pl.ds(0, 2 * geo.ap))), sem)

    @pl.when((sib >= 6) & (i // 4 != sib - 6))
    def _():
        arrive((z_ref, (slice(None), pl.ds(0, geo.ap))), sem)


def rot_tables(t):
    half = ROT // 2
    freq = (10000.0 ** (-2.0 * np.arange(half, dtype=np.float32) / ROT)).astype(np.float32)
    ang = np.arange(t, dtype=np.float32)[:, None] * freq[None, :]
    cos = np.ones((t, 128), np.float32)
    sin = np.zeros((t, 128), np.float32)
    for h in range(2):
        for k in range(2):
            lo = 64 * h + half * k
            cos[:, lo : lo + half] = np.cos(ang)
            sin[:, lo : lo + half] = np.sin(ang) * (1 if k else -1)
    return jnp.asarray(cos), jnp.asarray(sin)


def rot(v, cos, sin, lane, back):
    up = pltpu.roll(v, 120, 1)
    down = pltpu.roll(v, 8, 1)
    partner = jnp.where(lane % 16 < 8, up, down)
    turn = partner * sin
    return v * cos - turn if back else v * cos + turn


def main_kernel(
    geo, w_hbm, xin, gin, cos_ref, sin_ref, so_ref, sa_ref, f_hbm, tail_ref,
    buf, hb, e_ref, vs, z_ref, x_ref, g_ref, v_ref,
    vf, rowv, wq, wo, wu, wd, xh, n1, n2, qs, ks, vv, hid, du, ob, do, dqkv, dqs, acc, vp_ref, lse,
    rb_ref, rz, sibo, siba, rcvo, rcva, vr, vq, vsum, hbuf, lsem, ssem, rsem, csem, *spare,
):
    gz_ref = z_ref
    po_ref, fb = (g_ref, e_ref) if geo.tight else spare
    q, tl, t = geo.q, geo.tl, geo.t
    seg, ap, bp = geo.seg, geo.ap, geo.bp
    d, i, rho = geo.place()
    j = i
    z, c = i // 2, i % 2
    sib = 2 * z + 1 - c
    near = (None, d - d % 2 + (1 - d % 2), (d + 2) % 4, 3 - d)
    dev = partial(geo.dev, rho=rho)
    early = Sends(ssem, rsem)
    tx = early.group()
    lc = Sends(csem, None)
    whole = slice(None)

    def spread_one(tx, ok, part, sem):
        if geo.square:
            for k in (1, 2):
                tx.send(ok, part(d, None), part(d, None), sem + k - 1, dev(near[k], i))
        else:
            for k in range(1, q):
                tx.send(ok, part(d, None), part(d, None), sem + k - 1, dev((d + k) % q, i))

    def spread_two(tx, ok, part, sem):
        if geo.square:
            for k in (1, 2):
                Sends.when(ok, lambda: arrive(part(near[k], None), (rsem, sem + k - 1)))
                half = part(near[k], k - 1)
                tx.send(ok, half, half, sem + 1 + k, dev(near[3 - k], i))

    def spread_three(ok, part, sem):
        if geo.square:
            for k in (1, 2):
                Sends.when(ok, lambda: arrive(part(near[3], k - 1), (rsem, sem + 1 + k)))
        else:
            for k in range(1, q):
                Sends.when(ok, lambda: arrive(part((d + q - k) % q, None), (rsem, sem + k - 1)))

    load = pltpu.make_async_copy(w_hbm, buf.at[pl.ds(HEAD, OWN)], lsem.at[0])
    load.start()
    rows_own = pl.ds(mult(i * tl, 16), tl)
    own = [
        pltpu.make_async_copy(xin, x_ref.at[rows_own], lsem.at[1]),
        pltpu.make_async_copy(gin, g_ref.at[rows_own], lsem.at[2]),
    ]
    for cp in own:
        cp.start()
    entry_barrier(geo, d, i, rho)
    halo = pl.ds(OWN - 109, 109)
    early.send(i < V - 1, (w_hbm, halo), (hb, pl.ds(0, 109)), 0, dev(d, (i + 1) % V))

    def chain(a, src, ref):
        dst = (ref, rows_own)
        early.send(z < CHIPS - 1, src, dst, 4 + 6 * a, dev(d, (i + 2) % V))
        early.send(z > 0, src, dst, 7 + 6 * a, dev(d, (i + V - 2) % V))
        early.send(None, src, dst, 2 + a, dev(d, sib))

    def hop(a, ref, k):
        for s, sign in ((0, 1), (1, -1)):
            there = (z >= k + 1) if sign == 1 else (z + k + 1 < CHIPS)
            src_i = (i - 2 * sign * (k + 1) + 2 * V) % V
            rows = pl.ds(mult(src_i * tl, 16), tl)
            rs = 4 + 6 * a + 3 * s + k
            part = (ref, rows)

            @pl.when(there)
            def _():
                arrive(part, (rsem, rs))

            if k < CHIPS - 2:
                on = (z < CHIPS - 1) if sign == 1 else (z > 0)
                early.send(there & on, part, part, rs + 1, dev(d, (i + 2 * sign + V) % V))
            early.send(there, part, part, 2 + a, dev(d, sib))

    chain(0, xin, x_ref)
    load.wait()

    @pl.when(i > 0)
    def _():
        arrive((hb, pl.ds(0, 109)), (rsem, 0))
        buf[pl.ds(HEAD - 104, 104), :] = hb[pl.ds(5, 104), :]

    @pl.when(i == V - 1)
    def _():
        vs[...] = buf[pl.ds(HEAD + OWN - VECS, VECS), :].astype(BF16)
        v_ref[...] = vs[...]

    cut_share(geo, i, buf, e_ref)

    def slices_to(k):
        tx = early.group()
        for cc in range(2):
            to = (2 * (z + k) + cc) % V
            for ok, erow, zrow, n in owner_moves(geo, i, to):
                src = (e_ref, (to, d, pl.ds(erow, n)))
                tx.send(ok, src, (z_ref, (d, pl.ds(zrow, n))), 16 + k, dev(d, to))
        return tx

    def slices_of(k):
        base = ((z + CHIPS - k) % CHIPS) * 2 * seg

        def part(e, half):
            at, n = (base, 2 * seg) if half is None else (base + half * seg, seg)
            return (z_ref, (e, pl.ds(mult(at, 16), n)))

        return None, part, SPREAD + geo.ss * (k - 1)

    first = slices_to(1)
    for k in range(1, V):
        early.send(i == V - 1, vs, v_ref, 1, dev(d, (i + k) % V))
    for ok, erow, zrow, n in owner_moves(geo, i, sib):
        src = (e_ref, (sib, whole, pl.ds(erow, n)))
        early.send(ok, src, (z_ref, (whole, pl.ds(zrow, n))), 16, dev(d, sib))
    for ok, erow, zrow, n in owner_moves(geo, i, i):
        lc.copy(ok, (e_ref, (i, whole, pl.ds(erow, n))), (z_ref, (whole, pl.ds(zrow, n))))
    first.finish()
    second = slices_to(2)
    arrive((z_ref, (0, pl.ds(0, 2 * seg))), (rsem, 17))
    spread_one(early, *slices_of(1))
    second.finish()
    third = slices_to(3)
    arrive((z_ref, (0, pl.ds(0, 2 * seg))), (rsem, 18))
    spread_one(early, *slices_of(2))
    third.finish()
    hop(0, x_ref, 0)
    arrive((z_ref, (0, pl.ds(0, 2 * seg))), (rsem, 19))
    spread_one(early, *slices_of(3))
    spread_two(early, *slices_of(1))
    hop(0, x_ref, 1)
    chain(1, gin, g_ref)
    spread_two(early, *slices_of(2))
    hop(0, x_ref, 2)
    for cp in own:
        cp.wait()

    @pl.when(i < V - 1)
    def _():
        arrive(v_ref, (rsem, 1))

    nrb = t // RB
    vf[...] = v_ref[...].astype(F32)
    for k in range(9):
        for b in range(8):
            rowv[k : k + 1, 128 * b : 128 * b + 128] = vf[8 * k + b : 8 * k + b + 1, :]
    acc[...] = jnp.zeros_like(acc)
    vp_ref[...] = jnp.zeros_like(vp_ref)
    gp = lambda b, r: pl.ds(mult(b * t + r * RB, RB), RB)
    kv0, kv1 = 4 * t, 5 * t
    buf[kv0 : kv0 + 2 * t, :] = jnp.zeros((2 * t, 128), F32)

    def rb_of(r):
        return pl.ds(mult(r * RB, RB), RB)

    lane = lax.broadcasted_iota(jnp.int32, (RB, 128), 1)
    arrive((x_ref, pl.ds(0, CHIPS * tl)), (rsem, 2))

    def norms(r, carry):
        rb = rb_of(r)
        x = x_ref[rb, :].astype(F32)
        mean = jnp.mean(x, axis=1, keepdims=True)
        mid = x - mean
        var = jnp.mean(mid * mid, axis=1, keepdims=True)
        inv = lax.rsqrt(var + 1e-05)
        xhat = mid * inv
        xh[rb, 0:1] = mean
        xh[rb, 1:2] = inv
        n1[rb, :] = (xhat * rowv[0:1, :] + rowv[1:2, :]).astype(BF16)
        n2[rb, :] = (xhat * rowv[2:3, :] + rowv[3:4, :]).astype(BF16)
        return carry

    lax.fori_loop(0, nrb, norms, 0)
    spread_two(early, *slices_of(3))
    hop(1, g_ref, 0)
    sib_owner_rows(geo, sib, z_ref, (rsem, 16))
    lc.finish()
    for k in range(1, CHIPS):
        spread_three(*slices_of(k))
    mats = (wq, wo, wu, wd)
    for e, zrow, n, m, row, ln in geo.maps():
        mats[m][row : row + n, ln : ln + 128] = z_ref[e, zrow : zrow + n, :]
    hop(1, g_ref, 1)

    def forward(r, carry):
        rb = rb_of(r)
        qkv = dot(n1[rb, :], wq[...])
        cos, sin = cos_ref[rb, :], sin_ref[rb, :]
        qh = qkv[:, 0:128] + vf[pl.ds(32 + j, 1), :]
        kh = qkv[:, 128:256] + vf[pl.ds(40 + j, 1), :]
        vh = qkv[:, 256:384] + vf[pl.ds(48 + j, 1), :]
        qs[rb, :] = (rot(qh, cos, sin, lane, False) * 0.125).astype(BF16)
        ks[rb, :] = rot(kh, cos, sin, lane, False).astype(BF16)
        vv[rb, :] = vh.astype(BF16)
        up = dot(n2[rb, :], wu[...])
        for b in range(4):
            cols = slice(128 * b, 128 * b + 128)
            u = up[:, cols] + vf[pl.ds(72 + 8 * b + j, 1), :]
            phi = 0.5 + 0.5 * lax.erf(u * (1.0 / math.sqrt(2.0)))
            hid[rb, cols] = (u * phi).astype(BF16)
            buf[gp(b, r), :] = phi + u * (jnp.exp(-0.5 * u * u) * (1.0 / math.sqrt(2.0 * math.pi)))
        return carry

    lax.fori_loop(0, nrb, forward, 0)
    hop(1, g_ref, 2)

    ra = geo.rba
    left = lax.broadcasted_iota(jnp.int32, (ra, 128), 1) < 64
    diag = lax.broadcasted_iota(jnp.int32, (ra, ra), 0) >= lax.broadcasted_iota(jnp.int32, (ra, ra), 1)
    zero = jnp.zeros((), BF16)

    def mine(h, v):
        return jnp.where(left if h == 0 else jnp.logical_not(left), v, zero)

    def scores(r, qm):
        n = (r + 1) * ra
        s = dot_nt(qm, ks[0:n, :])
        tail = jnp.where(diag, s[:, n - ra : n], -1e30)
        return tail if r == 0 else jnp.concatenate([s[:, : n - ra], tail], axis=1)

    for r in range(t // ra):
        rb, n = slice(r * ra, r * ra + ra), (r + 1) * ra
        outs = []
        for h in range(2):
            s = scores(r, mine(h, qs[rb, :]))
            top = jnp.max(s, axis=1, keepdims=True)
            ex = jnp.exp(s - top)
            tot = jnp.sum(ex, axis=1, keepdims=True)
            lse[rb, h : h + 1] = top + jnp.log(tot)
            outs.append(dot((ex * (1.0 / tot)).astype(BF16), vv[0:n, :]))
        ob[rb, :] = jnp.where(left, outs[0], outs[1]).astype(BF16)

    def outputs(r, carry):
        rb = rb_of(r)
        po_ref[rb, :] = (dot(hid[rb, :], wd[...]) + dot(ob[rb, :], wo[...])).astype(BF16)
        return carry

    def to_sibling(a, part, sums):
        for k in range(CHIPS):
            rows = pl.ds(mult((2 * k + 1 - c) * tl, 16), tl)
            tx.send(None, (part, rows), (sums, k), 20 + a, dev(d, sib))

    def to_line(a, part, sums, got):
        arrive(sums, (rsem, 20 + a))
        for k in range(CHIPS):
            rows = pl.ds(mult((2 * k + c) * tl, 16), tl)
            sums[k] = (part[rows, :].astype(F32) + sums[k].astype(F32)).astype(BF16)
        for k in range(1, CHIPS):
            to = (z + k) % CHIPS
            tx.send(None, (sums, to), (got, k - 1), 22 + a, dev(d, 2 * to + c))

    if not geo.tight:
        lax.fori_loop(0, nrb, outputs, 0)
        to_sibling(0, po_ref, sibo)
    arrive((g_ref, pl.ds(0, CHIPS * tl)), (rsem, 3))

    def back_mlp(r, carry):
        rb = rb_of(r)
        g = g_ref[rb, :]
        dh = dot_nt(g, wd[...])
        for b in range(4):
            cols = slice(128 * b, 128 * b + 128)
            low = (dh[:, cols] * buf[gp(b, r), :]).astype(BF16)
            du[rb, cols] = low
            acc[5:6, cols] += jnp.sum(low.astype(F32), axis=0, keepdims=True)
        do[rb, :] = dot_nt(g, wo[...]).astype(BF16)
        acc[4:5, :] += jnp.sum(g.astype(F32), axis=0, keepdims=True)
        return carry

    lax.fori_loop(0, nrb, back_mlp, 0)
    early.finish()
    pc = 4096 // q
    ph = pc // 2

    def grad_down(k, carry):
        res = dot_tn(hid[:, pl.ds(mult(k * 256, 256), 256)], g_ref[...]).astype(BF16)
        for h in range(2):
            row = 5 * seg + bp + ap * (2 * k + h)
            for e in range(q):
                for b in range(8):
                    r0 = 128 * h + geo.ho * e
                    block = res[r0 : r0 + geo.ho, 128 * b : 128 * b + 128]
                    gz_ref[e, pl.ds(mult(row + geo.ho * b, 16), geo.ho), :] = block
        return carry

    def grad_cols(left_ref, right_ref, out, blocks):
        def body(k, carry):
            cols = pl.ds(mult(k * 256, 256), 256)
            out[cols, :] = dot_tn(left_ref[:, cols], right_ref[...]).astype(BF16)
            return carry

        lax.fori_loop(0, blocks, body, 0)

    def pack(which):
        for e, zrow, n, m, row, ln in geo.maps():
            if m in which:
                gz_ref[e, zrow : zrow + n, :] = mats[m][row : row + n, ln : ln + 128]

    def halves(p, h):
        return pl.ds(p * pc + h * ph, ph), pl.ds(p * ph, ph)

    def sum_one(p):
        sem = SUMS + geo.ss * p
        if geo.square:
            for k in (1, 2):
                rows, at = halves(p, k - 1)
                for slot, e in enumerate((near[k], near[3])):
                    dst = (rb_ref, (2 * (k - 1) + slot, at))
                    tx.send(None, (gz_ref, (e, rows)), dst, sem + k - 1, dev(near[k], i))
        else:
            rows = pl.ds(p * pc, pc)
            for k in range(1, q):
                e = (d + k) % q
                tx.send(None, (gz_ref, (e, rows)), (rb_ref, (k - 1, rows)), sem + k - 1, dev(e, i))

    def sum_two(p):
        sem = SUMS + geo.ss * p
        if geo.square:
            for k in (1, 2):
                rows, at = halves(p, k - 1)
                arrive((rb_ref, (pl.ds(2 * (k - 1), 2), at)), (rsem, sem + k - 1))
                mid = 2 * (k - 1) + 1
                tot = gz_ref[near[3 - k], rows, :].astype(F32) + rb_ref[mid, at, :].astype(F32)
                rb_ref[mid, at, :] = tot.astype(BF16)
                tx.send(None, (rb_ref, (mid, at)), (rb_ref, (3 + k, at)), sem + 1 + k, dev(near[3 - k], i))

    def sum_three(p):
        sem = SUMS + geo.ss * p
        if geo.square:
            for k in (1, 2):
                rows, at = halves(p, k - 1)
                arrive((rb_ref, (3 + k, at)), (rsem, sem + 1 + k))
                tot = gz_ref[d, rows, :].astype(F32) + rb_ref[2 * (k - 1), at, :].astype(F32)
                rz[rows, :] = (tot + rb_ref[3 + k, at, :].astype(F32)).astype(BF16)
        else:
            rows = pl.ds(p * pc, pc)
            for k in range(1, q):
                arrive((rb_ref, (k - 1, rows)), (rsem, sem + k - 1))
            tot = gz_ref[d, rows, :].astype(F32)
            for k in range(q - 1):
                tot = tot + rb_ref[k, rows, :].astype(F32)
            rz[rows, :] = tot.astype(BF16)

    moves = (
        ((0, 0, 0, seg, 0), (1, seg, 0, seg, 0), (2, 2 * seg, 0, ap, 0)),
        (
            (2, 2 * seg + ap, ap, bp, 1),
            (3, 3 * seg, 0, seg, 1),
            (4, 4 * seg, 0, seg, 1),
            (5, 5 * seg, 0, bp, 1),
        ),
        ((5, 5 * seg + bp, bp, ap, 2), (6, 6 * seg, 0, ap, 2), (7, 6 * seg + 2 * ap, ap, ap, 2)),
    )

    def to_owners(p):
        sum_three(p)
        for o, zrow, frow, n, kind in moves[p]:
            src, dst = (rz, pl.ds(zrow, n)), (fb, (i, d, pl.ds(frow, n)))
            tx.send(i != o, src, dst, 27 + kind, dev(d, o))
            lc.copy(i == o, src, dst)
        if p == 2:
            for o in (6, 7):
                here = i // 4 == o - 6
                src, dst = (rz, pl.ds(6 * seg + ap, ap)), (fb, (i, d, pl.ds(ap * (7 - o), ap)))
                tx.send(here & (i != o), src, dst, 30, dev(d, o))
                lc.copy(here & (i == o), src, dst)

    def held(p):
        out = [(o, 0, V, V - 1, frow, n, kind) for o, _, frow, n, kind in moves[p]]
        if p == 2:
            out += [(6, 0, 4, 4, ap, ap, 3), (7, 4, 4, 3, 0, ap, 3)]
        return out

    def held_part(j0, js, frow, n):
        def part(e, half):
            at, m = (j0, js) if half is None else (j0 + half * (js // 2), js // 2)
            return (fb, (pl.ds(at, m), e, pl.ds(frow, n)))

        return part

    def plane(p, stage):
        if stage == 1:
            lc.finish()
        for o, j0, js, remote, frow, n, kind in held(p):
            ok, part, sem = i == o, held_part(j0, js, frow, n), SPREAD + geo.ss * (3 + kind)
            if stage == 1:
                Sends.when(ok, lambda: arrive((fb, (pl.ds(0, remote), 0, pl.ds(frow, n))), (rsem, 27 + kind)))
                spread_one(tx, ok, part, sem)
            elif stage == 2:
                spread_two(tx, ok, part, sem)
            else:
                spread_three(ok, part, sem)

    lax.fori_loop(0, 2, grad_down, 0)
    sum_one(2)
    if not geo.tight:
        to_line(0, po_ref, sibo, rcvo)

    for r in range(t // ra):
        rb, n = slice(r * ra, r * ra + ra), (r + 1) * ra
        dqh = []
        for h in range(2):
            qm, gm = mine(h, qs[rb, :]), mine(h, do[rb, :])
            prob = jnp.exp(scores(r, qm) - lse[rb, h : h + 1])
            dp = dot_nt(gm, vv[0:n, :])
            delta = jnp.sum(prob * dp, axis=1, keepdims=True)
            ds = (prob * (dp - delta)).astype(BF16)
            dqh.append(dot(ds, ks[0:n, :]))
            buf[kv0 : kv0 + n, :] += dot_tn(ds, qm)
            buf[kv1 : kv1 + n, :] += dot_tn(prob.astype(BF16), gm)
        dqs[rb, :] = jnp.where(left, dqh[0], dqh[1])

    sum_two(2)

    def back(r, carry):
        rb = rb_of(r)
        cos, sin = cos_ref[rb, :], sin_ref[rb, :]
        low = jnp.concatenate(
            [
                (rot(dqs[rb, :], cos, sin, lane, True) * 0.125).astype(BF16),
                rot(buf[pl.ds(mult(kv0 + r * RB, RB), RB), :], cos, sin, lane, True).astype(BF16),
                buf[pl.ds(mult(kv1 + r * RB, RB), RB), :].astype(BF16),
            ],
            axis=1,
        )
        dqkv[rb, :] = low
        acc[6:7, 0:384] += jnp.sum(low.astype(F32), axis=0, keepdims=True)
        xhat = (x_ref[rb, :].astype(F32) - xh[rb, 0:1]) * xh[rb, 1:2]
        d1 = dot_nt(low, wq[...])
        acc[0:1, :] += jnp.sum(d1 * xhat, axis=0, keepdims=True)
        acc[1:2, :] += jnp.sum(d1, axis=0, keepdims=True)
        d2 = dot_nt(du[rb, :], wu[...])
        acc[2:3, :] += jnp.sum(d2 * xhat, axis=0, keepdims=True)
        acc[3:4, :] += jnp.sum(d2, axis=0, keepdims=True)
        x_ref[rb, :] = (d1 * rowv[0:1, :] + d2 * rowv[2:3, :]).astype(BF16)
        return carry

    lax.fori_loop(0, nrb, back, 0)
    to_sibling(1, x_ref, siba)
    res = dot_tn(ob[...], g_ref[...]).astype(BF16)
    for e in range(q):
        for b in range(8):
            row = 2 * seg + geo.ho * b
            gz_ref[e, row : row + geo.ho, :] = res[geo.ho * e : geo.ho * e + geo.ho, 128 * b : 128 * b + 128]
    if geo.tight:
        lax.fori_loop(0, nrb, outputs, 0)
        to_sibling(0, po_ref, sibo)
    grad_cols(n1, dqkv, wq, 4)
    pack((0,))
    sum_one(0)
    to_owners(2)
    grad_cols(n2, du, wu, 4)
    pack((2,))
    sum_one(1)
    sum_two(0)
    if geo.tight:
        to_line(0, po_ref, sibo, rcvo)
    to_line(1, x_ref, siba, rcva)
    plane(2, 1)
    zeroth = jnp.where(j == 0, 1.0, 0.0)
    for b in range(8):
        cols = slice(128 * b, 128 * b + 128)
        for k in range(4):
            vp_ref[8 * k + b : 8 * k + b + 1, :] = acc[k : k + 1, cols]
        for k in (7, 8):
            vp_ref[8 * k + b : 8 * k + b + 1, :] = acc[4:5, cols] * zeroth
    for k in range(3):
        vp_ref[pl.ds(32 + 8 * k + j, 1), :] = acc[6:7, 128 * k : 128 * k + 128]
    for k in range(4):
        vp_ref[pl.ds(72 + 8 * k + j, 1), :] = acc[5:6, 128 * k : 128 * k + 128]
    tx.send(i < V - 1, vp_ref, (vr, i), 24, dev(d, V - 1))
    to_owners(0)
    sum_two(1)
    plane(2, 2)
    plane(0, 1)
    to_owners(1)
    plane(0, 2)
    plane(1, 1)
    for a, (sums, got, out) in enumerate(((sibo, rcvo, so_ref), (siba, rcva, sa_ref))):
        arrive(got, (rsem, 22 + a))
        tot = sums[z].astype(F32)
        for k in range(CHIPS - 1):
            tot = tot + got[k].astype(F32)
        if a == 0:
            tot = tot + (rowv[7:8, :] + rowv[8:9, :])
        out[...] = tot

    def head_rows(jj, row, n, stride, s):
        for b in range(8):
            at = row if jj is None else row + n * b
            src = fb[b if jj is None else jj, 0, at : at + 16, :]
            hbuf[pl.ds(8 * s + b, 16, stride=stride), :] = src.astype(F32)

    @pl.when((d == 0) & (i == 1))
    def _():
        for s in range(3):
            head_rows(None, geo.qr * s, geo.qr, 24, s)

    for o, n in ((3, geo.u3), (4, geo.u3), (5, geo.u2)):
        @pl.when((d == 0) & (i == o))
        def _():
            for s in range(4):
                head_rows(None, n * s, n, 32, s)

    for o, jj in ((2, 0), (6, 0), (7, 4)):
        @pl.when((d == 0) & (i == o))
        def _():
            head_rows(jj, 0, geo.ho, 8, 0)

    for e in range(q):
        to = dev(e, (i + V - 1) % V)
        tx.send((d == 0) & (i > 0), (hbuf, pl.ds(0, VECS)), tail_ref, 26, to)

    @pl.when(i == V - 1)
    def _():
        arrive((vr, pl.ds(0, V - 1)), (rsem, 24))
        tot = vp_ref[...]
        for k in range(V - 1):
            tot = tot + vr[k]
        vsum[...] = tot

    for k in range(1, q):
        tx.send(i == V - 1, vsum, (vq, k - 1), 25, dev((d + k) % q, i))
    plane(1, 2)

    @pl.when(i == V - 1)
    def _():
        arrive(vq, (rsem, 25))
        tot = vsum[...]
        for k in range(q - 1):
            tot = tot + vq[k]
        tail_ref[...] = tot

    @pl.when(i < V - 1)
    def _():
        arrive(tail_ref, (rsem, 26))

    for p in (2, 0, 1):
        plane(p, 3)
    tx.finish()
    out = pltpu.make_async_copy(fb, f_hbm, lsem.at[3])
    out.start()
    out.wait()


def main(geo, w, x, g):
    q, tl, t = geo.q, geo.tl, geo.t
    vm = pl.BlockSpec(memory_space=pltpu.VMEM)
    hbm = pl.BlockSpec(memory_space=pl.ANY)
    cos, sin = rot_tables(t)
    line = pltpu.VMEM((CHIPS, tl, D), BF16)
    line3 = pltpu.VMEM((CHIPS - 1, tl, D), BF16)
    vec = pltpu.VMEM((VECS, 128), F32)
    low = lambda *dims: pltpu.VMEM(dims, BF16)
    full = lambda *dims: pltpu.VMEM(dims, F32)
    return pl.pallas_call(
        partial(main_kernel, geo),
        out_shape=(
            jax.ShapeDtypeStruct((tl, D), F32),
            jax.ShapeDtypeStruct((tl, D), F32),
            jax.ShapeDtypeStruct((V, q, geo.er, 128), BF16),
            jax.ShapeDtypeStruct((VECS, 128), F32),
        ),
        in_specs=[hbm, hbm, hbm, vm, vm],
        out_specs=(vm, vm, hbm, vm),
        scratch_shapes=[
            full(HEAD + OWN + 3, 128),
            full(112, 128),
            low(V, q, geo.er, 128),
            low(VECS, 128),
            low(q, geo.zr, 128),
            low(t, D),
            low(t, D),
            low(VECS, 128),
            vec,
            full(16, D),
            low(D, 384),
            low(128, D),
            low(D, 512),
            low(512, D),
            full(t, 2),
            low(t, D),
            low(t, D),
            low(t, 128),
            low(t, 128),
            low(t, 128),
            low(t, 512),
            low(t, 512),
            low(t, 128),
            low(t, 128),
            low(t, 384),
            full(t, 128),
            full(8, D),
            vec,
            full(t, 2),
            low(6, geo.zr // 2, 128) if geo.square else low(q - 1, geo.zr, 128),
            low(geo.zr, 128),
            line, line, line3, line3,
            full(V - 1, VECS, 128),
            full(q - 1, VECS, 128),
            vec,
            full(512, 128),
            pltpu.SemaphoreType.DMA((4,)),
            pltpu.SemaphoreType.DMA((400,)),
            pltpu.SemaphoreType.DMA((SUMS + 3 * geo.ss,)),
            pltpu.SemaphoreType.DMA((24,)),
        ] + ([] if geo.tight else [low(t, D), low(V, q, geo.er, 128)]),
        compiler_params=pltpu.CompilerParams(
            collective_id=0, has_side_effects=True, vmem_limit_bytes=63 << 20
        ),
        name="layer",
    )(w, x, g, cos, sin)


def adam_kernel(
    geo, so_ref, sa_ref, x_ref, g_ref, tail_ref, f_hbm, w_hbm, m_hbm, s_hbm,
    lo_ref, tg_ref, wg_hbm, nw_hbm, nm_hbm, ns_hbm, wb, mb, sb, ob, gb, fb, lsem,
):
    _, i, _ = geo.place()
    loads = [pltpu.make_async_copy(f_hbm, fb, lsem.at[0])]
    for k, (h, b) in enumerate(((w_hbm, wb), (m_hbm, mb), (s_hbm, sb))):
        loads.append(pltpu.make_async_copy(h, b.at[pl.ds(0, OWN)], lsem.at[k + 1]))
    for ld in loads:
        ld.start()
    x = x_ref[...].astype(F32)
    sa = sa_ref[...]
    lo_ref[...] = (x + so_ref[...]).astype(BF16)
    mid = x - jnp.mean(x, axis=1, keepdims=True)
    inv = lax.rsqrt(jnp.mean(mid * mid, axis=1, keepdims=True) + 1e-05)
    xhat = mid * inv
    dx = inv * (sa - jnp.mean(sa, axis=1, keepdims=True) - xhat * jnp.mean(sa * xhat, axis=1, keepdims=True))
    tg_ref[...] = g_ref[...].astype(F32) + dx
    gb[pl.ds(ALI, VECS), :] = tail_ref[...]
    loads[0].wait()
    paste_share(geo, i, gb, fb)
    for ld in loads[1:]:
        ld.wait()
    rows_n = 1024
    full = OWN // rows_n
    pairs = ((wg_hbm, ob), (nw_hbm, wb), (nm_hbm, mb), (ns_hbm, sb))

    def adam(n, carry):
        rows = pl.ds(mult(n * rows_n, rows_n), rows_n)
        adam_rows(i, rows, n * rows_n, rows_n, wb, mb, sb, ob, gb)
        for k, (h, b) in enumerate(pairs):
            pltpu.make_async_copy(b.at[rows], h.at[rows], lsem.at[4 + k]).start()
        return carry

    lax.fori_loop(0, full, adam, 0)
    rest = OWN - full * rows_n
    adam_rows(i, pl.ds(full * rows_n, 16), full * rows_n, 16, wb, mb, sb, ob, gb)
    for k, (h, b) in enumerate(pairs):
        rows = pl.ds(full * rows_n, rest)
        pltpu.make_async_copy(b.at[rows], h.at[rows], lsem.at[4 + k]).start()
    for k, (h, b) in enumerate(pairs):
        pltpu.make_async_copy(b.at[pl.ds(0, OWN)], h, lsem.at[4 + k]).wait()


def adam_rows(i, rows, start, n, wb, mb, sb, ob, gb):
    g = gb[pl.ds(13 * i + start, n), :]
    w = wb[rows, :]
    m = BETA_ONE * mb[rows, :] + (1.0 - BETA_ONE) * g
    s = BETA_TWO * sb[rows, :] + (1.0 - BETA_TWO) * g * g
    ob[rows, :] = g
    mb[rows, :] = m
    sb[rows, :] = s
    mh = m * (1.0 / (1.0 - BETA_ONE**STEP))
    vh = s * (1.0 / (1.0 - BETA_TWO**STEP))
    wb[rows, :] = w - LEARN_RATE * (mh / (jnp.sqrt(vh) + EPSILON) + DECAY_RATE * w)


def paste_share(geo, i, gb, f_ref):
    q = geo.q

    def put(j, e, row, n, start, stride):
        gb[pl.ds(start, n, stride=stride), :] = f_ref[j, e, pl.ds(row, n), :].astype(F32)

    @pl.when(i < 2)
    def _():
        def body(n, c):
            e, s = n % q, n // q
            for b in range(8):
                put(b, e, mult(geo.qr * s, 16), geo.qr, 24 * geo.qr * e + 8 * s + b, 24)
            return c

        lax.fori_loop(0, 3 * q, body, 0)

    def rows_part(a0, ro, shift, count):
        def body(n, c):
            e, bl = n % q, n // q
            bb = bl + shift
            for b in range(8):
                put(
                    bb % V,
                    e,
                    mult(ro + geo.ap * (bb // V) + geo.ho * b, 16),
                    geo.ho,
                    a0 + 8 * (128 * bl + geo.ho * e) + b,
                    8,
                )
            return c

        lax.fori_loop(0, count * q, body, 0)

    def cols_part(a0, nr, ro):
        def body(n, c):
            e, t = n % q, n // q
            for b in range(8):
                put(b, e, mult(ro + nr * t, 16), nr, a0 + 32 * nr * e + 8 * t + b, 32)
            return c

        lax.fori_loop(0, 4 * q, body, 0)

    @pl.when(i == 2)
    def _():
        rows_part(0, 0, 0, 8)
        cols_part(8192, geo.u2, geo.ap)

    @pl.when((i == 3) | (i == 4))
    def _():
        cols_part(0, geo.u3, 0)

    @pl.when(i == 5)
    def _():
        cols_part(0, geo.u2, 0)
        rows_part(4096, geo.bp, 0, 8)

    @pl.when(i >= 6)
    def _():
        rows_part(0, 0, 4 * (i - 6), 12)


def adam(geo, so, sa, x, g, tail, f, w, m, s):
    tl = geo.tl
    vm = pl.BlockSpec(memory_space=pltpu.VMEM)
    hbm = pl.BlockSpec(memory_space=pl.ANY)
    flat = jax.ShapeDtypeStruct((OWN, 128), F32)
    big = pltpu.VMEM((OWN + 3, 128), F32)
    return pl.pallas_call(
        partial(adam_kernel, geo),
        out_shape=(
            jax.ShapeDtypeStruct((tl, D), BF16),
            jax.ShapeDtypeStruct((tl, D), F32),
            flat, flat, flat, flat,
        ),
        in_specs=[vm] * 5 + [hbm] * 4,
        out_specs=(vm, vm, hbm, hbm, hbm, hbm),
        scratch_shapes=[
            big, big, big, big,
            pltpu.VMEM((ALI + 128, 128), F32),
            pltpu.VMEM((V, geo.q, geo.er, 128), BF16),
            pltpu.SemaphoreType.DMA((8,)),
        ],
        compiler_params=pltpu.CompilerParams(vmem_limit_bytes=50 << 20),
        name="adam",
    )(so, sa, x, g, tail, f, w, m, s)


def local(mesh, tokens, cotangent, weights, first_moment, second_moment):
    rep = mesh.shape["ctx"] // V
    rows = tokens.shape[1]
    x, g = tokens[0], cotangent[0]
    flats = [weights, first_moment, second_moment]
    if rep > 1:
        groups = [[rep * k + r for r in range(rep)] for k in range(V)]
        join = lambda a: lax.all_gather(a, "ctx", axis=0, axis_index_groups=groups, tiled=True)
        x, g = join(x), join(g)
        flats = [join(a) for a in flats]
    w, m, s = [a.reshape(OWN, 128) for a in flats]
    geo = Geo(mesh, x.shape[0] * V)
    so, sa, f, tail = main(geo, w, x, g)
    outs = list(adam(geo, so, sa, x, g, tail, f, w, m, s))
    outs[2:] = [a.reshape(-1) for a in outs[2:]]
    if rep > 1:
        r = lax.axis_index("ctx") % rep
        outs = [lax.dynamic_slice_in_dim(a, r * (a.shape[0] // rep), a.shape[0] // rep, 0) for a in outs]
    return (outs[0][None], outs[1][None], *outs[2:])


def solution(mesh):
    return jax.shard_map(
        partial(local, mesh),
        mesh=mesh,
        in_specs=(P("dp", "ctx", None), P("dp", "ctx", None), P("ctx"), P("ctx"), P("ctx")),
        out_specs=(P("dp", "ctx", None), P("dp", "ctx", None), P("ctx"), P("ctx"), P("ctx"), P("ctx")),
        check_vma=False,
    )
```

```python
from functools import partial
import math

import numpy as np
import jax
import jax.numpy as jnp
from jax import lax
from jax.experimental import pallas as pl
from jax.experimental.pallas import tpu as pltpu
from jax.sharding import PartitionSpec as P

D = 1024
FF = 4096
HEADS = 16
HEAD_DIM = 64
ROT = 16
STEP = 3
BETA_ONE = 0.9
BETA_TWO = 0.95
LEARN_RATE = 0.004
DECAY_RATE = 0.1
EPSILON = 1e-08

F32 = jnp.float32
BF16 = jnp.bfloat16
MESH = pl.DeviceIdType.MESH
V = 8
CHIPS = V // 2
OWN = 12301
ALI = 12288
VECS = 104
HEAD = 112
RB = 256
PARTS = 29
SPREAD = 45


class Geo:
    def __init__(self, mesh, tokens):
        self.q = mesh.shape["dp"]
        self.rep = mesh.shape["ctx"] // V
        self.tl = tokens // V
        self.t = tokens
        q = self.q
        self.qr = 512 // q
        self.ho = 128 // q
        self.u2 = 128 // q
        self.u3 = 384 // q
        self.seg = 1536 // q
        self.zr = V * self.seg
        self.ap = 1024 // q
        self.bp = 512 // q
        self.er = 2 * self.ap
        self.tight = tokens > 1024
        self.rba = RB // 2 if self.tight else RB
        self.square = q == 4
        self.ss = max(4, q - 1)
        self.sums = SPREAD + 19 * self.ss
        self.lines = self.sums + 3 * self.ss

    def place(self):
        d = lax.axis_index("dp")
        a = lax.axis_index("ctx")
        return d, a // self.rep, a % self.rep

    def dev(self, e, j, rho):
        return {"dp": e, "ctx": j * self.rep + rho}

    def up_parts(self):
        return (
            (0, self.u2, 2 * self.seg + self.ap),
            (128, self.u3, 3 * self.seg),
            (512, self.u3, 4 * self.seg),
            (896, self.u2, 5 * self.seg),
        )

    def maps(self):
        q, out = self.q, []
        for e in range(q):
            for i in range(2):
                for s in range(3):
                    out.append((e, self.seg * i + self.qr * s, self.qr, 0, 512 * i + self.qr * e, 128 * s))
            for b in range(8):
                out.append((e, 2 * self.seg + self.ho * b, self.ho, 1, self.ho * e, 128 * b))
            for r0, nr, off in self.up_parts():
                for t in range(4):
                    out.append((e, off + nr * t, nr, 2, r0 + nr * e, 128 * t))
            for t in range(4):
                for b in range(8):
                    row = 5 * self.seg + self.bp + self.ap * t + self.ho * b
                    out.append((e, row, self.ho, 3, 128 * t + self.ho * e, 128 * b))
        return out


def dot(a, b):
    return jnp.dot(a, b, preferred_element_type=F32)


def dot_nt(a, b):
    return lax.dot_general(a, b, (((1,), (1,)), ((), ())), preferred_element_type=F32)


def dot_tn(a, b):
    return lax.dot_general(a, b, (((0,), (0,)), ((), ())), preferred_element_type=F32)


def mult(x, n):
    return pl.multiple_of(x, n)


def view(part):
    return part[0].at[part[1]] if isinstance(part, tuple) else part


def rcopy(src, dst, ssem, rsem, dev):
    return pltpu.make_async_remote_copy(
        src_ref=view(src),
        dst_ref=view(dst),
        send_sem=view(ssem),
        recv_sem=view(rsem),
        device_id=dev,
        device_id_type=MESH,
    )


class Sends:
    def __init__(self, ssem, rsem, used=None):
        self.ssem, self.rsem, self.open = ssem, rsem, []
        self.used = {} if used is None else used

    def group(self):
        return Sends(self.ssem, self.rsem, self.used)

    def slot(self, key):
        return (self.ssem, self.used.setdefault(key or ("own", len(self.used)), len(self.used)))

    def send(self, cond, src, dst, rs, dev, key=None):
        slot = self.slot(key)
        make = lambda: rcopy(src, dst, slot, (self.rsem, rs), dev)
        self.when(cond, lambda: make().start())
        self.open.append((cond, lambda: make().wait_send()))

    def copy(self, cond, src, dst, key=None):
        slot = self.slot(key)
        make = lambda: pltpu.make_async_copy(view(src), view(dst), view(slot))
        self.when(cond, lambda: make().start())
        self.open.append((cond, lambda: make().wait()))

    def block(self, cond, act):
        inner = self.group()
        self.when(cond, lambda: act(inner))
        if inner.open:

            def end():
                for _, wait in inner.open:
                    wait()

            self.open.append((cond, end))

    @staticmethod
    def when(cond, act):
        if cond is None:
            act()
        else:
            pl.when(cond)(act)

    def finish(self):
        for cond, act in self.open:
            self.when(cond, act)
        self.open.clear()


def arrive(part, sem):
    pltpu.make_async_copy(view(part), view(part), view(sem)).wait()


def entry_barrier(geo, d, i, rho):
    sem = pltpu.get_barrier_semaphore()
    for k in range(1, V):
        pl.semaphore_signal(sem, inc=1, device_id=geo.dev(d, (i + k) % V, rho), device_id_type=MESH)
    for k in range(1, geo.q):
        pl.semaphore_signal(sem, inc=1, device_id=geo.dev((d + k) % geo.q, i, rho), device_id_type=MESH)
    pl.semaphore_wait(sem, V - 1 + geo.q - 1)


def cut_share(geo, i, buf, e_ref):
    q, base = geo.q, HEAD - 13 * i

    def put(j, e, row, n, start, stride):
        e_ref[j, e, pl.ds(row, n), :] = buf[pl.ds(start, n, stride=stride), :].astype(BF16)

    @pl.when(i < 2)
    def _():
        def body(n, c):
            e, s = n % q, n // q
            for b in range(8):
                put(b, e, mult(geo.qr * s, 16), geo.qr, base + 24 * geo.qr * e + 8 * s + b, 24)
            return c

        lax.fori_loop(0, 3 * q, body, 0)

    def rows_part(a0, ro, shift, count):
        def body(n, c):
            e, bl = n % q, n // q
            bb = bl + shift
            for b in range(8):
                put(
                    bb % V,
                    e,
                    mult(ro + geo.ap * (bb // V) + geo.ho * b, 16),
                    geo.ho,
                    base + a0 + 8 * (128 * bl + geo.ho * e) + b,
                    8,
                )
            return c

        lax.fori_loop(0, count * q, body, 0)

    def cols_part(a0, nr, ro):
        def body(n, c):
            e, t = n % q, n // q
            for b in range(8):
                put(b, e, mult(ro + nr * t, 16), nr, base + a0 + 32 * nr * e + 8 * t + b, 32)
            return c

        lax.fori_loop(0, 4 * q, body, 0)

    @pl.when(i == 2)
    def _():
        rows_part(0, 0, 0, 8)
        cols_part(8192, geo.u2, geo.ap)

    @pl.when((i == 3) | (i == 4))
    def _():
        cols_part(0, geo.u3, 0)

    @pl.when(i == 5)
    def _():
        cols_part(0, geo.u2, 0)
        rows_part(4096, geo.bp, 0, 8)

    @pl.when(i >= 6)
    def _():
        rows_part(0, 0, 4 * (i - 6), 12)


def owner_moves(geo, i, j):
    k = i - 6
    return (
        (i < 6, 0, mult(geo.seg * i, 16), geo.seg),
        (i >= 6, mult(geo.ap * k, 16), mult(6 * geo.seg + 2 * geo.ap * k, 16), geo.ap),
        ((i >= 6) & (j // 4 == k), mult(geo.ap * (1 - k), 16), 6 * geo.seg + geo.ap, geo.ap),
    )


def sib_owner_rows(geo, sib, z_ref, sem):
    _, i, _ = geo.place()

    @pl.when(sib < 6)
    def _():
        arrive((z_ref, (slice(None), pl.ds(0, geo.seg))), sem)

    @pl.when((sib >= 6) & (i // 4 == sib - 6))
    def _():
        arrive((z_ref, (slice(None), pl.ds(0, 2 * geo.ap))), sem)

    @pl.when((sib >= 6) & (i // 4 != sib - 6))
    def _():
        arrive((z_ref, (slice(None), pl.ds(0, geo.ap))), sem)


def rot_tables(t):
    half = ROT // 2
    freq = (10000.0 ** (-2.0 * np.arange(half, dtype=np.float32) / ROT)).astype(np.float32)
    ang = np.arange(t, dtype=np.float32)[:, None] * freq[None, :]
    cos = np.ones((t, 128), np.float32)
    sin = np.zeros((t, 128), np.float32)
    for h in range(2):
        for k in range(2):
            lo = 64 * h + half * k
            cos[:, lo : lo + half] = np.cos(ang)
            sin[:, lo : lo + half] = np.sin(ang) * (1 if k else -1)
    return jnp.asarray(cos), jnp.asarray(sin)


def rot(v, cos, sin, lane, back):
    up = pltpu.roll(v, 120, 1)
    down = pltpu.roll(v, 8, 1)
    partner = jnp.where(lane % 16 < 8, up, down)
    turn = partner * sin
    return v * cos - turn if back else v * cos + turn


def main_kernel(
    geo, w_hbm, xin, gin, cos_ref, sin_ref, so_ref, sa_ref, f_hbm, tail_ref,
    buf, hb, e_ref, vs, z_ref, x_ref, g_ref, v_ref,
    vf, rowv, wq, wo, wu, wd, xh, n1, n2, qs, ks, vv, hid, du, ob, do, dqkv, dqs, acc, vp_ref,
    rb_ref, rz, sibo, siba, rcvo, rcva, vr, vq, vsum, hbuf, lsem, ssem, rsem, csem, *spare,
):
    gz_ref = z_ref
    po_ref, fb = (g_ref, e_ref) if geo.tight else spare
    q, tl, t = geo.q, geo.tl, geo.t
    seg, ap, bp = geo.seg, geo.ap, geo.bp
    d, i, rho = geo.place()
    j = i
    z, c = i // 2, i % 2
    sib = 2 * z + 1 - c
    near = (None, d - d % 2 + (1 - d % 2), (d + 2) % 4, 3 - d)
    rank = [(d + k) % q for k in range(q)]
    dev = partial(geo.dev, rho=rho)
    peers = [dev(e, i) for e in ((d, *near[1:]) if geo.square else rank)]
    early = Sends(ssem, rsem)
    tx = early.group()
    lc = Sends(csem, None)
    whole = slice(None)

    def spread_one(tx, part, sem, key):
        for k in (1, 2) if geo.square else range(1, q):
            tx.send(None, part(d, None), part(d, None), sem + k - 1, peers[k], (key, 1, k))

    def spread_two(tx, part, sem, key):
        if geo.square:
            for k in (1, 2):
                arrive(part(near[k], None), (rsem, sem + k - 1))
                half = part(near[k], k - 1)
                tx.send(None, half, half, sem + 1 + k, peers[3 - k], (key, 2, k))

    def spread_three(part, sem):
        if geo.square:
            for k in (1, 2):
                arrive(part(near[3], k - 1), (rsem, sem + 1 + k))
        else:
            for k in range(1, q):
                arrive(part(rank[q - k], None), (rsem, sem + k - 1))

    load = pltpu.make_async_copy(w_hbm, buf.at[pl.ds(HEAD, OWN)], lsem.at[0])
    load.start()
    rows_own = pl.ds(mult(i * tl, 16), tl)
    own = [
        pltpu.make_async_copy(xin, x_ref.at[rows_own], lsem.at[1]),
        pltpu.make_async_copy(gin, g_ref.at[rows_own], lsem.at[2]),
    ]
    for cp in own:
        cp.start()
    entry_barrier(geo, d, i, rho)
    halo = pl.ds(OWN - 109, 109)
    early.send(i < V - 1, (w_hbm, halo), (hb, pl.ds(0, 109)), 0, dev(d, (i + 1) % V))

    def chain(a, src, ref):
        dst = (ref, rows_own)
        early.send(z < CHIPS - 1, src, dst, 4 + 6 * a, dev(d, (i + 2) % V))
        early.send(z > 0, src, dst, 7 + 6 * a, dev(d, (i + V - 2) % V))
        early.send(None, src, dst, 2 + a, dev(d, sib))

    def hop(a, ref, k, last):
        for s, sign in ((0, 1), (1, -1)):
            there = (z >= k + 1) if sign == 1 else (z + k + 1 < CHIPS)
            on = (z < CHIPS - 1) if sign == 1 else (z > 0)
            ok = there & jnp.logical_not(on) if last else there & on
            src_i = (i - 2 * sign * (k + 1) + 2 * V) % V
            rs = 4 + 6 * a + 3 * s + k
            part = (ref, pl.ds(mult(src_i * tl, 16), tl))

            @pl.when(ok)
            def _():
                arrive(part, (rsem, rs))

            if not last:
                early.send(ok, part, part, rs + 1, dev(d, (i + 2 * sign + V) % V))
            early.send(ok, part, part, 2 + a, dev(d, sib), ("hop", a, k, s))

    def relay(a, ref, k):
        hop(a, ref, k, False)

    def end_of_line(a, ref):
        for k in range(CHIPS - 1):
            hop(a, ref, k, True)

    chain(0, xin, x_ref)
    load.wait()

    @pl.when(i > 0)
    def _():
        arrive((hb, pl.ds(0, 109)), (rsem, 0))
        buf[pl.ds(HEAD - 104, 104), :] = hb[pl.ds(5, 104), :]

    @pl.when(i == V - 1)
    def _():
        vs[...] = buf[pl.ds(HEAD + OWN - VECS, VECS), :].astype(BF16)
        v_ref[...] = vs[...]

    cut_share(geo, i, buf, e_ref)

    def slices_to(k):
        tx = early.group()
        for cc in range(2):
            to = (2 * (z + k) + cc) % V
            for m, (ok, erow, zrow, n) in enumerate(owner_moves(geo, i, to)):
                src = (e_ref, (to, d, pl.ds(erow, n)))
                tx.send(ok, src, (z_ref, (d, pl.ds(zrow, n))), 16 + k, dev(d, to), ("slice", k, cc, m // 2))
        return tx

    def slices_of(k):
        base = ((z + CHIPS - k) % CHIPS) * 2 * seg

        def part(e, half):
            at, n = (base, 2 * seg) if half is None else (base + half * seg, seg)
            return (z_ref, (e, pl.ds(mult(at, 16), n)))

        return part, SPREAD + geo.ss * (k - 1), ("slices", k)

    first = slices_to(1)
    for k in range(1, V):
        early.send(i == V - 1, vs, v_ref, 1, dev(d, (i + k) % V))
    for m, (ok, erow, zrow, n) in enumerate(owner_moves(geo, i, sib)):
        src = (e_ref, (sib, whole, pl.ds(erow, n)))
        early.send(ok, src, (z_ref, (whole, pl.ds(zrow, n))), 16, dev(d, sib), ("slice", 0, 0, m // 2))
    for m, (ok, erow, zrow, n) in enumerate(owner_moves(geo, i, i)):
        lc.copy(ok, (e_ref, (i, whole, pl.ds(erow, n))), (z_ref, (whole, pl.ds(zrow, n))), ("own", m // 2))
    first.finish()
    second = slices_to(2)
    relay(0, x_ref, 0)
    arrive((z_ref, (0, pl.ds(0, 2 * seg))), (rsem, 17))
    spread_one(early, *slices_of(1))
    second.finish()
    third = slices_to(3)
    arrive((z_ref, (0, pl.ds(0, 2 * seg))), (rsem, 18))
    spread_one(early, *slices_of(2))
    relay(0, x_ref, 1)
    chain(1, gin, g_ref)
    arrive((z_ref, (0, pl.ds(0, 2 * seg))), (rsem, 19))
    spread_one(early, *slices_of(3))
    relay(1, g_ref, 0)
    spread_two(early, *slices_of(1))
    spread_two(early, *slices_of(2))
    for cp in own:
        cp.wait()

    @pl.when(i < V - 1)
    def _():
        arrive(v_ref, (rsem, 1))

    nrb = t // RB
    vf[...] = v_ref[...].astype(F32)
    for k in range(9):
        for b in range(8):
            rowv[k : k + 1, 128 * b : 128 * b + 128] = vf[8 * k + b : 8 * k + b + 1, :]
    acc[...] = jnp.zeros_like(acc)
    vp_ref[...] = jnp.zeros_like(vp_ref)
    gp = lambda b, r: pl.ds(mult(b * t + r * RB, RB), RB)
    kv0, kv1 = 4 * t, 5 * t
    buf[kv0 : kv0 + 2 * t, :] = jnp.zeros((2 * t, 128), F32)

    def rb_of(r):
        return pl.ds(mult(r * RB, RB), RB)

    lane = lax.broadcasted_iota(jnp.int32, (RB, 128), 1)
    end_of_line(0, x_ref)
    arrive((x_ref, pl.ds(0, CHIPS * tl)), (rsem, 2))

    def norms(r, carry):
        rb = rb_of(r)
        x = x_ref[rb, :].astype(F32)
        mean = jnp.mean(x, axis=1, keepdims=True)
        mid = x - mean
        var = jnp.mean(mid * mid, axis=1, keepdims=True)
        inv = lax.rsqrt(var + 1e-05)
        xhat = mid * inv
        xh[rb, 0:1] = mean
        xh[rb, 1:2] = inv
        n1[rb, :] = (xhat * rowv[0:1, :] + rowv[1:2, :]).astype(BF16)
        n2[rb, :] = (xhat * rowv[2:3, :] + rowv[3:4, :]).astype(BF16)
        return carry

    spread_two(early, *slices_of(3))
    lax.fori_loop(0, nrb, norms, 0)
    relay(1, g_ref, 1)
    sib_owner_rows(geo, sib, z_ref, (rsem, 16))
    lc.finish()
    for k in range(1, CHIPS):
        spread_three(*slices_of(k)[:2])
    mats = (wq, wo, wu, wd)
    for e, zrow, n, m, row, ln in geo.maps():
        mats[m][row : row + n, ln : ln + 128] = z_ref[e, zrow : zrow + n, :]

    def forward(r, carry):
        rb = rb_of(r)
        qkv = dot(n1[rb, :], wq[...])
        cos, sin = cos_ref[rb, :], sin_ref[rb, :]
        qh = qkv[:, 0:128] + vf[pl.ds(32 + j, 1), :]
        kh = qkv[:, 128:256] + vf[pl.ds(40 + j, 1), :]
        vh = qkv[:, 256:384] + vf[pl.ds(48 + j, 1), :]
        qs[rb, :] = (rot(qh, cos, sin, lane, False) * 0.125).astype(BF16)
        ks[rb, :] = rot(kh, cos, sin, lane, False).astype(BF16)
        vv[rb, :] = vh.astype(BF16)
        up = dot(n2[rb, :], wu[...])
        for b in range(4):
            cols = slice(128 * b, 128 * b + 128)
            u = up[:, cols] + vf[pl.ds(72 + 8 * b + j, 1), :]
            phi = 0.5 + 0.5 * lax.erf(u * (1.0 / math.sqrt(2.0)))
            hid[rb, cols] = (u * phi).astype(BF16)
            buf[gp(b, r), :] = phi + u * (jnp.exp(-0.5 * u * u) * (1.0 / math.sqrt(2.0 * math.pi)))
        return carry

    lax.fori_loop(0, nrb, forward, 0)

    ra = geo.rba
    left = lax.broadcasted_iota(jnp.int32, (ra, 128), 1) < 64
    diag = lax.broadcasted_iota(jnp.int32, (ra, ra), 0) >= lax.broadcasted_iota(jnp.int32, (ra, ra), 1)
    zero = jnp.zeros((), BF16)

    def mine(h, v):
        return jnp.where(left if h == 0 else jnp.logical_not(left), v, zero)

    def scores(r, qm):
        n = (r + 1) * ra
        s = dot_nt(qm, ks[0:n, :])
        tail = jnp.where(diag, s[:, n - ra : n], -1e30)
        return tail if r == 0 else jnp.concatenate([s[:, : n - ra], tail], axis=1)

    for r in range(t // ra):
        rb, n = slice(r * ra, r * ra + ra), (r + 1) * ra
        outs = []
        for h in range(2):
            s = scores(r, mine(h, qs[rb, :]))
            top = jnp.max(s, axis=1, keepdims=True)
            ex = jnp.exp(s - top)
            tot = jnp.sum(ex, axis=1, keepdims=True)
            xh[rb, 2 + h : 3 + h] = top + jnp.log(tot)
            outs.append(dot((ex * (1.0 / tot)).astype(BF16), vv[0:n, :]))
        ob[rb, :] = jnp.where(left, outs[0], outs[1]).astype(BF16)

    def outputs(r, carry):
        rb = rb_of(r)
        po_ref[rb, :] = (dot(hid[rb, :], wd[...]) + dot(ob[rb, :], wo[...])).astype(BF16)
        return carry

    def to_sibling(a, part, sums):
        for k in range(CHIPS):
            rows = pl.ds(mult((2 * k + 1 - c) * tl, 16), tl)
            tx.send(None, (part, rows), (sums, k), 20 + a, dev(d, sib))

    def line_rows(a, part, sums):
        arrive(sums, (rsem, 20 + a))
        for k in range(CHIPS):
            rows = pl.ds(mult((2 * k + c) * tl, 16), tl)
            sums[k] = (part[rows, :].astype(F32) + sums[k].astype(F32)).astype(BF16)

    def slot_of(s, step):
        return 2 * (step - 1) - 1 + s if step > 1 else 0

    def line_step(a, step, sums, got):
        for s, sign in ((0, 1), (1, -1)):
            far = z if sign == 1 else CHIPS - 1 - z
            ok = far < step
            dest = z + sign * (CHIPS - step)
            rs = geo.lines + 6 * a + 3 * s + step - 1
            if step > 1:

                @pl.when(ok & (far > 0))
                def _():
                    at = slot_of(s, step - 1)
                    arrive((got, at), (rsem, rs - 1))
                    sums[dest] = (sums[dest].astype(F32) + got[at].astype(F32)).astype(BF16)

            tx.send(ok, (sums, dest), (got, slot_of(s, step)), rs, dev(d, (i + 2 * sign + V) % V))

    def line_end(a, sums, got, out):
        tot = sums[z].astype(F32)
        if a == 0:
            tot = tot + (rowv[7:8, :] + rowv[8:9, :])
        out[...] = tot
        for s, more in ((0, z > 0), (1, z < CHIPS - 1)):

            @pl.when(more)
            def _():
                at = slot_of(s, 3)
                arrive((got, at), (rsem, geo.lines + 6 * a + 3 * s + 2))
                out[...] += got[at].astype(F32)

    if not geo.tight:
        lax.fori_loop(0, nrb, outputs, 0)
        to_sibling(0, po_ref, sibo)
    end_of_line(1, g_ref)
    arrive((g_ref, pl.ds(0, CHIPS * tl)), (rsem, 3))

    if not geo.tight:
        line_rows(0, po_ref, sibo)
        line_step(0, 1, sibo, rcvo)
    def grad_heads(r, carry):
        rb = rb_of(r)
        do[rb, :] = dot_nt(g_ref[rb, :], wo[...]).astype(BF16)
        return carry

    lax.fori_loop(0, nrb, grad_heads, 0)
    third.finish()
    early.finish()
    pc = 4096 // q
    ph = pc // 2

    def grad_down(k, carry):
        res = dot_tn(hid[:, pl.ds(mult(k * 256, 256), 256)], g_ref[...]).astype(BF16)
        for h in range(2):
            row = 5 * seg + bp + ap * (2 * k + h)
            for e in range(q):
                for b in range(8):
                    r0 = 128 * h + geo.ho * e
                    block = res[r0 : r0 + geo.ho, 128 * b : 128 * b + 128]
                    gz_ref[e, pl.ds(mult(row + geo.ho * b, 16), geo.ho), :] = block
        return carry

    def halves(p, h):
        return pl.ds(p * pc + h * ph, ph), pl.ds(p * ph, ph)

    def sum_one(p):
        sem = geo.sums + geo.ss * p
        if geo.square:
            for k in (1, 2):
                rows, at = halves(p, k - 1)
                for slot, e in enumerate((near[k], near[3])):
                    dst = (rb_ref, (2 * (k - 1) + slot, at))
                    tx.send(None, (gz_ref, (e, rows)), dst, sem + k - 1, dev(near[k], i))
        else:
            rows = pl.ds(p * pc, pc)
            for k in range(1, q):
                e = (d + k) % q
                tx.send(None, (gz_ref, (e, rows)), (rb_ref, (k - 1, rows)), sem + k - 1, dev(e, i))

    def sum_two(p):
        sem = geo.sums + geo.ss * p
        if geo.square:
            for k in (1, 2):
                rows, at = halves(p, k - 1)
                arrive((rb_ref, (pl.ds(2 * (k - 1), 2), at)), (rsem, sem + k - 1))
                mid = 2 * (k - 1) + 1
                tot = gz_ref[near[3 - k], rows, :].astype(F32) + rb_ref[mid, at, :].astype(F32)
                rb_ref[mid, at, :] = tot.astype(BF16)
                tx.send(None, (rb_ref, (mid, at)), (rb_ref, (3 + k, at)), sem + 1 + k, dev(near[3 - k], i))

    def sum_three(p):
        sem = geo.sums + geo.ss * p
        if geo.square:
            for k in (1, 2):
                rows, at = halves(p, k - 1)
                arrive((rb_ref, (3 + k, at)), (rsem, sem + 1 + k))
                tot = gz_ref[d, rows, :].astype(F32) + rb_ref[2 * (k - 1), at, :].astype(F32)
                rz[rows, :] = (tot + rb_ref[3 + k, at, :].astype(F32)).astype(BF16)
        else:
            rows = pl.ds(p * pc, pc)
            for k in range(1, q):
                arrive((rb_ref, (k - 1, rows)), (rsem, sem + k - 1))
            tot = gz_ref[d, rows, :].astype(F32)
            for k in range(q - 1):
                tot = tot + rb_ref[k, rows, :].astype(F32)
            rz[rows, :] = tot.astype(BF16)

    moves = (
        ((0, 0, 0, seg, 0), (1, seg, 0, seg, 0), (2, 2 * seg, 0, ap, 0)),
        (
            (2, 2 * seg + ap, ap, bp, 1),
            (3, 3 * seg, 0, seg, 1),
            (4, 4 * seg, 0, seg, 1),
            (5, 5 * seg, 0, bp, 1),
        ),
        ((5, 5 * seg + bp, bp, ap, 2), (6, 6 * seg, 0, ap, 2), (7, 6 * seg + 2 * ap, ap, ap, 2)),
    )

    chip = [(z + k) % CHIPS for k in range(CHIPS)]
    pair = [mult(2 * at, 2) for at in chip]
    single = [(2 * at, 2 * at + 1) for at in chip]

    def to_owners(p):
        sum_three(p)
        for o, zrow, frow, n, kind in moves[p]:
            src, dst = (rz, pl.ds(zrow, n)), (fb, (i, d, pl.ds(frow, n)))
            tx.send(i != o, src, dst, PARTS + 4 * kind + (z + CHIPS - o // 2) % CHIPS, dev(d, o))
            lc.copy(i == o, src, dst, ("part", kind))
        if p == 2:
            for o in (6, 7):
                here = i // 4 == o - 6
                src, dst = (rz, pl.ds(6 * seg + ap, ap)), (fb, (i, d, pl.ds(ap * (7 - o), ap)))
                rs = PARTS + 12 + (z + CHIPS - o // 2) % CHIPS
                tx.send(here & (i != o), src, dst, rs, dev(d, o), ("last", 0))
                lc.copy(here & (i == o), src, dst, ("part", 3))

    def held(p, k):
        out = [(o, frow, n, kind) for o, _, frow, n, kind in moves[p]]
        if p == 2:
            out += [(6, ap, ap, 3)] if k in (1, 2) else [(7, 0, ap, 3)]
        return out

    def plane(p, stage, k):
        if stage == 1 and k == 0:
            lc.finish()
        for o, frow, n, kind in held(p, k):

            def part(e, half):
                js = pl.ds(pair[k], 2) if half is None else single[k][half]
                return (fb, (js, e, pl.ds(frow, n)))

            sem, key = SPREAD + geo.ss * (3 + 4 * kind + k), ("held", kind, k)

            def act(tx):
                if stage == 1:
                    arrive((fb, (pl.ds(0, 2 if k else 1), 0, pl.ds(frow, n))), (rsem, PARTS + 4 * kind + k))
                    spread_one(tx, part, sem, key)
                elif stage == 2:
                    spread_two(tx, part, sem, key)
                else:
                    spread_three(part, sem)

            tx.block(i == o, act)

    for r in range(t // ra):
        rb, n = slice(r * ra, r * ra + ra), (r + 1) * ra
        dqh = []
        for h in range(2):
            qm, gm = mine(h, qs[rb, :]), mine(h, do[rb, :])
            prob = jnp.exp(scores(r, qm) - xh[rb, 2 + h : 3 + h])
            dp = dot_nt(gm, vv[0:n, :])
            delta = jnp.sum(prob * dp, axis=1, keepdims=True)
            ds = (prob * (dp - delta)).astype(BF16)
            dqh.append(dot(ds, ks[0:n, :]))
            buf[kv0 : kv0 + n, :] += dot_tn(ds, qm)
            buf[kv1 : kv1 + n, :] += dot_tn(prob.astype(BF16), gm)
        dqs[rb, :] = jnp.where(left, dqh[0], dqh[1])

    if not geo.tight:
        line_step(0, 2, sibo, rcvo)

    def back_one(r, carry):
        rb = rb_of(r)
        cos, sin = cos_ref[rb, :], sin_ref[rb, :]
        low = jnp.concatenate(
            [
                (rot(dqs[rb, :], cos, sin, lane, True) * 0.125).astype(BF16),
                rot(buf[pl.ds(mult(kv0 + r * RB, RB), RB), :], cos, sin, lane, True).astype(BF16),
                buf[pl.ds(mult(kv1 + r * RB, RB), RB), :].astype(BF16),
            ],
            axis=1,
        )
        dqkv[rb, :] = low
        acc[6:7, 0:384] += jnp.sum(low.astype(F32), axis=0, keepdims=True)
        return carry

    lax.fori_loop(0, nrb, back_one, 0)
    res = dot_tn(ob[...], g_ref[...]).astype(BF16)
    for e in range(q):
        for b in range(8):
            row = 2 * seg + geo.ho * b
            gz_ref[e, row : row + geo.ho, :] = res[geo.ho * e : geo.ho * e + geo.ho, 128 * b : 128 * b + 128]
    for k in range(2):
        res = dot_tn(n1[:, 512 * k : 512 * k + 512], dqkv[...]).astype(BF16)
        for e in range(q):
            for b in range(3):
                row = seg * k + geo.qr * b
                block = res[geo.qr * e : geo.qr * e + geo.qr, 128 * b : 128 * b + 128]
                gz_ref[e, row : row + geo.qr, :] = block
    sum_one(0)

    def back_mlp(r, carry):
        rb = rb_of(r)
        g = g_ref[rb, :]
        dh = dot_nt(g, wd[...])
        for b in range(4):
            cols = slice(128 * b, 128 * b + 128)
            low = (dh[:, cols] * buf[gp(b, r), :]).astype(BF16)
            du[rb, cols] = low
            acc[5:6, cols] += jnp.sum(low.astype(F32), axis=0, keepdims=True)
        acc[4:5, :] += jnp.sum(g.astype(F32), axis=0, keepdims=True)
        return carry

    lax.fori_loop(0, nrb, back_mlp, 0)

    def back_two(r, carry):
        rb = rb_of(r)
        xhat = (x_ref[rb, :].astype(F32) - xh[rb, 0:1]) * xh[rb, 1:2]
        d1 = dot_nt(dqkv[rb, :], wq[...])
        acc[0:1, :] += jnp.sum(d1 * xhat, axis=0, keepdims=True)
        acc[1:2, :] += jnp.sum(d1, axis=0, keepdims=True)
        d2 = dot_nt(du[rb, :], wu[...])
        acc[2:3, :] += jnp.sum(d2 * xhat, axis=0, keepdims=True)
        acc[3:4, :] += jnp.sum(d2, axis=0, keepdims=True)
        x_ref[rb, :] = (d1 * rowv[0:1, :] + d2 * rowv[2:3, :]).astype(BF16)
        return carry

    lax.fori_loop(0, nrb, back_two, 0)
    to_sibling(1, x_ref, siba)
    lax.fori_loop(0, 2, grad_down, 0)
    sum_two(0)
    sum_one(2)
    if geo.tight:
        lax.fori_loop(0, nrb, outputs, 0)
        to_sibling(0, po_ref, sibo)
        line_rows(0, po_ref, sibo)
        line_step(0, 1, sibo, rcvo)
        line_step(0, 2, sibo, rcvo)
    line_step(0, 3, sibo, rcvo)
    line_rows(1, x_ref, siba)
    line_step(1, 1, siba, rcva)
    for r0, nr, off in geo.up_parts():
        res = dot_tn(n2[:, r0 : r0 + q * nr], du[...]).astype(BF16)
        for e in range(q):
            for b in range(4):
                gz_ref[e, off + nr * b : off + nr * b + nr, :] = res[nr * e : nr * e + nr, 128 * b : 128 * b + 128]
    sum_one(1)
    to_owners(0)
    plane(0, 1, 0)
    sum_two(2)
    line_step(1, 2, siba, rcva)
    to_owners(2)
    plane(2, 1, 0)
    sum_two(1)
    to_owners(1)
    plane(1, 1, 0)
    plane(0, 1, 1)
    plane(0, 2, 0)
    line_step(1, 3, siba, rcva)
    plane(2, 1, 1)
    plane(2, 2, 0)
    plane(1, 1, 1)
    plane(1, 2, 0)
    zeroth = jnp.where(j == 0, 1.0, 0.0)
    for b in range(8):
        cols = slice(128 * b, 128 * b + 128)
        for k in range(4):
            vp_ref[8 * k + b : 8 * k + b + 1, :] = acc[k : k + 1, cols]
        for k in (7, 8):
            vp_ref[8 * k + b : 8 * k + b + 1, :] = acc[4:5, cols] * zeroth
    for k in range(3):
        vp_ref[pl.ds(32 + 8 * k + j, 1), :] = acc[6:7, 128 * k : 128 * k + 128]
    for k in range(4):
        vp_ref[pl.ds(72 + 8 * k + j, 1), :] = acc[5:6, 128 * k : 128 * k + 128]
    tx.send(i < V - 1, vp_ref, (vr, i), 26, dev(d, V - 1))
    for k in (2, 3):
        for p in (0, 2, 1):
            plane(p, 1, k)
            plane(p, 2, k - 1)
    line_end(0, sibo, rcvo, so_ref)
    line_end(1, siba, rcva, sa_ref)
    for p in (0, 2, 1):
        plane(p, 2, 3)

    def head_rows(jj, row, n, stride, s):
        for b in range(8):
            at = row if jj is None else row + n * b
            src = fb[b if jj is None else jj, 0, at : at + 16, :]
            hbuf[pl.ds(8 * s + b, 16, stride=stride), :] = src.astype(F32)

    @pl.when((d == 0) & (i == 1))
    def _():
        for s in range(3):
            head_rows(None, geo.qr * s, geo.qr, 24, s)

    for o, n in ((3, geo.u3), (4, geo.u3), (5, geo.u2)):
        @pl.when((d == 0) & (i == o))
        def _():
            for s in range(4):
                head_rows(None, n * s, n, 32, s)

    for o, jj in ((2, 0), (6, 0), (7, 4)):
        @pl.when((d == 0) & (i == o))
        def _():
            head_rows(jj, 0, geo.ho, 8, 0)

    for e in range(q):
        to = dev(e, (i + V - 1) % V)
        tx.send((d == 0) & (i > 0), (hbuf, pl.ds(0, VECS)), tail_ref, 28, to)

    @pl.when(i == V - 1)
    def _():
        arrive((vr, pl.ds(0, V - 1)), (rsem, 26))
        tot = vp_ref[...]
        for k in range(V - 1):
            tot = tot + vr[k]
        vsum[...] = tot

    for k in range(1, q):
        tx.send(i == V - 1, vsum, (vq, k - 1), 27, dev((d + k) % q, i))

    @pl.when(i == V - 1)
    def _():
        arrive(vq, (rsem, 27))
        tot = vsum[...]
        for k in range(q - 1):
            tot = tot + vq[k]
        tail_ref[...] = tot

    @pl.when(i < V - 1)
    def _():
        arrive(tail_ref, (rsem, 28))

    for k in range(CHIPS):
        for p in (0, 2, 1):
            plane(p, 3, k)
    tx.finish()
    out = pltpu.make_async_copy(fb, f_hbm, lsem.at[3])
    out.start()
    out.wait()


def main(geo, w, x, g):
    q, tl, t = geo.q, geo.tl, geo.t
    vm = pl.BlockSpec(memory_space=pltpu.VMEM)
    hbm = pl.BlockSpec(memory_space=pl.ANY)
    cos, sin = rot_tables(t)
    line = pltpu.VMEM((CHIPS, tl, D), BF16)
    lines = pltpu.VMEM((2 * CHIPS - 3, tl, D), BF16)
    vec = pltpu.VMEM((VECS, 128), F32)
    low = lambda *dims: pltpu.VMEM(dims, BF16)
    full = lambda *dims: pltpu.VMEM(dims, F32)
    return pl.pallas_call(
        partial(main_kernel, geo),
        out_shape=(
            jax.ShapeDtypeStruct((tl, D), F32),
            jax.ShapeDtypeStruct((tl, D), F32),
            jax.ShapeDtypeStruct((V, q, geo.er, 128), BF16),
            jax.ShapeDtypeStruct((VECS, 128), F32),
        ),
        in_specs=[hbm, hbm, hbm, vm, vm],
        out_specs=(vm, vm, hbm, vm),
        scratch_shapes=[
            full(HEAD + OWN + 3, 128),
            full(112, 128),
            low(V, q, geo.er, 128),
            low(VECS, 128),
            low(q, geo.zr, 128),
            low(t, D),
            low(t, D),
            low(VECS, 128),
            vec,
            full(16, D),
            low(D, 384),
            low(128, D),
            low(D, 512),
            low(512, D),
            full(t, 4),
            low(t, D),
            low(t, D),
            low(t, 128),
            low(t, 128),
            low(t, 128),
            low(t, 512),
            low(t, 512),
            low(t, 128),
            low(t, 128),
            low(t, 384),
            full(t, 128),
            full(8, D),
            vec,
            low(6, geo.zr // 2, 128) if geo.square else low(q - 1, geo.zr, 128),
            low(geo.zr, 128),
            line, line, lines, lines,
            full(V - 1, VECS, 128),
            full(q - 1, VECS, 128),
            vec,
            full(512, 128),
            pltpu.SemaphoreType.DMA((4,)),
            pltpu.SemaphoreType.DMA((184 if geo.square else 256,)),
            pltpu.SemaphoreType.DMA((geo.lines + 12,)),
            pltpu.SemaphoreType.DMA((8,)),
        ] + ([] if geo.tight else [low(t, D), low(V, q, geo.er, 128)]),
        compiler_params=pltpu.CompilerParams(
            collective_id=0, has_side_effects=True, vmem_limit_bytes=67_000_000
        ),
        name="layer",
    )(w, x, g, cos, sin)


def adam_kernel(
    geo, so_hbm, sa_hbm, x_hbm, g_hbm, tail_hbm, f_hbm, w_hbm, m_hbm, s_hbm,
    lo_ref, tg_ref, wg_hbm, nw_hbm, nm_hbm, ns_hbm, wb, mb, sb, ob, gb, fb, so_ref, sa_ref, x_ref, g_ref, lsem,
):
    _, i, _ = geo.place()
    first = (so_hbm, so_ref), (sa_hbm, sa_ref), (x_hbm, x_ref), (g_hbm, g_ref)
    then = (tail_hbm, gb.at[pl.ds(ALI, VECS)]), (f_hbm, fb)
    last = tuple((h, b.at[pl.ds(0, OWN)]) for h, b in ((w_hbm, wb), (m_hbm, mb), (s_hbm, sb)))
    loads = [pltpu.make_async_copy(h, b, lsem.at[4 + k]) for k, (h, b) in enumerate(first + then + last)]
    for ld in loads:
        ld.start()
    for ld in loads[:4]:
        ld.wait()
    x = x_ref[...].astype(F32)
    sa = sa_ref[...]
    lo_ref[...] = (x + so_ref[...]).astype(BF16)
    mid = x - jnp.mean(x, axis=1, keepdims=True)
    inv = lax.rsqrt(jnp.mean(mid * mid, axis=1, keepdims=True) + 1e-05)
    xhat = mid * inv
    dx = inv * (sa - jnp.mean(sa, axis=1, keepdims=True) - xhat * jnp.mean(sa * xhat, axis=1, keepdims=True))
    tg_ref[...] = g_ref[...].astype(F32) + dx
    for ld in loads[4:6]:
        ld.wait()
    paste_share(geo, i, gb, fb)
    for ld in loads[6:]:
        ld.wait()
    rows_n = 1024
    full = OWN // rows_n
    pairs = ((wg_hbm, ob), (nw_hbm, wb), (nm_hbm, mb), (ns_hbm, sb))

    def adam(n, carry):
        rows = pl.ds(mult(n * rows_n, rows_n), rows_n)
        adam_rows(i, rows, n * rows_n, rows_n, wb, mb, sb, ob, gb)
        for k, (h, b) in enumerate(pairs):
            pltpu.make_async_copy(b.at[rows], h.at[rows], lsem.at[k]).start()
        return carry

    lax.fori_loop(0, full, adam, 0)
    rest = OWN - full * rows_n
    adam_rows(i, pl.ds(full * rows_n, 16), full * rows_n, 16, wb, mb, sb, ob, gb)
    for k, (h, b) in enumerate(pairs):
        rows = pl.ds(full * rows_n, rest)
        pltpu.make_async_copy(b.at[rows], h.at[rows], lsem.at[k]).start()
    for k, (h, b) in enumerate(pairs):
        pltpu.make_async_copy(b.at[pl.ds(0, OWN)], h, lsem.at[k]).wait()


def adam_rows(i, rows, start, n, wb, mb, sb, ob, gb):
    g = gb[pl.ds(13 * i + start, n), :]
    w = wb[rows, :]
    m = BETA_ONE * mb[rows, :] + (1.0 - BETA_ONE) * g
    s = BETA_TWO * sb[rows, :] + (1.0 - BETA_TWO) * g * g
    ob[rows, :] = g
    mb[rows, :] = m
    sb[rows, :] = s
    mh = m * (1.0 / (1.0 - BETA_ONE**STEP))
    vh = s * (1.0 / (1.0 - BETA_TWO**STEP))
    wb[rows, :] = w - LEARN_RATE * (mh / (jnp.sqrt(vh) + EPSILON) + DECAY_RATE * w)


def paste_share(geo, i, gb, f_ref):
    q = geo.q

    def put(j, e, row, n, start, stride):
        gb[pl.ds(start, n, stride=stride), :] = f_ref[j, e, pl.ds(row, n), :].astype(F32)

    @pl.when(i < 2)
    def _():
        def body(n, c):
            e, s = n % q, n // q
            for b in range(8):
                put(b, e, mult(geo.qr * s, 16), geo.qr, 24 * geo.qr * e + 8 * s + b, 24)
            return c

        lax.fori_loop(0, 3 * q, body, 0)

    def rows_part(a0, ro, shift, count):
        def body(n, c):
            e, bl = n % q, n // q
            bb = bl + shift
            for b in range(8):
                put(
                    bb % V,
                    e,
                    mult(ro + geo.ap * (bb // V) + geo.ho * b, 16),
                    geo.ho,
                    a0 + 8 * (128 * bl + geo.ho * e) + b,
                    8,
                )
            return c

        lax.fori_loop(0, count * q, body, 0)

    def cols_part(a0, nr, ro):
        def body(n, c):
            e, t = n % q, n // q
            for b in range(8):
                put(b, e, mult(ro + nr * t, 16), nr, a0 + 32 * nr * e + 8 * t + b, 32)
            return c

        lax.fori_loop(0, 4 * q, body, 0)

    @pl.when(i == 2)
    def _():
        rows_part(0, 0, 0, 8)
        cols_part(8192, geo.u2, geo.ap)

    @pl.when((i == 3) | (i == 4))
    def _():
        cols_part(0, geo.u3, 0)

    @pl.when(i == 5)
    def _():
        cols_part(0, geo.u2, 0)
        rows_part(4096, geo.bp, 0, 8)

    @pl.when(i >= 6)
    def _():
        rows_part(0, 0, 4 * (i - 6), 12)


def adam(geo, so, sa, x, g, tail, f, w, m, s):
    tl = geo.tl
    vm = pl.BlockSpec(memory_space=pltpu.VMEM)
    hbm = pl.BlockSpec(memory_space=pl.ANY)
    flat = jax.ShapeDtypeStruct((OWN, 128), F32)
    big = pltpu.VMEM((OWN + 3, 128), F32)
    return pl.pallas_call(
        partial(adam_kernel, geo),
        out_shape=(
            jax.ShapeDtypeStruct((tl, D), BF16),
            jax.ShapeDtypeStruct((tl, D), F32),
            flat, flat, flat, flat,
        ),
        in_specs=[hbm] * 9,
        out_specs=(vm, vm, hbm, hbm, hbm, hbm),
        scratch_shapes=[
            big, big, big, big,
            pltpu.VMEM((ALI + 128, 128), F32),
            pltpu.VMEM((V, geo.q, geo.er, 128), BF16),
            pltpu.VMEM((tl, D), F32),
            pltpu.VMEM((tl, D), F32),
            pltpu.VMEM((tl, D), BF16),
            pltpu.VMEM((tl, D), BF16),
            pltpu.SemaphoreType.DMA((13,)),
        ],
        compiler_params=pltpu.CompilerParams(vmem_limit_bytes=67_000_000),
        name="adam",
    )(so, sa, x, g, tail, f, w, m, s)


def local(mesh, tokens, cotangent, weights, first_moment, second_moment):
    rep = mesh.shape["ctx"] // V
    rows = tokens.shape[1]
    x, g = tokens[0], cotangent[0]
    flats = [weights, first_moment, second_moment]
    if rep > 1:
        groups = [[rep * k + r for r in range(rep)] for k in range(V)]
        join = lambda a: lax.all_gather(a, "ctx", axis=0, axis_index_groups=groups, tiled=True)
        x, g = join(x), join(g)
        flats = [join(a) for a in flats]
    w, m, s = [a.reshape(OWN, 128) for a in flats]
    geo = Geo(mesh, x.shape[0] * V)
    so, sa, f, tail = main(geo, w, x, g)
    outs = list(adam(geo, so, sa, x, g, tail, f, w, m, s))
    outs[2:] = [a.reshape(-1) for a in outs[2:]]
    if rep > 1:
        r = lax.axis_index("ctx") % rep
        outs = [lax.dynamic_slice_in_dim(a, r * (a.shape[0] // rep), a.shape[0] // rep, 0) for a in outs]
    return (outs[0][None], outs[1][None], *outs[2:])


def solution(mesh):
    return jax.shard_map(
        partial(local, mesh),
        mesh=mesh,
        in_specs=(P("dp", "ctx", None), P("dp", "ctx", None), P("ctx"), P("ctx"), P("ctx")),
        out_specs=(P("dp", "ctx", None), P("dp", "ctx", None), P("ctx"), P("ctx"), P("ctx"), P("ctx")),
        check_vma=False,
    )
```

```python
from functools import partial
import math

import numpy as np
import jax
import jax.numpy as jnp
from jax import lax
from jax.experimental import pallas as pl
from jax.experimental.pallas import tpu as pltpu
from jax.sharding import PartitionSpec as P

D = 1024
FF = 4096
HEADS = 16
HEAD_DIM = 64
ROT = 16
STEP = 3
BETA_ONE = 0.9
BETA_TWO = 0.95
LEARN_RATE = 0.004
DECAY_RATE = 0.1
EPSILON = 1e-08

F32 = jnp.float32
BF16 = jnp.bfloat16
MESH = pl.DeviceIdType.MESH
V = 8
CHIPS = V // 2
OWN = 12301
ALI = 12288
VECS = 104
HEAD = 112
RB = 256
PARTS = 29
SPREAD = 37


class Geo:
    def __init__(self, mesh, tokens):
        self.q = mesh.shape["dp"]
        self.rep = mesh.shape["ctx"] // V
        self.tl = tokens // V
        self.t = tokens
        q = self.q
        self.qr = 512 // q
        self.ho = 128 // q
        self.u2 = 128 // q
        self.u3 = 384 // q
        self.seg = 1536 // q
        self.zr = V * self.seg
        self.ap = 1024 // q
        self.bp = 512 // q
        self.er = 2 * self.ap
        self.tight = tokens > 1024
        self.rba = RB // 2 if self.tight else RB
        self.square = q == 4
        self.ss = max(4, q - 1)
        self.sums = SPREAD + 11 * self.ss
        self.lines = self.sums + 3 * self.ss

    def place(self):
        d = lax.axis_index("dp")
        a = lax.axis_index("ctx")
        return d, a // self.rep, a % self.rep

    def dev(self, e, j, rho):
        return {"dp": e, "ctx": j * self.rep + rho}

    def up_parts(self):
        return (
            (0, self.u2, 2 * self.seg + self.ap),
            (128, self.u3, 3 * self.seg),
            (512, self.u3, 4 * self.seg),
            (896, self.u2, 5 * self.seg),
        )

    def maps(self):
        q, out = self.q, []
        for e in range(q):
            for i in range(2):
                for s in range(3):
                    out.append((e, self.seg * i + self.qr * s, self.qr, 0, 512 * i + self.qr * e, 128 * s))
            for b in range(8):
                out.append((e, 2 * self.seg + self.ho * b, self.ho, 1, self.ho * e, 128 * b))
            for r0, nr, off in self.up_parts():
                for t in range(4):
                    out.append((e, off + nr * t, nr, 2, r0 + nr * e, 128 * t))
            for t in range(4):
                for b in range(8):
                    row = 5 * self.seg + self.bp + self.ap * t + self.ho * b
                    out.append((e, row, self.ho, 3, 128 * t + self.ho * e, 128 * b))
        return out


def dot(a, b):
    return jnp.dot(a, b, preferred_element_type=F32)


def dot_nt(a, b):
    return lax.dot_general(a, b, (((1,), (1,)), ((), ())), preferred_element_type=F32)


def dot_tn(a, b):
    return lax.dot_general(a, b, (((0,), (0,)), ((), ())), preferred_element_type=F32)


def mult(x, n):
    return pl.multiple_of(x, n)


def view(part):
    return part[0].at[part[1]] if isinstance(part, tuple) else part


def rcopy(src, dst, ssem, rsem, dev):
    return pltpu.make_async_remote_copy(
        src_ref=view(src),
        dst_ref=view(dst),
        send_sem=view(ssem),
        recv_sem=view(rsem),
        device_id=dev,
        device_id_type=MESH,
    )


class Sends:
    def __init__(self, ssem, rsem, used=None):
        self.ssem, self.rsem, self.open = ssem, rsem, []
        self.used = {} if used is None else used

    def group(self):
        return Sends(self.ssem, self.rsem, self.used)

    def slot(self, key):
        return (self.ssem, self.used.setdefault(key or ("own", len(self.used)), len(self.used)))

    def send(self, cond, src, dst, rs, dev, key=None):
        slot = self.slot(key)
        make = lambda: rcopy(src, dst, slot, (self.rsem, rs), dev)
        self.when(cond, lambda: make().start())
        self.open.append((cond, lambda: make().wait_send()))

    def copy(self, cond, src, dst, key=None):
        slot = self.slot(key)
        make = lambda: pltpu.make_async_copy(view(src), view(dst), view(slot))
        self.when(cond, lambda: make().start())
        self.open.append((cond, lambda: make().wait()))

    def block(self, cond, act):
        inner = self.group()
        self.when(cond, lambda: act(inner))
        if inner.open:

            def end():
                for _, wait in inner.open:
                    wait()

            self.open.append((cond, end))

    @staticmethod
    def when(cond, act):
        if cond is None:
            act()
        else:
            pl.when(cond)(act)

    def finish(self):
        for cond, act in self.open:
            self.when(cond, act)
        self.open.clear()


def arrive(part, sem):
    pltpu.make_async_copy(view(part), view(part), view(sem)).wait()


def entry_barrier(geo, d, i, rho):
    sem = pltpu.get_barrier_semaphore()
    for k in range(1, V):
        pl.semaphore_signal(sem, inc=1, device_id=geo.dev(d, (i + k) % V, rho), device_id_type=MESH)
    for k in range(1, geo.q):
        pl.semaphore_signal(sem, inc=1, device_id=geo.dev((d + k) % geo.q, i, rho), device_id_type=MESH)
    pl.semaphore_wait(sem, V - 1 + geo.q - 1)


def cut_share(geo, i, buf, e_ref):
    q, base = geo.q, HEAD - 13 * i

    def put(j, e, row, n, start, stride):
        e_ref[j, e, pl.ds(row, n), :] = buf[pl.ds(start, n, stride=stride), :].astype(BF16)

    @pl.when(i < 2)
    def _():
        def body(n, c):
            e, s = n % q, n // q
            for b in range(8):
                put(b, e, mult(geo.qr * s, 16), geo.qr, base + 24 * geo.qr * e + 8 * s + b, 24)
            return c

        lax.fori_loop(0, 3 * q, body, 0)

    def rows_part(a0, ro, shift, count):
        def body(n, c):
            e, bl = n % q, n // q
            bb = bl + shift
            for b in range(8):
                put(
                    bb % V,
                    e,
                    mult(ro + geo.ap * (bb // V) + geo.ho * b, 16),
                    geo.ho,
                    base + a0 + 8 * (128 * bl + geo.ho * e) + b,
                    8,
                )
            return c

        lax.fori_loop(0, count * q, body, 0)

    def cols_part(a0, nr, ro):
        def body(n, c):
            e, t = n % q, n // q
            for b in range(8):
                put(b, e, mult(ro + nr * t, 16), nr, base + a0 + 32 * nr * e + 8 * t + b, 32)
            return c

        lax.fori_loop(0, 4 * q, body, 0)

    @pl.when(i == 2)
    def _():
        rows_part(0, 0, 0, 8)
        cols_part(8192, geo.u2, geo.ap)

    @pl.when((i == 3) | (i == 4))
    def _():
        cols_part(0, geo.u3, 0)

    @pl.when(i == 5)
    def _():
        cols_part(0, geo.u2, 0)
        rows_part(4096, geo.bp, 0, 8)

    @pl.when(i >= 6)
    def _():
        rows_part(0, 0, 4 * (i - 6), 12)


def owner_moves(geo, i, j):
    k = i - 6
    return (
        (i < 6, 0, mult(geo.seg * i, 16), geo.seg),
        (i >= 6, mult(geo.ap * k, 16), mult(6 * geo.seg + 2 * geo.ap * k, 16), geo.ap),
        ((i >= 6) & (j // 4 == k), mult(geo.ap * (1 - k), 16), 6 * geo.seg + geo.ap, geo.ap),
    )


def sib_owner_rows(geo, sib, z_ref, sem):
    _, i, _ = geo.place()

    @pl.when(sib < 6)
    def _():
        arrive((z_ref, (slice(None), pl.ds(0, geo.seg))), sem)

    @pl.when((sib >= 6) & (i // 4 == sib - 6))
    def _():
        arrive((z_ref, (slice(None), pl.ds(0, 2 * geo.ap))), sem)

    @pl.when((sib >= 6) & (i // 4 != sib - 6))
    def _():
        arrive((z_ref, (slice(None), pl.ds(0, geo.ap))), sem)


def rot_tables(t):
    half = ROT // 2
    freq = (10000.0 ** (-2.0 * np.arange(half, dtype=np.float32) / ROT)).astype(np.float32)
    ang = np.arange(t, dtype=np.float32)[:, None] * freq[None, :]
    cos = np.ones((t, 128), np.float32)
    sin = np.zeros((t, 128), np.float32)
    for h in range(2):
        for k in range(2):
            lo = 64 * h + half * k
            cos[:, lo : lo + half] = np.cos(ang)
            sin[:, lo : lo + half] = np.sin(ang) * (1 if k else -1)
    return jnp.asarray(cos), jnp.asarray(sin)


def rot(v, cos, sin, lane, back):
    up = pltpu.roll(v, 120, 1)
    down = pltpu.roll(v, 8, 1)
    partner = jnp.where(lane % 16 < 8, up, down)
    turn = partner * sin
    return v * cos - turn if back else v * cos + turn


def main_kernel(
    geo, w_hbm, xin, gin, cos_ref, sin_ref, so_ref, sa_ref, f_hbm, tail_ref,
    buf, hb, e_ref, vs, z_ref, x_ref, g_ref, v_ref,
    vf, rowv, wq, wo, wu, wd, xh, n1, n2, qs, ks, vv, hid, du, ob, do, dqkv, dqs, acc, vp_ref,
    rb_ref, rz, sibo, siba, rcvo, rcva, vr, vq, vsum, hbuf, lsem, ssem, rsem, csem, *spare,
):
    gz_ref = z_ref
    po_ref, fb = (g_ref, e_ref) if geo.tight else spare
    q, tl, t = geo.q, geo.tl, geo.t
    seg, ap, bp = geo.seg, geo.ap, geo.bp
    d, i, rho = geo.place()
    j = i
    z, c = i // 2, i % 2
    sib = 2 * z + 1 - c
    near = (None, d - d % 2 + (1 - d % 2), (d + 2) % 4, 3 - d)
    rank = [(d + k) % q for k in range(q)]
    dev = partial(geo.dev, rho=rho)
    peers = [dev(e, i) for e in ((d, *near[1:]) if geo.square else rank)]
    early = Sends(ssem, rsem)
    tx = early.group()
    lc = Sends(csem, None)
    whole = slice(None)

    def spread_one(tx, part, sem, key):
        for k in (1, 2) if geo.square else range(1, q):
            tx.send(None, part(d, None), part(d, None), sem + k - 1, peers[k], (key, 1, k))

    def spread_two(tx, part, sem, key):
        if geo.square:
            for k in (1, 2):
                arrive(part(near[k], None), (rsem, sem + k - 1))
                half = part(near[k], k - 1)
                tx.send(None, half, half, sem + 1 + k, peers[3 - k], (key, 2, k))

    def spread_three(part, sem):
        if geo.square:
            for k in (1, 2):
                arrive(part(near[3], k - 1), (rsem, sem + 1 + k))
        else:
            for k in range(1, q):
                arrive(part(rank[q - k], None), (rsem, sem + k - 1))

    load = pltpu.make_async_copy(w_hbm, buf.at[pl.ds(HEAD, OWN)], lsem.at[0])
    load.start()
    rows_own = pl.ds(mult(i * tl, 16), tl)
    own = [
        pltpu.make_async_copy(xin, x_ref.at[rows_own], lsem.at[1]),
        pltpu.make_async_copy(gin, g_ref.at[rows_own], lsem.at[2]),
    ]
    for cp in own:
        cp.start()
    entry_barrier(geo, d, i, rho)
    halo = pl.ds(OWN - 109, 109)
    early.send(i < V - 1, (w_hbm, halo), (hb, pl.ds(0, 109)), 0, dev(d, (i + 1) % V))

    def chain(a, src, ref):
        dst = (ref, rows_own)
        early.send(z < CHIPS - 1, src, dst, 4 + 6 * a, dev(d, (i + 2) % V))
        early.send(z > 0, src, dst, 7 + 6 * a, dev(d, (i + V - 2) % V))
        early.send(None, src, dst, 2 + a, dev(d, sib))

    def hop(a, ref, k, last):
        for s, sign in ((0, 1), (1, -1)):
            there = (z >= k + 1) if sign == 1 else (z + k + 1 < CHIPS)
            on = (z < CHIPS - 1) if sign == 1 else (z > 0)
            ok = there & jnp.logical_not(on) if last else there & on
            src_i = (i - 2 * sign * (k + 1) + 2 * V) % V
            rs = 4 + 6 * a + 3 * s + k
            part = (ref, pl.ds(mult(src_i * tl, 16), tl))

            @pl.when(ok)
            def _():
                arrive(part, (rsem, rs))

            if not last:
                early.send(ok, part, part, rs + 1, dev(d, (i + 2 * sign + V) % V))
            early.send(ok, part, part, 2 + a, dev(d, sib), ("hop", a, k, s))

    def relay(a, ref, k):
        hop(a, ref, k, False)

    def end_of_line(a, ref):
        for k in range(CHIPS - 1):
            hop(a, ref, k, True)

    chain(0, xin, x_ref)
    load.wait()

    @pl.when(i > 0)
    def _():
        arrive((hb, pl.ds(0, 109)), (rsem, 0))
        buf[pl.ds(HEAD - 104, 104), :] = hb[pl.ds(5, 104), :]

    @pl.when(i == V - 1)
    def _():
        vs[...] = buf[pl.ds(HEAD + OWN - VECS, VECS), :].astype(BF16)
        v_ref[...] = vs[...]

    cut_share(geo, i, buf, e_ref)

    def slices_to(k):
        tx = early.group()
        for cc in range(2):
            to = (2 * (z + k) + cc) % V
            for m, (ok, erow, zrow, n) in enumerate(owner_moves(geo, i, to)):
                src = (e_ref, (to, d, pl.ds(erow, n)))
                tx.send(ok, src, (z_ref, (d, pl.ds(zrow, n))), 16 + k, dev(d, to), ("slice", k, cc, m // 2))
        return tx

    def slices_of(k):
        base = ((z + CHIPS - k) % CHIPS) * 2 * seg

        def part(e, half):
            at, n = (base, 2 * seg) if half is None else (base + half * seg, seg)
            return (z_ref, (e, pl.ds(mult(at, 16), n)))

        return part, SPREAD + geo.ss * (k - 1), ("slices", k)

    first = slices_to(1)
    for k in range(1, V):
        early.send(i == V - 1, vs, v_ref, 1, dev(d, (i + k) % V))
    for m, (ok, erow, zrow, n) in enumerate(owner_moves(geo, i, sib)):
        src = (e_ref, (sib, whole, pl.ds(erow, n)))
        early.send(ok, src, (z_ref, (whole, pl.ds(zrow, n))), 16, dev(d, sib), ("slice", 0, 0, m // 2))
    for m, (ok, erow, zrow, n) in enumerate(owner_moves(geo, i, i)):
        lc.copy(ok, (e_ref, (i, whole, pl.ds(erow, n))), (z_ref, (whole, pl.ds(zrow, n))), ("own", m // 2))
    first.finish()
    second = slices_to(2)
    relay(0, x_ref, 0)
    arrive((z_ref, (0, pl.ds(0, 2 * seg))), (rsem, 17))
    spread_one(early, *slices_of(1))
    second.finish()
    third = slices_to(3)
    arrive((z_ref, (0, pl.ds(0, 2 * seg))), (rsem, 18))
    spread_one(early, *slices_of(2))
    relay(0, x_ref, 1)
    chain(1, gin, g_ref)
    arrive((z_ref, (0, pl.ds(0, 2 * seg))), (rsem, 19))
    spread_one(early, *slices_of(3))
    relay(1, g_ref, 0)
    spread_two(early, *slices_of(1))
    spread_two(early, *slices_of(2))
    for cp in own:
        cp.wait()

    @pl.when(i < V - 1)
    def _():
        arrive(v_ref, (rsem, 1))

    nrb = t // RB
    vf[...] = v_ref[...].astype(F32)
    for k in range(9):
        for b in range(8):
            rowv[k : k + 1, 128 * b : 128 * b + 128] = vf[8 * k + b : 8 * k + b + 1, :]
    acc[...] = jnp.zeros_like(acc)
    vp_ref[...] = jnp.zeros_like(vp_ref)
    gp = lambda b, r: pl.ds(mult(b * t + r * RB, RB), RB)
    kv0, kv1 = 4 * t, 5 * t
    buf[kv0 : kv0 + 2 * t, :] = jnp.zeros((2 * t, 128), F32)

    def rb_of(r):
        return pl.ds(mult(r * RB, RB), RB)

    lane = lax.broadcasted_iota(jnp.int32, (RB, 128), 1)
    end_of_line(0, x_ref)
    arrive((x_ref, pl.ds(0, CHIPS * tl)), (rsem, 2))

    def norms(r, carry):
        rb = rb_of(r)
        x = x_ref[rb, :].astype(F32)
        mean = jnp.mean(x, axis=1, keepdims=True)
        mid = x - mean
        var = jnp.mean(mid * mid, axis=1, keepdims=True)
        inv = lax.rsqrt(var + 1e-05)
        xhat = mid * inv
        xh[rb, 0:1] = mean
        xh[rb, 1:2] = inv
        n1[rb, :] = (xhat * rowv[0:1, :] + rowv[1:2, :]).astype(BF16)
        n2[rb, :] = (xhat * rowv[2:3, :] + rowv[3:4, :]).astype(BF16)
        return carry

    spread_two(early, *slices_of(3))
    lax.fori_loop(0, nrb, norms, 0)
    relay(1, g_ref, 1)
    sib_owner_rows(geo, sib, z_ref, (rsem, 16))
    lc.finish()
    for k in range(1, CHIPS):
        spread_three(*slices_of(k)[:2])
    mats = (wq, wo, wu, wd)
    for e, zrow, n, m, row, ln in geo.maps():
        mats[m][row : row + n, ln : ln + 128] = z_ref[e, zrow : zrow + n, :]

    def forward(r, carry):
        rb = rb_of(r)
        qkv = dot(n1[rb, :], wq[...])
        cos, sin = cos_ref[rb, :], sin_ref[rb, :]
        qh = qkv[:, 0:128] + vf[pl.ds(32 + j, 1), :]
        kh = qkv[:, 128:256] + vf[pl.ds(40 + j, 1), :]
        vh = qkv[:, 256:384] + vf[pl.ds(48 + j, 1), :]
        qs[rb, :] = (rot(qh, cos, sin, lane, False) * 0.125).astype(BF16)
        ks[rb, :] = rot(kh, cos, sin, lane, False).astype(BF16)
        vv[rb, :] = vh.astype(BF16)
        up = dot(n2[rb, :], wu[...])
        for b in range(4):
            cols = slice(128 * b, 128 * b + 128)
            u = up[:, cols] + vf[pl.ds(72 + 8 * b + j, 1), :]
            phi = 0.5 + 0.5 * lax.erf(u * (1.0 / math.sqrt(2.0)))
            hid[rb, cols] = (u * phi).astype(BF16)
            buf[gp(b, r), :] = phi + u * (jnp.exp(-0.5 * u * u) * (1.0 / math.sqrt(2.0 * math.pi)))
        return carry

    lax.fori_loop(0, nrb, forward, 0)

    ra = geo.rba
    left = lax.broadcasted_iota(jnp.int32, (ra, 128), 1) < 64
    diag = lax.broadcasted_iota(jnp.int32, (ra, ra), 0) >= lax.broadcasted_iota(jnp.int32, (ra, ra), 1)
    zero = jnp.zeros((), BF16)

    def mine(h, v):
        return jnp.where(left if h == 0 else jnp.logical_not(left), v, zero)

    def scores(r, qm):
        n = (r + 1) * ra
        s = dot_nt(qm, ks[0:n, :])
        tail = jnp.where(diag, s[:, n - ra : n], -1e30)
        return tail if r == 0 else jnp.concatenate([s[:, : n - ra], tail], axis=1)

    for r in range(t // ra):
        rb, n = slice(r * ra, r * ra + ra), (r + 1) * ra
        outs = []
        for h in range(2):
            s = scores(r, mine(h, qs[rb, :]))
            top = jnp.max(s, axis=1, keepdims=True)
            ex = jnp.exp(s - top)
            tot = jnp.sum(ex, axis=1, keepdims=True)
            xh[rb, 2 + h : 3 + h] = top + jnp.log(tot)
            outs.append(dot((ex * (1.0 / tot)).astype(BF16), vv[0:n, :]))
        ob[rb, :] = jnp.where(left, outs[0], outs[1]).astype(BF16)

    def outputs(r, carry):
        rb = rb_of(r)
        po_ref[rb, :] = (dot(hid[rb, :], wd[...]) + dot(ob[rb, :], wo[...])).astype(BF16)
        return carry

    def to_sibling(a, part, sums):
        for k in range(CHIPS):
            rows = pl.ds(mult((2 * k + 1 - c) * tl, 16), tl)
            tx.send(None, (part, rows), (sums, k), 20 + a, dev(d, sib))

    def line_rows(a, part, sums):
        arrive(sums, (rsem, 20 + a))
        for k in range(CHIPS):
            rows = pl.ds(mult((2 * k + c) * tl, 16), tl)
            sums[k] = (part[rows, :].astype(F32) + sums[k].astype(F32)).astype(BF16)

    def slot_of(s, step):
        return 2 * (step - 1) - 1 + s if step > 1 else 0

    def line_step(a, step, sums, got):
        for s, sign in ((0, 1), (1, -1)):
            far = z if sign == 1 else CHIPS - 1 - z
            ok = far < step
            dest = z + sign * (CHIPS - step)
            rs = geo.lines + 6 * a + 3 * s + step - 1
            if step > 1:

                @pl.when(ok & (far > 0))
                def _():
                    at = slot_of(s, step - 1)
                    arrive((got, at), (rsem, rs - 1))
                    sums[dest] = (sums[dest].astype(F32) + got[at].astype(F32)).astype(BF16)

            tx.send(ok, (sums, dest), (got, slot_of(s, step)), rs, dev(d, (i + 2 * sign + V) % V))

    def line_end(a, sums, got, out):
        tot = sums[z].astype(F32)
        if a == 0:
            tot = tot + (rowv[7:8, :] + rowv[8:9, :])
        out[...] = tot
        for s, more in ((0, z > 0), (1, z < CHIPS - 1)):

            @pl.when(more)
            def _():
                at = slot_of(s, 3)
                arrive((got, at), (rsem, geo.lines + 6 * a + 3 * s + 2))
                out[...] += got[at].astype(F32)

    if not geo.tight:
        lax.fori_loop(0, nrb, outputs, 0)
        to_sibling(0, po_ref, sibo)
    end_of_line(1, g_ref)
    arrive((g_ref, pl.ds(0, CHIPS * tl)), (rsem, 3))

    if not geo.tight:
        line_rows(0, po_ref, sibo)
        line_step(0, 1, sibo, rcvo)
    def grad_heads(r, carry):
        rb = rb_of(r)
        do[rb, :] = dot_nt(g_ref[rb, :], wo[...]).astype(BF16)
        return carry

    lax.fori_loop(0, nrb, grad_heads, 0)

    def back_mlp(r, carry):
        rb = rb_of(r)
        g = g_ref[rb, :]
        dh = dot_nt(g, wd[...])
        for b in range(4):
            cols = slice(128 * b, 128 * b + 128)
            low = (dh[:, cols] * buf[gp(b, r), :]).astype(BF16)
            du[rb, cols] = low
            acc[5:6, cols] += jnp.sum(low.astype(F32), axis=0, keepdims=True)
        acc[4:5, :] += jnp.sum(g.astype(F32), axis=0, keepdims=True)
        return carry

    lax.fori_loop(0, nrb, back_mlp, 0)

    third.finish()
    early.finish()
    pc = 4096 // q
    ph = pc // 2

    def grad_down(k, carry):
        res = dot_tn(hid[:, pl.ds(mult(k * 256, 256), 256)], g_ref[...]).astype(BF16)
        for h in range(2):
            row = 5 * seg + bp + ap * (2 * k + h)
            for e in range(q):
                for b in range(8):
                    r0 = 128 * h + geo.ho * e
                    block = res[r0 : r0 + geo.ho, 128 * b : 128 * b + 128]
                    gz_ref[e, pl.ds(mult(row + geo.ho * b, 16), geo.ho), :] = block
        return carry

    def halves(p, h):
        return pl.ds(p * pc + h * ph, ph), pl.ds(p * ph, ph)

    def sum_one(p):
        sem = geo.sums + geo.ss * p
        if geo.square:
            for k in (1, 2):
                rows, at = halves(p, k - 1)
                for slot, e in enumerate((near[k], near[3])):
                    dst = (rb_ref, (2 * (k - 1) + slot, at))
                    tx.send(None, (gz_ref, (e, rows)), dst, sem + k - 1, dev(near[k], i))
        else:
            rows = pl.ds(p * pc, pc)
            for k in range(1, q):
                e = (d + k) % q
                tx.send(None, (gz_ref, (e, rows)), (rb_ref, (k - 1, rows)), sem + k - 1, dev(e, i))

    def sum_two(p):
        sem = geo.sums + geo.ss * p
        if geo.square:
            for k in (1, 2):
                rows, at = halves(p, k - 1)
                arrive((rb_ref, (pl.ds(2 * (k - 1), 2), at)), (rsem, sem + k - 1))
                mid = 2 * (k - 1) + 1
                tot = gz_ref[near[3 - k], rows, :].astype(F32) + rb_ref[mid, at, :].astype(F32)
                rb_ref[mid, at, :] = tot.astype(BF16)
                tx.send(None, (rb_ref, (mid, at)), (rb_ref, (3 + k, at)), sem + 1 + k, dev(near[3 - k], i))

    def sum_three(p):
        sem = geo.sums + geo.ss * p
        if geo.square:
            for k in (1, 2):
                rows, at = halves(p, k - 1)
                arrive((rb_ref, (3 + k, at)), (rsem, sem + 1 + k))
                tot = gz_ref[d, rows, :].astype(F32) + rb_ref[2 * (k - 1), at, :].astype(F32)
                rz[rows, :] = (tot + rb_ref[3 + k, at, :].astype(F32)).astype(BF16)
        else:
            rows = pl.ds(p * pc, pc)
            for k in range(1, q):
                arrive((rb_ref, (k - 1, rows)), (rsem, sem + k - 1))
            tot = gz_ref[d, rows, :].astype(F32)
            for k in range(q - 1):
                tot = tot + rb_ref[k, rows, :].astype(F32)
            rz[rows, :] = tot.astype(BF16)

    moves = (
        ((0, 0, 0, seg, 0), (1, seg, 0, seg, 0), (2, 2 * seg, 0, ap, 0)),
        (
            (2, 2 * seg + ap, ap, bp, 1),
            (3, 3 * seg, 0, seg, 1),
            (4, 4 * seg, 0, seg, 1),
            (5, 5 * seg, 0, bp, 1),
        ),
        ((5, 5 * seg + bp, bp, ap, 2), (6, 6 * seg, 0, ap, 2), (7, 6 * seg + 2 * ap, ap, ap, 2)),
    )

    chip = [(z + k) % CHIPS for k in range(CHIPS)]
    pair = [mult(2 * at, 2) for at in chip]
    single = [(2 * at, 2 * at + 1) for at in chip]

    def to_owners(p):
        sum_three(p)
        for o, zrow, frow, n, kind in moves[p]:
            src, dst = (rz, pl.ds(zrow, n)), (fb, (i, d, pl.ds(frow, n)))
            tx.send(i != o, src, dst, PARTS + 4 * (kind % 2) + (z + CHIPS - o // 2) % CHIPS, dev(d, o))
            lc.copy(i == o, src, dst, ("part", kind))
        if p == 2:
            for o in (6, 7):
                here = i // 4 == o - 6
                src, dst = (rz, pl.ds(6 * seg + ap, ap)), (fb, (i, d, pl.ds(ap * (7 - o), ap)))
                rs = PARTS + 4 + (z + CHIPS - o // 2) % CHIPS
                tx.send(here & (i != o), src, dst, rs, dev(d, o), ("last", 0))
                lc.copy(here & (i == o), src, dst, ("part", 3))

    def held(p, k):
        out = [(o, frow, n, kind) for o, _, frow, n, kind in moves[p]]
        if p == 2:
            out += [(6, ap, ap, 3)] if k in (1, 2) else [(7, 0, ap, 3)]
        return out

    def plane(p, stage, k):
        if stage == 1 and k == 0:
            lc.finish()
        for o, frow, n, kind in held(p, k):

            def part(e, half):
                js = pl.ds(pair[k], 2) if half is None else single[k][half]
                return (fb, (js, e, pl.ds(frow, n)))

            sem, key = SPREAD + geo.ss * (3 + 4 * (kind % 2) + k), ("held", kind % 2, k)

            def act(tx):
                if stage == 1:
                    arrive((fb, (pl.ds(0, 2 if k else 1), 0, pl.ds(frow, n))), (rsem, PARTS + 4 * (kind % 2) + k))
                    spread_one(tx, part, sem, key)
                elif stage == 2:
                    spread_two(tx, part, sem, key)
                else:
                    spread_three(part, sem)

            tx.block(i == o, act)

    lax.fori_loop(0, 2, grad_down, 0)
    sum_one(2)

    for r in range(t // ra):
        rb, n = slice(r * ra, r * ra + ra), (r + 1) * ra
        dqh = []
        for h in range(2):
            qm, gm = mine(h, qs[rb, :]), mine(h, do[rb, :])
            prob = jnp.exp(scores(r, qm) - xh[rb, 2 + h : 3 + h])
            dp = dot_nt(gm, vv[0:n, :])
            delta = jnp.sum(prob * dp, axis=1, keepdims=True)
            ds = (prob * (dp - delta)).astype(BF16)
            dqh.append(dot(ds, ks[0:n, :]))
            buf[kv0 : kv0 + n, :] += dot_tn(ds, qm)
            buf[kv1 : kv1 + n, :] += dot_tn(prob.astype(BF16), gm)
        dqs[rb, :] = jnp.where(left, dqh[0], dqh[1])

    sum_two(2)
    if not geo.tight:
        line_step(0, 2, sibo, rcvo)

    def back_one(r, carry):
        rb = rb_of(r)
        cos, sin = cos_ref[rb, :], sin_ref[rb, :]
        low = jnp.concatenate(
            [
                (rot(dqs[rb, :], cos, sin, lane, True) * 0.125).astype(BF16),
                rot(buf[pl.ds(mult(kv0 + r * RB, RB), RB), :], cos, sin, lane, True).astype(BF16),
                buf[pl.ds(mult(kv1 + r * RB, RB), RB), :].astype(BF16),
            ],
            axis=1,
        )
        dqkv[rb, :] = low
        acc[6:7, 0:384] += jnp.sum(low.astype(F32), axis=0, keepdims=True)
        return carry

    lax.fori_loop(0, nrb, back_one, 0)
    res = dot_tn(ob[...], g_ref[...]).astype(BF16)
    for e in range(q):
        for b in range(8):
            row = 2 * seg + geo.ho * b
            gz_ref[e, row : row + geo.ho, :] = res[geo.ho * e : geo.ho * e + geo.ho, 128 * b : 128 * b + 128]
    for k in range(2):
        res = dot_tn(n1[:, 512 * k : 512 * k + 512], dqkv[...]).astype(BF16)
        for e in range(q):
            for b in range(3):
                row = seg * k + geo.qr * b
                block = res[geo.qr * e : geo.qr * e + geo.qr, 128 * b : 128 * b + 128]
                gz_ref[e, row : row + geo.qr, :] = block
    sum_one(0)
    to_owners(2)
    plane(2, 1, 0)
    if not geo.tight:
        line_step(0, 3, sibo, rcvo)

    def back_two(r, carry):
        rb = rb_of(r)
        xhat = (x_ref[rb, :].astype(F32) - xh[rb, 0:1]) * xh[rb, 1:2]
        d1 = dot_nt(dqkv[rb, :], wq[...])
        acc[0:1, :] += jnp.sum(d1 * xhat, axis=0, keepdims=True)
        acc[1:2, :] += jnp.sum(d1, axis=0, keepdims=True)
        d2 = dot_nt(du[rb, :], wu[...])
        acc[2:3, :] += jnp.sum(d2 * xhat, axis=0, keepdims=True)
        acc[3:4, :] += jnp.sum(d2, axis=0, keepdims=True)
        x_ref[rb, :] = (d1 * rowv[0:1, :] + d2 * rowv[2:3, :]).astype(BF16)
        return carry

    lax.fori_loop(0, nrb, back_two, 0)
    to_sibling(1, x_ref, siba)
    for r0, nr, off in geo.up_parts():
        res = dot_tn(n2[:, r0 : r0 + q * nr], du[...]).astype(BF16)
        for e in range(q):
            for b in range(4):
                gz_ref[e, off + nr * b : off + nr * b + nr, :] = res[nr * e : nr * e + nr, 128 * b : 128 * b + 128]
    sum_two(0)
    sum_one(1)
    if geo.tight:
        lax.fori_loop(0, nrb, outputs, 0)
        to_sibling(0, po_ref, sibo)
        line_rows(0, po_ref, sibo)
        line_step(0, 1, sibo, rcvo)
        line_step(0, 2, sibo, rcvo)
        line_step(0, 3, sibo, rcvo)
    line_rows(1, x_ref, siba)
    line_step(1, 1, siba, rcva)
    to_owners(0)
    plane(0, 1, 0)
    sum_two(1)
    plane(2, 1, 1)
    plane(2, 2, 0)
    to_owners(1)
    line_step(1, 2, siba, rcva)
    plane(1, 1, 0)
    plane(0, 1, 1)
    plane(0, 2, 0)
    plane(1, 1, 1)
    plane(1, 2, 0)
    zeroth = jnp.where(j == 0, 1.0, 0.0)
    for b in range(8):
        cols = slice(128 * b, 128 * b + 128)
        for k in range(4):
            vp_ref[8 * k + b : 8 * k + b + 1, :] = acc[k : k + 1, cols]
        for k in (7, 8):
            vp_ref[8 * k + b : 8 * k + b + 1, :] = acc[4:5, cols] * zeroth
    for k in range(3):
        vp_ref[pl.ds(32 + 8 * k + j, 1), :] = acc[6:7, 128 * k : 128 * k + 128]
    for k in range(4):
        vp_ref[pl.ds(72 + 8 * k + j, 1), :] = acc[5:6, 128 * k : 128 * k + 128]
    tx.send(i < V - 1, vp_ref, (vr, i), 26, dev(d, V - 1))
    for k in (2, 3):
        for p in (2, 0, 1):
            plane(p, 1, k)
            plane(p, 2, k - 1)
        if k == 2:
            line_step(1, 3, siba, rcva)
    line_end(0, sibo, rcvo, so_ref)
    line_end(1, siba, rcva, sa_ref)
    for p in (0, 2, 1):
        plane(p, 2, 3)

    def head_rows(jj, row, n, stride, s):
        for b in range(8):
            at = row if jj is None else row + n * b
            src = fb[b if jj is None else jj, 0, at : at + 16, :]
            hbuf[pl.ds(8 * s + b, 16, stride=stride), :] = src.astype(F32)

    @pl.when((d == 0) & (i == 1))
    def _():
        for s in range(3):
            head_rows(None, geo.qr * s, geo.qr, 24, s)

    for o, n in ((3, geo.u3), (4, geo.u3), (5, geo.u2)):
        @pl.when((d == 0) & (i == o))
        def _():
            for s in range(4):
                head_rows(None, n * s, n, 32, s)

    for o, jj in ((2, 0), (6, 0), (7, 4)):
        @pl.when((d == 0) & (i == o))
        def _():
            head_rows(jj, 0, geo.ho, 8, 0)

    for e in range(q):
        to = dev(e, (i + V - 1) % V)
        tx.send((d == 0) & (i > 0), (hbuf, pl.ds(0, VECS)), tail_ref, 28, to)

    @pl.when(i == V - 1)
    def _():
        arrive((vr, pl.ds(0, V - 1)), (rsem, 26))
        tot = vp_ref[...]
        for k in range(V - 1):
            tot = tot + vr[k]
        vsum[...] = tot

    for k in range(1, q):
        tx.send(i == V - 1, vsum, (vq, k - 1), 27, dev((d + k) % q, i))

    @pl.when(i == V - 1)
    def _():
        arrive(vq, (rsem, 27))
        tot = vsum[...]
        for k in range(q - 1):
            tot = tot + vq[k]
        tail_ref[...] = tot

    @pl.when(i < V - 1)
    def _():
        arrive(tail_ref, (rsem, 28))

    for k in range(CHIPS):
        for p in (0, 2, 1):
            plane(p, 3, k)
        js = pl.ds(pair[k], 2)
        lc.copy(None, (fb, js), (f_hbm, js), ("part", k))
    tx.finish()
    lc.finish()


def main(geo, w, x, g):
    q, tl, t = geo.q, geo.tl, geo.t
    vm = pl.BlockSpec(memory_space=pltpu.VMEM)
    hbm = pl.BlockSpec(memory_space=pl.ANY)
    cos, sin = rot_tables(t)
    line = pltpu.VMEM((CHIPS, tl, D), BF16)
    lines = pltpu.VMEM((2 * CHIPS - 3, tl, D), BF16)
    vec = pltpu.VMEM((VECS, 128), F32)
    low = lambda *dims: pltpu.VMEM(dims, BF16)
    full = lambda *dims: pltpu.VMEM(dims, F32)
    return pl.pallas_call(
        partial(main_kernel, geo),
        out_shape=(
            jax.ShapeDtypeStruct((tl, D), F32),
            jax.ShapeDtypeStruct((tl, D), F32),
            jax.ShapeDtypeStruct((V, q, geo.er, 128), BF16),
            jax.ShapeDtypeStruct((VECS, 128), F32),
        ),
        in_specs=[hbm, hbm, hbm, vm, vm],
        out_specs=(vm, vm, hbm, vm),
        scratch_shapes=[
            full(HEAD + OWN + 3, 128),
            full(112, 128),
            low(V, q, geo.er, 128),
            low(VECS, 128),
            low(q, geo.zr, 128),
            low(t, D),
            low(t, D),
            low(VECS, 128),
            vec,
            full(16, D),
            low(D, 384),
            low(128, D),
            low(D, 512),
            low(512, D),
            full(t, 4),
            low(t, D),
            low(t, D),
            low(t, 128),
            low(t, 128),
            low(t, 128),
            low(t, 512),
            low(t, 512),
            low(t, 128),
            low(t, 128),
            low(t, 384),
            full(t, 128),
            full(8, D),
            vec,
            low(6, geo.zr // 2, 128) if geo.square else low(q - 1, geo.zr, 128),
            low(geo.zr, 128),
            line, line, lines, lines,
            full(V - 1, VECS, 128),
            full(q - 1, VECS, 128),
            vec,
            full(512, 128),
            pltpu.SemaphoreType.DMA((4,)),
            pltpu.SemaphoreType.DMA((150 if geo.square else 256,)),
            pltpu.SemaphoreType.DMA((geo.lines + 12,)),
            pltpu.SemaphoreType.DMA((8,)),
        ] + ([] if geo.tight else [low(t, D), low(V, q, geo.er, 128)]),
        compiler_params=pltpu.CompilerParams(
            collective_id=0, has_side_effects=True, vmem_limit_bytes=67_000_000
        ),
        name="layer",
    )(w, x, g, cos, sin)


def adam_kernel(
    geo, so_hbm, sa_hbm, x_hbm, g_hbm, tail_hbm, f_hbm, w_hbm, m_hbm, s_hbm,
    lo_ref, tg_ref, wg_hbm, nw_hbm, nm_hbm, ns_hbm, wb, mb, sb, ob, gb, fb, so_ref, sa_ref, x_ref, g_ref, lsem,
):
    _, i, _ = geo.place()
    first = (so_hbm, so_ref), (sa_hbm, sa_ref), (x_hbm, x_ref), (g_hbm, g_ref)
    then = (tail_hbm, gb.at[pl.ds(ALI, VECS)]), (f_hbm, fb)
    last = tuple((h, b.at[pl.ds(0, OWN)]) for h, b in ((w_hbm, wb), (m_hbm, mb), (s_hbm, sb)))
    loads = [pltpu.make_async_copy(h, b, lsem.at[4 + k]) for k, (h, b) in enumerate(first + then + last)]
    for ld in loads:
        ld.start()
    for ld in loads[:4]:
        ld.wait()
    x = x_ref[...].astype(F32)
    sa = sa_ref[...]
    lo_ref[...] = (x + so_ref[...]).astype(BF16)
    mid = x - jnp.mean(x, axis=1, keepdims=True)
    inv = lax.rsqrt(jnp.mean(mid * mid, axis=1, keepdims=True) + 1e-05)
    xhat = mid * inv
    dx = inv * (sa - jnp.mean(sa, axis=1, keepdims=True) - xhat * jnp.mean(sa * xhat, axis=1, keepdims=True))
    tg_ref[...] = g_ref[...].astype(F32) + dx
    for ld in loads[4:6]:
        ld.wait()
    paste_share(geo, i, gb, fb)
    for ld in loads[6:]:
        ld.wait()
    rows_n = 1024
    full = OWN // rows_n
    pairs = ((wg_hbm, ob), (nw_hbm, wb), (nm_hbm, mb), (ns_hbm, sb))

    def adam(n, carry):
        rows = pl.ds(mult(n * rows_n, rows_n), rows_n)
        adam_rows(i, rows, n * rows_n, rows_n, wb, mb, sb, ob, gb)
        for k, (h, b) in enumerate(pairs):
            pltpu.make_async_copy(b.at[rows], h.at[rows], lsem.at[k]).start()
        return carry

    lax.fori_loop(0, full, adam, 0)
    rest = OWN - full * rows_n
    adam_rows(i, pl.ds(full * rows_n, 16), full * rows_n, 16, wb, mb, sb, ob, gb)
    for k, (h, b) in enumerate(pairs):
        rows = pl.ds(full * rows_n, rest)
        pltpu.make_async_copy(b.at[rows], h.at[rows], lsem.at[k]).start()
    for k, (h, b) in enumerate(pairs):
        pltpu.make_async_copy(b.at[pl.ds(0, OWN)], h, lsem.at[k]).wait()


def adam_rows(i, rows, start, n, wb, mb, sb, ob, gb):
    g = gb[pl.ds(13 * i + start, n), :]
    w = wb[rows, :]
    m = BETA_ONE * mb[rows, :] + (1.0 - BETA_ONE) * g
    s = BETA_TWO * sb[rows, :] + (1.0 - BETA_TWO) * g * g
    ob[rows, :] = g
    mb[rows, :] = m
    sb[rows, :] = s
    mh = m * (1.0 / (1.0 - BETA_ONE**STEP))
    vh = s * (1.0 / (1.0 - BETA_TWO**STEP))
    wb[rows, :] = w - LEARN_RATE * (mh / (jnp.sqrt(vh) + EPSILON) + DECAY_RATE * w)


def paste_share(geo, i, gb, f_ref):
    q = geo.q

    def put(j, e, row, n, start, stride):
        gb[pl.ds(start, n, stride=stride), :] = f_ref[j, e, pl.ds(row, n), :].astype(F32)

    @pl.when(i < 2)
    def _():
        def body(n, c):
            e, s = n % q, n // q
            for b in range(8):
                put(b, e, mult(geo.qr * s, 16), geo.qr, 24 * geo.qr * e + 8 * s + b, 24)
            return c

        lax.fori_loop(0, 3 * q, body, 0)

    def rows_part(a0, ro, shift, count):
        def body(n, c):
            e, bl = n % q, n // q
            bb = bl + shift
            for b in range(8):
                put(
                    bb % V,
                    e,
                    mult(ro + geo.ap * (bb // V) + geo.ho * b, 16),
                    geo.ho,
                    a0 + 8 * (128 * bl + geo.ho * e) + b,
                    8,
                )
            return c

        lax.fori_loop(0, count * q, body, 0)

    def cols_part(a0, nr, ro):
        def body(n, c):
            e, t = n % q, n // q
            for b in range(8):
                put(b, e, mult(ro + nr * t, 16), nr, a0 + 32 * nr * e + 8 * t + b, 32)
            return c

        lax.fori_loop(0, 4 * q, body, 0)

    @pl.when(i == 2)
    def _():
        rows_part(0, 0, 0, 8)
        cols_part(8192, geo.u2, geo.ap)

    @pl.when((i == 3) | (i == 4))
    def _():
        cols_part(0, geo.u3, 0)

    @pl.when(i == 5)
    def _():
        cols_part(0, geo.u2, 0)
        rows_part(4096, geo.bp, 0, 8)

    @pl.when(i >= 6)
    def _():
        rows_part(0, 0, 4 * (i - 6), 12)


def adam(geo, so, sa, x, g, tail, f, w, m, s):
    tl = geo.tl
    vm = pl.BlockSpec(memory_space=pltpu.VMEM)
    hbm = pl.BlockSpec(memory_space=pl.ANY)
    flat = jax.ShapeDtypeStruct((OWN, 128), F32)
    big = pltpu.VMEM((OWN + 3, 128), F32)
    return pl.pallas_call(
        partial(adam_kernel, geo),
        out_shape=(
            jax.ShapeDtypeStruct((tl, D), BF16),
            jax.ShapeDtypeStruct((tl, D), F32),
            flat, flat, flat, flat,
        ),
        in_specs=[hbm] * 9,
        out_specs=(vm, vm, hbm, hbm, hbm, hbm),
        scratch_shapes=[
            big, big, big, big,
            pltpu.VMEM((ALI + 128, 128), F32),
            pltpu.VMEM((V, geo.q, geo.er, 128), BF16),
            pltpu.VMEM((tl, D), F32),
            pltpu.VMEM((tl, D), F32),
            pltpu.VMEM((tl, D), BF16),
            pltpu.VMEM((tl, D), BF16),
            pltpu.SemaphoreType.DMA((13,)),
        ],
        compiler_params=pltpu.CompilerParams(vmem_limit_bytes=67_000_000),
        name="adam",
    )(so, sa, x, g, tail, f, w, m, s)


def local(mesh, tokens, cotangent, weights, first_moment, second_moment):
    rep = mesh.shape["ctx"] // V
    rows = tokens.shape[1]
    x, g = tokens[0], cotangent[0]
    flats = [weights, first_moment, second_moment]
    if rep > 1:
        groups = [[rep * k + r for r in range(rep)] for k in range(V)]
        join = lambda a: lax.all_gather(a, "ctx", axis=0, axis_index_groups=groups, tiled=True)
        x, g = join(x), join(g)
        flats = [join(a) for a in flats]
    w, m, s = [a.reshape(OWN, 128) for a in flats]
    geo = Geo(mesh, x.shape[0] * V)
    so, sa, f, tail = main(geo, w, x, g)
    outs = list(adam(geo, so, sa, x, g, tail, f, w, m, s))
    outs[2:] = [a.reshape(-1) for a in outs[2:]]
    if rep > 1:
        r = lax.axis_index("ctx") % rep
        outs = [lax.dynamic_slice_in_dim(a, r * (a.shape[0] // rep), a.shape[0] // rep, 0) for a in outs]
    return (outs[0][None], outs[1][None], *outs[2:])


def solution(mesh):
    return jax.shard_map(
        partial(local, mesh),
        mesh=mesh,
        in_specs=(P("dp", "ctx", None), P("dp", "ctx", None), P("ctx"), P("ctx"), P("ctx")),
        out_specs=(P("dp", "ctx", None), P("dp", "ctx", None), P("ctx"), P("ctx"), P("ctx"), P("ctx")),
        check_vma=False,
    )
```

```python
from functools import partial
import math

import numpy as np
import jax
import jax.numpy as jnp
from jax import lax
from jax.experimental import pallas as pl
from jax.experimental.pallas import tpu as pltpu
from jax.sharding import PartitionSpec as P

D = 1024
FF = 4096
HEADS = 16
HEAD_DIM = 64
ROT = 16
STEP = 3
BETA_ONE = 0.9
BETA_TWO = 0.95
LEARN_RATE = 0.004
DECAY_RATE = 0.1
EPSILON = 1e-08

F32 = jnp.float32
BF16 = jnp.bfloat16
MESH = pl.DeviceIdType.MESH
V = 8
CHIPS = V // 2
OWN = 12301
ALI = 12288
VECS = 104
HEAD = 112
RB = 256
PARTS = 29
SPREAD = 37


class Geo:
    def __init__(self, mesh, tokens):
        self.q = mesh.shape["dp"]
        self.rep = mesh.shape["ctx"] // V
        self.tl = tokens // V
        self.t = tokens
        q = self.q
        self.qr = 512 // q
        self.ho = 128 // q
        self.u2 = 128 // q
        self.u3 = 384 // q
        self.seg = 1536 // q
        self.zr = V * self.seg
        self.ap = 1024 // q
        self.bp = 512 // q
        self.er = 2 * self.ap
        self.tight = tokens > 1024
        self.rba = RB // 2 if self.tight else RB
        self.square = q == 4
        self.ss = max(4, q - 1)
        self.sums = SPREAD + 11 * self.ss
        self.lines = self.sums + 3 * self.ss

    def place(self):
        d = lax.axis_index("dp")
        a = lax.axis_index("ctx")
        return d, a // self.rep, a % self.rep

    def dev(self, e, j, rho):
        return {"dp": e, "ctx": j * self.rep + rho}

    def up_parts(self):
        return (
            (0, self.u2, 2 * self.seg + self.ap),
            (128, self.u3, 3 * self.seg),
            (512, self.u3, 4 * self.seg),
            (896, self.u2, 5 * self.seg),
        )

    def maps(self):
        q, out = self.q, []
        for e in range(q):
            for i in range(2):
                for s in range(3):
                    out.append((e, self.seg * i + self.qr * s, self.qr, 0, 512 * i + self.qr * e, 128 * s))
            for b in range(8):
                out.append((e, 2 * self.seg + self.ho * b, self.ho, 1, self.ho * e, 128 * b))
            for r0, nr, off in self.up_parts():
                for t in range(4):
                    out.append((e, off + nr * t, nr, 2, r0 + nr * e, 128 * t))
            for t in range(4):
                for b in range(8):
                    row = 5 * self.seg + self.bp + self.ap * t + self.ho * b
                    out.append((e, row, self.ho, 3, 128 * t + self.ho * e, 128 * b))
        return out


def dot(a, b):
    return jnp.dot(a, b, preferred_element_type=F32)


def dot_nt(a, b):
    return lax.dot_general(a, b, (((1,), (1,)), ((), ())), preferred_element_type=F32)


def dot_tn(a, b):
    return lax.dot_general(a, b, (((0,), (0,)), ((), ())), preferred_element_type=F32)


def mult(x, n):
    return pl.multiple_of(x, n)


def view(part):
    return part[0].at[part[1]] if isinstance(part, tuple) else part


def rcopy(src, dst, ssem, rsem, dev):
    return pltpu.make_async_remote_copy(
        src_ref=view(src),
        dst_ref=view(dst),
        send_sem=view(ssem),
        recv_sem=view(rsem),
        device_id=dev,
        device_id_type=MESH,
    )


class Sends:
    def __init__(self, ssem, rsem, used=None):
        self.ssem, self.rsem, self.open = ssem, rsem, []
        self.used = {} if used is None else used

    def group(self):
        return Sends(self.ssem, self.rsem, self.used)

    def slot(self, key):
        return (self.ssem, self.used.setdefault(key or ("own", len(self.used)), len(self.used)))

    def send(self, cond, src, dst, rs, dev, key=None):
        slot = self.slot(key)
        make = lambda: rcopy(src, dst, slot, (self.rsem, rs), dev)
        self.when(cond, lambda: make().start())
        self.open.append((cond, lambda: make().wait_send()))

    def copy(self, cond, src, dst, key=None):
        slot = self.slot(key)
        make = lambda: pltpu.make_async_copy(view(src), view(dst), view(slot))
        self.when(cond, lambda: make().start())
        self.open.append((cond, lambda: make().wait()))

    def block(self, cond, act):
        inner = self.group()
        self.when(cond, lambda: act(inner))
        if inner.open:

            def end():
                for _, wait in inner.open:
                    wait()

            self.open.append((cond, end))

    @staticmethod
    def when(cond, act):
        if cond is None:
            act()
        else:
            pl.when(cond)(act)

    def finish(self):
        for cond, act in self.open:
            self.when(cond, act)
        self.open.clear()


def arrive(part, sem):
    pltpu.make_async_copy(view(part), view(part), view(sem)).wait()


def entry_barrier(geo, d, i, rho):
    sem = pltpu.get_barrier_semaphore()
    for k in range(1, V):
        pl.semaphore_signal(sem, inc=1, device_id=geo.dev(d, (i + k) % V, rho), device_id_type=MESH)
    for k in range(1, geo.q):
        pl.semaphore_signal(sem, inc=1, device_id=geo.dev((d + k) % geo.q, i, rho), device_id_type=MESH)
    pl.semaphore_wait(sem, V - 1 + geo.q - 1)


def cut_share(geo, i, buf, e_ref):
    q, base = geo.q, HEAD - 13 * i

    def put(j, e, row, n, start, stride):
        e_ref[j, e, pl.ds(row, n), :] = buf[pl.ds(start, n, stride=stride), :].astype(BF16)

    @pl.when(i < 2)
    def _():
        def body(n, c):
            e, s = n % q, n // q
            for b in range(8):
                put(b, e, mult(geo.qr * s, 16), geo.qr, base + 24 * geo.qr * e + 8 * s + b, 24)
            return c

        lax.fori_loop(0, 3 * q, body, 0)

    def rows_part(a0, ro, shift, count):
        def body(n, c):
            e, bl = n % q, n // q
            bb = bl + shift
            for b in range(8):
                put(
                    bb % V,
                    e,
                    mult(ro + geo.ap * (bb // V) + geo.ho * b, 16),
                    geo.ho,
                    base + a0 + 8 * (128 * bl + geo.ho * e) + b,
                    8,
                )
            return c

        lax.fori_loop(0, count * q, body, 0)

    def cols_part(a0, nr, ro):
        def body(n, c):
            e, t = n % q, n // q
            for b in range(8):
                put(b, e, mult(ro + nr * t, 16), nr, base + a0 + 32 * nr * e + 8 * t + b, 32)
            return c

        lax.fori_loop(0, 4 * q, body, 0)

    @pl.when(i == 2)
    def _():
        rows_part(0, 0, 0, 8)
        cols_part(8192, geo.u2, geo.ap)

    @pl.when((i == 3) | (i == 4))
    def _():
        cols_part(0, geo.u3, 0)

    @pl.when(i == 5)
    def _():
        cols_part(0, geo.u2, 0)
        rows_part(4096, geo.bp, 0, 8)

    @pl.when(i >= 6)
    def _():
        rows_part(0, 0, 4 * (i - 6), 12)


def owner_moves(geo, i, j):
    k = i - 6
    return (
        (i < 6, 0, mult(geo.seg * i, 16), geo.seg),
        (i >= 6, mult(geo.ap * k, 16), mult(6 * geo.seg + 2 * geo.ap * k, 16), geo.ap),
        ((i >= 6) & (j // 4 == k), mult(geo.ap * (1 - k), 16), 6 * geo.seg + geo.ap, geo.ap),
    )


def sib_owner_rows(geo, sib, z_ref, sem):
    _, i, _ = geo.place()

    @pl.when(sib < 6)
    def _():
        arrive((z_ref, (slice(None), pl.ds(0, geo.seg))), sem)

    @pl.when((sib >= 6) & (i // 4 == sib - 6))
    def _():
        arrive((z_ref, (slice(None), pl.ds(0, 2 * geo.ap))), sem)

    @pl.when((sib >= 6) & (i // 4 != sib - 6))
    def _():
        arrive((z_ref, (slice(None), pl.ds(0, geo.ap))), sem)


def rot_tables(t):
    half = ROT // 2
    freq = (10000.0 ** (-2.0 * np.arange(half, dtype=np.float32) / ROT)).astype(np.float32)
    ang = np.arange(t, dtype=np.float32)[:, None] * freq[None, :]
    cos = np.ones((t, 128), np.float32)
    sin = np.zeros((t, 128), np.float32)
    for h in range(2):
        for k in range(2):
            lo = 64 * h + half * k
            cos[:, lo : lo + half] = np.cos(ang)
            sin[:, lo : lo + half] = np.sin(ang) * (1 if k else -1)
    return jnp.asarray(cos), jnp.asarray(sin)


def rot(v, cos, sin, lane, back):
    up = pltpu.roll(v, 120, 1)
    down = pltpu.roll(v, 8, 1)
    partner = jnp.where(lane % 16 < 8, up, down)
    turn = partner * sin
    return v * cos - turn if back else v * cos + turn


def main_kernel(
    geo, w_hbm, xin, gin, cos_hbm, sin_hbm, so_hbm, sa_hbm, f_hbm, tail_ref,
    cos_ref, sin_ref, so_ref, sa_ref,
    buf, hb, e_ref, vs, z_ref, x_ref, g_ref, v_ref,
    vf, rowv, wq, wo, wu, wd, xh, n1, n2, qs, ks, vv, hid, du, ob, do, dqkv, dqs, acc, vp_ref,
    rb_ref, rz, sibo, siba, rcvo, rcva, vr, vq, vsum, hbuf, lsem, ssem, rsem, csem, *spare,
):
    gz_ref = z_ref
    po_ref, fb = (g_ref, e_ref) if geo.tight else spare
    q, tl, t = geo.q, geo.tl, geo.t
    seg, ap, bp = geo.seg, geo.ap, geo.bp
    d, i, rho = geo.place()
    j = i
    z, c = i // 2, i % 2
    sib = 2 * z + 1 - c
    near = (None, d - d % 2 + (1 - d % 2), (d + 2) % 4, 3 - d)
    rank = [(d + k) % q for k in range(q)]
    dev = partial(geo.dev, rho=rho)
    peers = [dev(e, i) for e in ((d, *near[1:]) if geo.square else rank)]
    early = Sends(ssem, rsem, dict.fromkeys(range(8)))
    tx = Sends(ssem, rsem)
    lc = Sends(csem, None)
    whole = slice(None)

    def spread_one(tx, part, sem, key):
        for k in (1, 2) if geo.square else range(1, q):
            tx.send(None, part(d, None), part(d, None), sem + k - 1, peers[k], (key, 1, k))

    def spread_two(tx, part, sem, key):
        if geo.square:
            for k in (1, 2):
                arrive(part(near[k], None), (rsem, sem + k - 1))
                half = part(near[k], k - 1)
                tx.send(None, half, half, sem + 1 + k, peers[3 - k], (key, 2, k))

    def spread_three(part, sem):
        if geo.square:
            for k in (1, 2):
                arrive(part(near[3], k - 1), (rsem, sem + 1 + k))
        else:
            for k in range(1, q):
                arrive(part(rank[q - k], None), (rsem, sem + k - 1))

    load = pltpu.make_async_copy(w_hbm, buf.at[pl.ds(HEAD, OWN)], lsem.at[0])
    load.start()
    rows_own = pl.ds(mult(i * tl, 16), tl)
    own = [
        pltpu.make_async_copy(xin, x_ref.at[rows_own], lsem.at[1]),
        pltpu.make_async_copy(gin, g_ref.at[rows_own], lsem.at[2]),
        pltpu.make_async_copy(cos_hbm, cos_ref, lsem.at[3]),
        pltpu.make_async_copy(sin_hbm, sin_ref, lsem.at[4]),
    ]
    for cp in own:
        cp.start()
    entry_barrier(geo, d, i, rho)
    halo = pl.ds(OWN - 109, 109)
    early.send(i < V - 1, (w_hbm, halo), (hb, pl.ds(0, 109)), 0, dev(d, (i + 1) % V))

    def chain(a, src, ref):
        dst = (ref, rows_own)
        early.send(z < CHIPS - 1, src, dst, 4 + 6 * a, dev(d, (i + 2) % V))
        early.send(z > 0, src, dst, 7 + 6 * a, dev(d, (i + V - 2) % V))
        early.send(None, src, dst, 2 + a, dev(d, sib))

    def hop(a, ref, k, last):
        for s, sign in ((0, 1), (1, -1)):
            there = (z >= k + 1) if sign == 1 else (z + k + 1 < CHIPS)
            on = (z < CHIPS - 1) if sign == 1 else (z > 0)
            ok = there & jnp.logical_not(on) if last else there & on
            src_i = (i - 2 * sign * (k + 1) + 2 * V) % V
            rs = 4 + 6 * a + 3 * s + k
            part = (ref, pl.ds(mult(src_i * tl, 16), tl))

            @pl.when(ok)
            def _():
                arrive(part, (rsem, rs))

            if not last:
                early.send(ok, part, part, rs + 1, dev(d, (i + 2 * sign + V) % V))
            early.send(ok, part, part, 2 + a, dev(d, sib), ("hop", a, k, s))

    def relay(a, ref, k):
        hop(a, ref, k, False)

    def end_of_line(a, ref):
        for k in range(CHIPS - 1):
            hop(a, ref, k, True)

    chain(0, xin, x_ref)
    load.wait()

    @pl.when(i > 0)
    def _():
        arrive((hb, pl.ds(0, 109)), (rsem, 0))
        buf[pl.ds(HEAD - 104, 104), :] = hb[pl.ds(5, 104), :]

    @pl.when(i == V - 1)
    def _():
        vs[...] = buf[pl.ds(HEAD + OWN - VECS, VECS), :].astype(BF16)
        v_ref[...] = vs[...]

    cut_share(geo, i, buf, e_ref)

    def slices_to(k):
        tx = early.group()
        for cc in range(2):
            to = (2 * (z + k) + cc) % V
            for m, (ok, erow, zrow, n) in enumerate(owner_moves(geo, i, to)):
                src = (e_ref, (to, d, pl.ds(erow, n)))
                tx.send(ok, src, (z_ref, (d, pl.ds(zrow, n))), 16 + k, dev(d, to), ("slice", k, cc, m // 2))
        return tx

    def slices_of(k):
        base = ((z + CHIPS - k) % CHIPS) * 2 * seg

        def part(e, half):
            at, n = (base, 2 * seg) if half is None else (base + half * seg, seg)
            return (z_ref, (e, pl.ds(mult(at, 16), n)))

        return part, SPREAD + geo.ss * (k - 1), ("slices", k)

    first = slices_to(1)
    for k in range(1, V):
        early.send(i == V - 1, vs, v_ref, 1, dev(d, (i + k) % V))
    for m, (ok, erow, zrow, n) in enumerate(owner_moves(geo, i, sib)):
        src = (e_ref, (sib, whole, pl.ds(erow, n)))
        early.send(ok, src, (z_ref, (whole, pl.ds(zrow, n))), 16, dev(d, sib), ("slice", 0, 0, m // 2))
    for m, (ok, erow, zrow, n) in enumerate(owner_moves(geo, i, i)):
        lc.copy(ok, (e_ref, (i, whole, pl.ds(erow, n))), (z_ref, (whole, pl.ds(zrow, n))), ("own", m // 2))
    first.finish()
    second = slices_to(2)
    relay(0, x_ref, 0)
    arrive((z_ref, (0, pl.ds(0, 2 * seg))), (rsem, 17))
    spread_one(early, *slices_of(1))
    second.finish()
    third = slices_to(3)
    arrive((z_ref, (0, pl.ds(0, 2 * seg))), (rsem, 18))
    spread_one(early, *slices_of(2))
    relay(0, x_ref, 1)
    chain(1, gin, g_ref)
    arrive((z_ref, (0, pl.ds(0, 2 * seg))), (rsem, 19))
    spread_one(early, *slices_of(3))
    relay(1, g_ref, 0)
    spread_two(early, *slices_of(1))
    spread_two(early, *slices_of(2))
    for cp in own:
        cp.wait()

    @pl.when(i < V - 1)
    def _():
        arrive(v_ref, (rsem, 1))

    nrb = t // RB
    vf[...] = v_ref[...].astype(F32)
    for k in range(9):
        for b in range(8):
            rowv[k : k + 1, 128 * b : 128 * b + 128] = vf[8 * k + b : 8 * k + b + 1, :]
    acc[...] = jnp.zeros_like(acc)
    vp_ref[...] = jnp.zeros_like(vp_ref)
    gp = lambda b, r: pl.ds(mult(b * t + r * RB, RB), RB)
    kv0, kv1 = 4 * t, 5 * t
    buf[kv0 : kv0 + 2 * t, :] = jnp.zeros((2 * t, 128), F32)

    def rb_of(r):
        return pl.ds(mult(r * RB, RB), RB)

    lane = lax.broadcasted_iota(jnp.int32, (RB, 128), 1)
    end_of_line(0, x_ref)
    arrive((x_ref, pl.ds(0, CHIPS * tl)), (rsem, 2))

    def norms(r, carry):
        rb = rb_of(r)
        x = x_ref[rb, :].astype(F32)
        mean = jnp.mean(x, axis=1, keepdims=True)
        mid = x - mean
        var = jnp.mean(mid * mid, axis=1, keepdims=True)
        inv = lax.rsqrt(var + 1e-05)
        xhat = mid * inv
        xh[rb, 0:1] = mean
        xh[rb, 1:2] = inv
        n1[rb, :] = (xhat * rowv[0:1, :] + rowv[1:2, :]).astype(BF16)
        n2[rb, :] = (xhat * rowv[2:3, :] + rowv[3:4, :]).astype(BF16)
        return carry

    spread_two(early, *slices_of(3))
    lax.fori_loop(0, nrb, norms, 0)
    relay(1, g_ref, 1)
    sib_owner_rows(geo, sib, z_ref, (rsem, 16))
    lc.finish()
    for k in range(1, CHIPS):
        spread_three(*slices_of(k)[:2])
    mats = (wq, wo, wu, wd)
    for e, zrow, n, m, row, ln in geo.maps():
        mats[m][row : row + n, ln : ln + 128] = z_ref[e, zrow : zrow + n, :]

    def forward(r, carry):
        rb = rb_of(r)
        qkv = dot(n1[rb, :], wq[...])
        cos, sin = cos_ref[rb, :], sin_ref[rb, :]
        qh = qkv[:, 0:128] + vf[pl.ds(32 + j, 1), :]
        kh = qkv[:, 128:256] + vf[pl.ds(40 + j, 1), :]
        vh = qkv[:, 256:384] + vf[pl.ds(48 + j, 1), :]
        qs[rb, :] = (rot(qh, cos, sin, lane, False) * 0.125).astype(BF16)
        ks[rb, :] = rot(kh, cos, sin, lane, False).astype(BF16)
        vv[rb, :] = vh.astype(BF16)
        up = dot(n2[rb, :], wu[...])
        for b in range(4):
            cols = slice(128 * b, 128 * b + 128)
            u = up[:, cols] + vf[pl.ds(72 + 8 * b + j, 1), :]
            phi = 0.5 + 0.5 * lax.erf(u * (1.0 / math.sqrt(2.0)))
            hid[rb, cols] = (u * phi).astype(BF16)
            buf[gp(b, r), :] = phi + u * (jnp.exp(-0.5 * u * u) * (1.0 / math.sqrt(2.0 * math.pi)))
        return carry

    lax.fori_loop(0, nrb, forward, 0)

    ra = geo.rba
    left = lax.broadcasted_iota(jnp.int32, (ra, 128), 1) < 64
    diag = lax.broadcasted_iota(jnp.int32, (ra, ra), 0) >= lax.broadcasted_iota(jnp.int32, (ra, ra), 1)
    zero = jnp.zeros((), BF16)

    def mine(h, v):
        return jnp.where(left if h == 0 else jnp.logical_not(left), v, zero)

    def scores(r, qm):
        n = (r + 1) * ra
        s = dot_nt(qm, ks[0:n, :])
        tail = jnp.where(diag, s[:, n - ra : n], -1e30)
        return tail if r == 0 else jnp.concatenate([s[:, : n - ra], tail], axis=1)

    for r in range(t // ra):
        rb, n = slice(r * ra, r * ra + ra), (r + 1) * ra
        outs = []
        for h in range(2):
            s = scores(r, mine(h, qs[rb, :]))
            top = jnp.max(s, axis=1, keepdims=True)
            ex = jnp.exp(s - top)
            tot = jnp.sum(ex, axis=1, keepdims=True)
            xh[rb, 2 + h : 3 + h] = top + jnp.log(tot)
            outs.append(dot((ex * (1.0 / tot)).astype(BF16), vv[0:n, :]))
        ob[rb, :] = jnp.where(left, outs[0], outs[1]).astype(BF16)

    def outputs(r, carry):
        rb = rb_of(r)
        po_ref[rb, :] = (dot(hid[rb, :], wd[...]) + dot(ob[rb, :], wo[...])).astype(BF16)
        return carry

    def to_sibling(a, part, sums):
        for k in range(CHIPS):
            rows = pl.ds(mult((2 * k + 1 - c) * tl, 16), tl)
            tx.send(None, (part, rows), (sums, k), 20 + a, dev(d, sib))

    def line_rows(a, part, sums):
        arrive(sums, (rsem, 20 + a))
        for k in range(CHIPS):
            rows = pl.ds(mult((2 * k + c) * tl, 16), tl)
            sums[k] = (part[rows, :].astype(F32) + sums[k].astype(F32)).astype(BF16)

    def slot_of(s, step):
        return 2 * (step - 1) - 1 + s if step > 1 else 0

    def line_step(a, step, sums, got):
        for s, sign in ((0, 1), (1, -1)):
            far = z if sign == 1 else CHIPS - 1 - z
            ok = far < step
            dest = z + sign * (CHIPS - step)
            rs = geo.lines + 6 * a + 3 * s + step - 1
            if step > 1:

                @pl.when(ok & (far > 0))
                def _():
                    at = slot_of(s, step - 1)
                    arrive((got, at), (rsem, rs - 1))
                    sums[dest] = (sums[dest].astype(F32) + got[at].astype(F32)).astype(BF16)

            tx.send(ok, (sums, dest), (got, slot_of(s, step)), rs, dev(d, (i + 2 * sign + V) % V))

    def line_end(a, sums, got, out):
        tot = sums[z].astype(F32)
        if a == 0:
            tot = tot + (rowv[7:8, :] + rowv[8:9, :])
        out[...] = tot
        for s, more in ((0, z > 0), (1, z < CHIPS - 1)):

            @pl.when(more)
            def _():
                at = slot_of(s, 3)
                arrive((got, at), (rsem, geo.lines + 6 * a + 3 * s + 2))
                out[...] += got[at].astype(F32)

    if not geo.tight:
        lax.fori_loop(0, nrb, outputs, 0)
        to_sibling(0, po_ref, sibo)
    end_of_line(1, g_ref)
    arrive((g_ref, pl.ds(0, CHIPS * tl)), (rsem, 3))

    if not geo.tight:
        line_rows(0, po_ref, sibo)
        line_step(0, 1, sibo, rcvo)
    def grad_heads(r, carry):
        rb = rb_of(r)
        do[rb, :] = dot_nt(g_ref[rb, :], wo[...]).astype(BF16)
        return carry

    lax.fori_loop(0, nrb, grad_heads, 0)

    def back_mlp(r, carry):
        rb = rb_of(r)
        g = g_ref[rb, :]
        dh = dot_nt(g, wd[...])
        for b in range(4):
            cols = slice(128 * b, 128 * b + 128)
            low = (dh[:, cols] * buf[gp(b, r), :]).astype(BF16)
            du[rb, cols] = low
            acc[5:6, cols] += jnp.sum(low.astype(F32), axis=0, keepdims=True)
        acc[4:5, :] += jnp.sum(g.astype(F32), axis=0, keepdims=True)
        return carry

    lax.fori_loop(0, nrb, back_mlp, 0)

    third.finish()
    early.finish()
    pc = 4096 // q
    ph = pc // 2

    def grad_down(k, carry):
        res = dot_tn(hid[:, pl.ds(mult(k * 256, 256), 256)], g_ref[...]).astype(BF16)
        for h in range(2):
            row = 5 * seg + bp + ap * (2 * k + h)
            for e in range(q):
                for b in range(8):
                    r0 = 128 * h + geo.ho * e
                    block = res[r0 : r0 + geo.ho, 128 * b : 128 * b + 128]
                    gz_ref[e, pl.ds(mult(row + geo.ho * b, 16), geo.ho), :] = block
        return carry

    def halves(p, h):
        return pl.ds(p * pc + h * ph, ph), pl.ds(p * ph, ph)

    def sum_one(p):
        sem = geo.sums + geo.ss * p
        if geo.square:
            for k in (1, 2):
                rows, at = halves(p, k - 1)
                for slot, e in enumerate((near[k], near[3])):
                    dst = (rb_ref, (2 * (k - 1) + slot, at))
                    tx.send(None, (gz_ref, (e, rows)), dst, sem + k - 1, dev(near[k], i))
        else:
            rows = pl.ds(p * pc, pc)
            for k in range(1, q):
                e = (d + k) % q
                tx.send(None, (gz_ref, (e, rows)), (rb_ref, (k - 1, rows)), sem + k - 1, dev(e, i))

    def sum_two(p):
        sem = geo.sums + geo.ss * p
        if geo.square:
            for k in (1, 2):
                rows, at = halves(p, k - 1)
                arrive((rb_ref, (pl.ds(2 * (k - 1), 2), at)), (rsem, sem + k - 1))
                mid = 2 * (k - 1) + 1
                tot = gz_ref[near[3 - k], rows, :].astype(F32) + rb_ref[mid, at, :].astype(F32)
                rb_ref[mid, at, :] = tot.astype(BF16)
                tx.send(None, (rb_ref, (mid, at)), (rb_ref, (3 + k, at)), sem + 1 + k, dev(near[3 - k], i))

    def sum_three(p):
        sem = geo.sums + geo.ss * p
        if geo.square:
            for k in (1, 2):
                rows, at = halves(p, k - 1)
                arrive((rb_ref, (3 + k, at)), (rsem, sem + 1 + k))
                tot = gz_ref[d, rows, :].astype(F32) + rb_ref[2 * (k - 1), at, :].astype(F32)
                rz[rows, :] = (tot + rb_ref[3 + k, at, :].astype(F32)).astype(BF16)
        else:
            rows = pl.ds(p * pc, pc)
            for k in range(1, q):
                arrive((rb_ref, (k - 1, rows)), (rsem, sem + k - 1))
            tot = gz_ref[d, rows, :].astype(F32)
            for k in range(q - 1):
                tot = tot + rb_ref[k, rows, :].astype(F32)
            rz[rows, :] = tot.astype(BF16)

    moves = (
        ((0, 0, 0, seg, 0), (1, seg, 0, seg, 0), (2, 2 * seg, 0, ap, 0)),
        (
            (2, 2 * seg + ap, ap, bp, 1),
            (3, 3 * seg, 0, seg, 1),
            (4, 4 * seg, 0, seg, 1),
            (5, 5 * seg, 0, bp, 1),
        ),
        ((5, 5 * seg + bp, bp, ap, 2), (6, 6 * seg, 0, ap, 2), (7, 6 * seg + 2 * ap, ap, ap, 2)),
    )

    chip = [(z + k) % CHIPS for k in range(CHIPS)]
    pair = [mult(2 * at, 2) for at in chip]
    single = [(2 * at, 2 * at + 1) for at in chip]

    def to_owners(p):
        sum_three(p)
        for o, zrow, frow, n, kind in moves[p]:
            src, dst = (rz, pl.ds(zrow, n)), (fb, (i, d, pl.ds(frow, n)))
            tx.send(i != o, src, dst, PARTS + 4 * (kind % 2) + (z + CHIPS - o // 2) % CHIPS, dev(d, o))
            lc.copy(i == o, src, dst, ("part", kind))
        if p == 2:
            for o in (6, 7):
                here = i // 4 == o - 6
                src, dst = (rz, pl.ds(6 * seg + ap, ap)), (fb, (i, d, pl.ds(ap * (7 - o), ap)))
                rs = PARTS + 4 + (z + CHIPS - o // 2) % CHIPS
                tx.send(here & (i != o), src, dst, rs, dev(d, o), ("last", 0))
                lc.copy(here & (i == o), src, dst, ("part", 3))

    def held(p, k):
        out = [(o, frow, n, kind) for o, _, frow, n, kind in moves[p]]
        if p == 2:
            out += [(6, ap, ap, 3)] if k in (1, 2) else [(7, 0, ap, 3)]
        return out

    def plane(p, stage, k):
        if stage == 1 and k == 0:
            lc.finish()
        for o, frow, n, kind in held(p, k):

            def part(e, half):
                js = pl.ds(pair[k], 2) if half is None else single[k][half]
                return (fb, (js, e, pl.ds(frow, n)))

            sem, key = SPREAD + geo.ss * (3 + 4 * (kind % 2) + k), ("held", kind % 2, k)

            def act(tx):
                if stage == 1:
                    arrive((fb, (pl.ds(0, 2 if k else 1), 0, pl.ds(frow, n))), (rsem, PARTS + 4 * (kind % 2) + k))
                    spread_one(tx, part, sem, key)
                elif stage == 2:
                    spread_two(tx, part, sem, key)
                else:
                    spread_three(part, sem)

            tx.block(i == o, act)

    lax.fori_loop(0, 2, grad_down, 0)
    sum_one(2)

    for r in range(t // ra):
        rb, n = slice(r * ra, r * ra + ra), (r + 1) * ra
        dqh = []
        for h in range(2):
            qm, gm = mine(h, qs[rb, :]), mine(h, do[rb, :])
            prob = jnp.exp(scores(r, qm) - xh[rb, 2 + h : 3 + h])
            dp = dot_nt(gm, vv[0:n, :])
            delta = jnp.sum(prob * dp, axis=1, keepdims=True)
            ds = (prob * (dp - delta)).astype(BF16)
            dqh.append(dot(ds, ks[0:n, :]))
            buf[kv0 : kv0 + n, :] += dot_tn(ds, qm)
            buf[kv1 : kv1 + n, :] += dot_tn(prob.astype(BF16), gm)
        dqs[rb, :] = jnp.where(left, dqh[0], dqh[1])

    sum_two(2)
    if not geo.tight:
        line_step(0, 2, sibo, rcvo)

    def back_one(r, carry):
        rb = rb_of(r)
        cos, sin = cos_ref[rb, :], sin_ref[rb, :]
        low = jnp.concatenate(
            [
                (rot(dqs[rb, :], cos, sin, lane, True) * 0.125).astype(BF16),
                rot(buf[pl.ds(mult(kv0 + r * RB, RB), RB), :], cos, sin, lane, True).astype(BF16),
                buf[pl.ds(mult(kv1 + r * RB, RB), RB), :].astype(BF16),
            ],
            axis=1,
        )
        dqkv[rb, :] = low
        acc[6:7, 0:384] += jnp.sum(low.astype(F32), axis=0, keepdims=True)
        return carry

    lax.fori_loop(0, nrb, back_one, 0)
    res = dot_tn(ob[...], g_ref[...]).astype(BF16)
    for e in range(q):
        for b in range(8):
            row = 2 * seg + geo.ho * b
            gz_ref[e, row : row + geo.ho, :] = res[geo.ho * e : geo.ho * e + geo.ho, 128 * b : 128 * b + 128]
    for k in range(2):
        res = dot_tn(n1[:, 512 * k : 512 * k + 512], dqkv[...]).astype(BF16)
        for e in range(q):
            for b in range(3):
                row = seg * k + geo.qr * b
                block = res[geo.qr * e : geo.qr * e + geo.qr, 128 * b : 128 * b + 128]
                gz_ref[e, row : row + geo.qr, :] = block
    sum_one(0)
    to_owners(2)
    plane(2, 1, 0)
    if not geo.tight:
        line_step(0, 3, sibo, rcvo)

    def back_two(r, carry):
        rb = rb_of(r)
        xhat = (x_ref[rb, :].astype(F32) - xh[rb, 0:1]) * xh[rb, 1:2]
        d1 = dot_nt(dqkv[rb, :], wq[...])
        acc[0:1, :] += jnp.sum(d1 * xhat, axis=0, keepdims=True)
        acc[1:2, :] += jnp.sum(d1, axis=0, keepdims=True)
        d2 = dot_nt(du[rb, :], wu[...])
        acc[2:3, :] += jnp.sum(d2 * xhat, axis=0, keepdims=True)
        acc[3:4, :] += jnp.sum(d2, axis=0, keepdims=True)
        x_ref[rb, :] = (d1 * rowv[0:1, :] + d2 * rowv[2:3, :]).astype(BF16)
        return carry

    lax.fori_loop(0, nrb, back_two, 0)
    to_sibling(1, x_ref, siba)
    for r0, nr, off in geo.up_parts():
        res = dot_tn(n2[:, r0 : r0 + q * nr], du[...]).astype(BF16)
        for e in range(q):
            for b in range(4):
                gz_ref[e, off + nr * b : off + nr * b + nr, :] = res[nr * e : nr * e + nr, 128 * b : 128 * b + 128]
    sum_two(0)
    sum_one(1)
    if geo.tight:
        lax.fori_loop(0, nrb, outputs, 0)
        to_sibling(0, po_ref, sibo)
        line_rows(0, po_ref, sibo)
        line_step(0, 1, sibo, rcvo)
        line_step(0, 2, sibo, rcvo)
        line_step(0, 3, sibo, rcvo)
    line_rows(1, x_ref, siba)
    line_step(1, 1, siba, rcva)
    to_owners(0)
    plane(0, 1, 0)
    sum_two(1)
    plane(2, 1, 1)
    plane(2, 2, 0)
    to_owners(1)
    line_step(1, 2, siba, rcva)
    plane(1, 1, 0)
    plane(0, 1, 1)
    plane(0, 2, 0)
    plane(1, 1, 1)
    plane(1, 2, 0)
    zeroth = jnp.where(j == 0, 1.0, 0.0)
    for b in range(8):
        cols = slice(128 * b, 128 * b + 128)
        for k in range(4):
            vp_ref[8 * k + b : 8 * k + b + 1, :] = acc[k : k + 1, cols]
        for k in (7, 8):
            vp_ref[8 * k + b : 8 * k + b + 1, :] = acc[4:5, cols] * zeroth
    for k in range(3):
        vp_ref[pl.ds(32 + 8 * k + j, 1), :] = acc[6:7, 128 * k : 128 * k + 128]
    for k in range(4):
        vp_ref[pl.ds(72 + 8 * k + j, 1), :] = acc[5:6, 128 * k : 128 * k + 128]
    tx.send(i < V - 1, vp_ref, (vr, i), 26, dev(d, V - 1))
    for k in (2, 3):
        for p in (2, 0, 1):
            plane(p, 1, k)
            plane(p, 2, k - 1)
        if k == 2:
            line_step(1, 3, siba, rcva)
    line_end(0, sibo, rcvo, so_ref)
    line_end(1, siba, rcva, sa_ref)
    lc.copy(None, so_ref, so_hbm, ("out", 0))
    lc.copy(None, sa_ref, sa_hbm, ("out", 1))
    for p in (0, 2, 1):
        plane(p, 2, 3)

    def head_rows(jj, row, n, stride, s):
        for b in range(8):
            at = row if jj is None else row + n * b
            src = fb[b if jj is None else jj, 0, at : at + 16, :]
            hbuf[pl.ds(8 * s + b, 16, stride=stride), :] = src.astype(F32)

    @pl.when((d == 0) & (i == 1))
    def _():
        for s in range(3):
            head_rows(None, geo.qr * s, geo.qr, 24, s)

    for o, n in ((3, geo.u3), (4, geo.u3), (5, geo.u2)):
        @pl.when((d == 0) & (i == o))
        def _():
            for s in range(4):
                head_rows(None, n * s, n, 32, s)

    for o, jj in ((2, 0), (6, 0), (7, 4)):
        @pl.when((d == 0) & (i == o))
        def _():
            head_rows(jj, 0, geo.ho, 8, 0)

    for e in range(q):
        to = dev(e, (i + V - 1) % V)
        tx.send((d == 0) & (i > 0), (hbuf, pl.ds(0, VECS)), tail_ref, 28, to)

    @pl.when(i == V - 1)
    def _():
        arrive((vr, pl.ds(0, V - 1)), (rsem, 26))
        tot = vp_ref[...]
        for k in range(V - 1):
            tot = tot + vr[k]
        vsum[...] = tot

    for k in range(1, q):
        tx.send(i == V - 1, vsum, (vq, k - 1), 27, dev((d + k) % q, i))

    @pl.when(i == V - 1)
    def _():
        arrive(vq, (rsem, 27))
        tot = vsum[...]
        for k in range(q - 1):
            tot = tot + vq[k]
        tail_ref[...] = tot

    @pl.when(i < V - 1)
    def _():
        arrive(tail_ref, (rsem, 28))

    for k in range(CHIPS):
        for p in (0, 2, 1):
            plane(p, 3, k)
        js = pl.ds(pair[k], 2)
        lc.copy(None, (fb, js), (f_hbm, js), ("part", k))
    tx.finish()
    lc.finish()


def main(geo, w, x, g):
    q, tl, t = geo.q, geo.tl, geo.t
    vm = pl.BlockSpec(memory_space=pltpu.VMEM)
    hbm = pl.BlockSpec(memory_space=pl.ANY)
    cos, sin = rot_tables(t)
    line = pltpu.VMEM((CHIPS, tl, D), BF16)
    lines = pltpu.VMEM((2 * CHIPS - 3, tl, D), BF16)
    vec = pltpu.VMEM((VECS, 128), F32)
    low = lambda *dims: pltpu.VMEM(dims, BF16)
    full = lambda *dims: pltpu.VMEM(dims, F32)
    return pl.pallas_call(
        partial(main_kernel, geo),
        out_shape=(
            jax.ShapeDtypeStruct((tl, D), F32),
            jax.ShapeDtypeStruct((tl, D), F32),
            jax.ShapeDtypeStruct((V, q, geo.er, 128), BF16),
            jax.ShapeDtypeStruct((VECS, 128), F32),
        ),
        in_specs=[hbm] * 5,
        out_specs=(hbm, hbm, hbm, vm),
        scratch_shapes=[
            full(t, 128),
            full(t, 128),
            full(tl, D),
            full(tl, D),
            full(HEAD + OWN + 3, 128),
            full(112, 128),
            low(V, q, geo.er, 128),
            low(VECS, 128),
            low(q, geo.zr, 128),
            low(t, D),
            low(t, D),
            low(VECS, 128),
            vec,
            full(16, D),
            low(D, 384),
            low(128, D),
            low(D, 512),
            low(512, D),
            full(t, 4),
            low(t, D),
            low(t, D),
            low(t, 128),
            low(t, 128),
            low(t, 128),
            low(t, 512),
            low(t, 512),
            low(t, 128),
            low(t, 128),
            low(t, 384),
            full(t, 128),
            full(8, D),
            vec,
            low(6, geo.zr // 2, 128) if geo.square else low(q - 1, geo.zr, 128),
            low(geo.zr, 128),
            line, line, lines, lines,
            full(V - 1, VECS, 128),
            full(q - 1, VECS, 128),
            vec,
            full(512, 128),
            pltpu.SemaphoreType.DMA((5,)),
            pltpu.SemaphoreType.DMA((92 if geo.square else 256,)),
            pltpu.SemaphoreType.DMA((geo.lines + 12,)),
            pltpu.SemaphoreType.DMA((8,)),
        ] + ([] if geo.tight else [low(t, D), low(V, q, geo.er, 128)]),
        compiler_params=pltpu.CompilerParams(
            collective_id=0, has_side_effects=True, vmem_limit_bytes=67_000_000
        ),
        name="layer",
    )(w, x, g, cos, sin)


def adam_kernel(
    geo, so_hbm, sa_hbm, x_hbm, g_hbm, tail_hbm, f_hbm, w_hbm, m_hbm, s_hbm,
    lo_ref, tg_ref, wg_hbm, nw_hbm, nm_hbm, ns_hbm, wb, mb, sb, ob, gb, fb, so_ref, sa_ref, x_ref, g_ref, lsem,
):
    _, i, _ = geo.place()
    first = (so_hbm, so_ref), (sa_hbm, sa_ref), (x_hbm, x_ref), (g_hbm, g_ref)
    then = (tail_hbm, gb.at[pl.ds(ALI, VECS)]), (f_hbm, fb)
    loads = [pltpu.make_async_copy(h, b, lsem.at[4 + k]) for k, (h, b) in enumerate(first + then)]
    cuts = [4096 * k for k in range(OWN // 4096 + 1)] + [OWN]
    parts = [
        [
            pltpu.make_async_copy(h.at[pl.ds(lo, hi - lo)], b.at[pl.ds(lo, hi - lo)], lsem.at[10 + 3 * n + k])
            for k, (h, b) in enumerate(((w_hbm, wb), (m_hbm, mb), (s_hbm, sb)))
        ]
        for n, (lo, hi) in enumerate(zip(cuts, cuts[1:]))
    ]
    for ld in loads + sum(parts, []):
        ld.start()
    for ld in loads[:4]:
        ld.wait()
    x = x_ref[...].astype(F32)
    sa = sa_ref[...]
    lo_ref[...] = (x + so_ref[...]).astype(BF16)
    mid = x - jnp.mean(x, axis=1, keepdims=True)
    inv = lax.rsqrt(jnp.mean(mid * mid, axis=1, keepdims=True) + 1e-05)
    xhat = mid * inv
    dx = inv * (sa - jnp.mean(sa, axis=1, keepdims=True) - xhat * jnp.mean(sa * xhat, axis=1, keepdims=True))
    tg_ref[...] = g_ref[...].astype(F32) + dx
    for ld in loads[4:6]:
        ld.wait()
    paste_share(geo, i, gb, fb)
    rows_n = 1024
    full = OWN // rows_n
    pairs = ((wg_hbm, ob), (nw_hbm, wb), (nm_hbm, mb), (ns_hbm, sb))

    def adam(n, carry):
        rows = pl.ds(mult(n * rows_n, rows_n), rows_n)
        adam_rows(i, rows, n * rows_n, rows_n, wb, mb, sb, ob, gb)
        for k, (h, b) in enumerate(pairs):
            pltpu.make_async_copy(b.at[rows], h.at[rows], lsem.at[k]).start()
        return carry

    for n, part in enumerate(parts):
        for ld in part:
            ld.wait()
        lax.fori_loop(min(4 * n, full), min(4 * n + 4, full), adam, 0)
    rest = OWN - full * rows_n
    adam_rows(i, pl.ds(full * rows_n, 16), full * rows_n, 16, wb, mb, sb, ob, gb)
    for k, (h, b) in enumerate(pairs):
        rows = pl.ds(full * rows_n, rest)
        pltpu.make_async_copy(b.at[rows], h.at[rows], lsem.at[k]).start()
    for k, (h, b) in enumerate(pairs):
        pltpu.make_async_copy(b.at[pl.ds(0, OWN)], h, lsem.at[k]).wait()


def adam_rows(i, rows, start, n, wb, mb, sb, ob, gb):
    g = gb[pl.ds(13 * i + start, n), :]
    w = wb[rows, :]
    m = BETA_ONE * mb[rows, :] + (1.0 - BETA_ONE) * g
    s = BETA_TWO * sb[rows, :] + (1.0 - BETA_TWO) * g * g
    ob[rows, :] = g
    mb[rows, :] = m
    sb[rows, :] = s
    mh = m * (1.0 / (1.0 - BETA_ONE**STEP))
    vh = s * (1.0 / (1.0 - BETA_TWO**STEP))
    wb[rows, :] = w - LEARN_RATE * (mh / (jnp.sqrt(vh) + EPSILON) + DECAY_RATE * w)


def paste_share(geo, i, gb, f_ref):
    q = geo.q

    def put(j, e, row, n, start, stride):
        gb[pl.ds(start, n, stride=stride), :] = f_ref[j, e, pl.ds(row, n), :].astype(F32)

    @pl.when(i < 2)
    def _():
        def body(n, c):
            e, s = n % q, n // q
            for b in range(8):
                put(b, e, mult(geo.qr * s, 16), geo.qr, 24 * geo.qr * e + 8 * s + b, 24)
            return c

        lax.fori_loop(0, 3 * q, body, 0)

    def rows_part(a0, ro, shift, count):
        def body(n, c):
            e, bl = n % q, n // q
            bb = bl + shift
            for b in range(8):
                put(
                    bb % V,
                    e,
                    mult(ro + geo.ap * (bb // V) + geo.ho * b, 16),
                    geo.ho,
                    a0 + 8 * (128 * bl + geo.ho * e) + b,
                    8,
                )
            return c

        lax.fori_loop(0, count * q, body, 0)

    def cols_part(a0, nr, ro):
        def body(n, c):
            e, t = n % q, n // q
            for b in range(8):
                put(b, e, mult(ro + nr * t, 16), nr, a0 + 32 * nr * e + 8 * t + b, 32)
            return c

        lax.fori_loop(0, 4 * q, body, 0)

    @pl.when(i == 2)
    def _():
        rows_part(0, 0, 0, 8)
        cols_part(8192, geo.u2, geo.ap)

    @pl.when((i == 3) | (i == 4))
    def _():
        cols_part(0, geo.u3, 0)

    @pl.when(i == 5)
    def _():
        cols_part(0, geo.u2, 0)
        rows_part(4096, geo.bp, 0, 8)

    @pl.when(i >= 6)
    def _():
        rows_part(0, 0, 4 * (i - 6), 12)


def adam(geo, so, sa, x, g, tail, f, w, m, s):
    tl = geo.tl
    vm = pl.BlockSpec(memory_space=pltpu.VMEM)
    hbm = pl.BlockSpec(memory_space=pl.ANY)
    flat = jax.ShapeDtypeStruct((OWN, 128), F32)
    big = pltpu.VMEM((OWN + 3, 128), F32)
    return pl.pallas_call(
        partial(adam_kernel, geo),
        out_shape=(
            jax.ShapeDtypeStruct((tl, D), BF16),
            jax.ShapeDtypeStruct((tl, D), F32),
            flat, flat, flat, flat,
        ),
        in_specs=[hbm] * 9,
        out_specs=(vm, vm, hbm, hbm, hbm, hbm),
        scratch_shapes=[
            big, big, big, big,
            pltpu.VMEM((ALI + 128, 128), F32),
            pltpu.VMEM((V, geo.q, geo.er, 128), BF16),
            pltpu.VMEM((tl, D), F32),
            pltpu.VMEM((tl, D), F32),
            pltpu.VMEM((tl, D), BF16),
            pltpu.VMEM((tl, D), BF16),
            pltpu.SemaphoreType.DMA((24,)),
        ],
        compiler_params=pltpu.CompilerParams(vmem_limit_bytes=67_000_000),
        name="adam",
    )(so, sa, x, g, tail, f, w, m, s)


def local(mesh, tokens, cotangent, weights, first_moment, second_moment):
    rep = mesh.shape["ctx"] // V
    rows = tokens.shape[1]
    x, g = tokens[0], cotangent[0]
    flats = [weights, first_moment, second_moment]
    if rep > 1:
        groups = [[rep * k + r for r in range(rep)] for k in range(V)]
        join = lambda a: lax.all_gather(a, "ctx", axis=0, axis_index_groups=groups, tiled=True)
        x, g = join(x), join(g)
        flats = [join(a) for a in flats]
    w, m, s = [a.reshape(OWN, 128) for a in flats]
    geo = Geo(mesh, x.shape[0] * V)
    so, sa, f, tail = main(geo, w, x, g)
    outs = list(adam(geo, so, sa, x, g, tail, f, w, m, s))
    outs[2:] = [a.reshape(-1) for a in outs[2:]]
    if rep > 1:
        r = lax.axis_index("ctx") % rep
        outs = [lax.dynamic_slice_in_dim(a, r * (a.shape[0] // rep), a.shape[0] // rep, 0) for a in outs]
    return (outs[0][None], outs[1][None], *outs[2:])


def solution(mesh):
    return jax.shard_map(
        partial(local, mesh),
        mesh=mesh,
        in_specs=(P("dp", "ctx", None), P("dp", "ctx", None), P("ctx"), P("ctx"), P("ctx")),
        out_specs=(P("dp", "ctx", None), P("dp", "ctx", None), P("ctx"), P("ctx"), P("ctx"), P("ctx")),
        check_vma=False,
    )
```
